32 devices in a mesh: gx: 2 (over x), gy: 4 (over y, core), gz: 4 (over z).
Axes of the slice: x: 2, y: 2, z: 4, core: 2. Of those that a mesh axis runs over, the one named last changes fastest.
Arguments:
- velocity: float32 [3, 32, 128, 512], P(None, 'gx', 'gy', 'gz'), may hold values from -6 to 6
- forcing: float32 [3, 32, 128, 512], P(None, 'gx', 'gy', 'gz'), may hold values from -12 to 12
- phase_block: int32 [8, 32, 128], P('gx', 'gy', 'gz'), may hold values from 0 to 7
- prefactor: float32 [8], replicated, may hold values from 0.5 to 4
- yield_stress: float32 [8], replicated, may hold values from 1 to 16
Outputs:
- smoothed: float32 [3, 32, 128, 512], P(None, 'gx', 'gy', 'gz')
- viscosity_field: float32 [32, 128, 512], P('gx', 'gy', 'gz')
- coarse_one: float32 [16, 64, 256], P('gx', 'gy', 'gz')
- coarse_two: float32 [8, 32, 128], P('gx', 'gy', 'gz')
- coarse_three: float32 [4, 16, 64], P('gx', 'gy', 'gz')
- residual_field: float32 [3, 32, 128, 512], P(None, 'gx', 'gy', 'gz')
- residual_rms: float32 [], replicated
The draws below stay inside these ranges and needn't reach their ends.
All inputs are finite; a program needn't handle non-finite values.
Results may differ from the reference program's by a relative error of at most 0.000053.
Values sent between devices are 32-bit elements; how exact they have to be, the bound alone decides.
A program may use at most 64 MiB of HBM per device.

```python
import math
import jax
import jax.numpy as jnp
from jax import lax

BLOCK = 4
NPHASE = 8
SWEEPS = 2
NX = 32
NY = 128
NZ = 512


def draw_forcing(key, part):
    first_key = jax.random.fold_in(key, 11)
    position = jnp.arange(NX, dtype=jnp.float32) / NX
    ramp = (1.0 + 2.0 * position)[None, :, None, None]
    values = jax.random.truncated_normal(first_key, -4.0, 4.0, (3, NX, NY, NZ), jnp.float32)
    return values * ramp


def set_ends(array, stream_key, smallest, high):
    place = [jax.random.randint(jax.random.fold_in(stream_key, axis), (), 0, length) for axis, length in enumerate(array.shape)]
    widest = array.shape.index(max(array.shape))
    beside = place[:widest] + [(place[widest] + 1) % array.shape[widest]] + place[widest + 1:]
    return array.at[tuple(place)].set(smallest).at[tuple(beside)].set(high)


def block_scale(own_key, shape, pieces, smallest, largest):
    def one(dim, parts):
        steps = jax.random.uniform(jax.random.fold_in(jax.random.fold_in(own_key, 6), dim), (parts,), jnp.float32, smallest / len(pieces), largest / len(pieces))
        return jnp.repeat(jnp.exp(steps), shape[dim] // parts).reshape((-1,) + (1,) * (len(shape) - dim - 1))

    loudness = one(*pieces[0])
    for cut in pieces[1:]:
        loudness = loudness * one(*cut)
    return loudness


def bell_draw(own_key, shape, spread, bound, shards=(), kind=jnp.bfloat16):
    values = spread * jax.random.normal(own_key, shape, jnp.float32)
    if shards:
        values = values * block_scale(own_key, shape, shards, -0.22, 0.18)
    return jnp.clip(values, -bound, bound).astype(kind)


def setup_inputs(seed: int = 0) -> dict:
    splits = jax.random.split(jax.random.key(seed), 6)
    velocity = bell_draw(splits[0], (3, NX, NY, NZ), 1.0, 6.0, ((1, 2), (2, 4), (3, 4)), jnp.float32)
    forcing = draw_forcing(jax.random.fold_in(splits[5], 71), 0)
    phase_block = set_ends(jax.random.randint(splits[2], (NX // BLOCK, NY // BLOCK, NZ // BLOCK), 0, NPHASE), jax.random.fold_in(splits[2], 1), 0, NPHASE - 1).astype(jnp.int32)
    prefactor = jnp.clip(jnp.exp(jax.random.uniform(splits[3], (NPHASE,), jnp.float32, math.log(0.5), math.log(4.0))), 0.5, 4.0)
    yield_stress = jnp.clip(jnp.exp(jax.random.uniform(splits[4], (NPHASE,), jnp.float32, math.log(1.0), math.log(16.0))), 1.0, 16.0)
    return dict(velocity=velocity, forcing=forcing, phase_block=phase_block, prefactor=prefactor, yield_stress=yield_stress)


RELAXATION = 0.8
NEIGHBOUR_OFFSETS = ((1, 0, 0), (-1, 0, 0), (0, 1, 0), (0, -1, 0), (0, 0, 1), (0, 0, -1))
UNIT_STEPS = ((1, 0, 0), (0, 1, 0), (0, 0, 1))

def offset_view(field, shift_x, shift_y, shift_z):
    size_x = field.shape[-3] - 2
    size_y = field.shape[-2] - 2
    size_z = field.shape[-1] - 2
    return field[..., 1 + shift_x:1 + shift_x + size_x, 1 + shift_y:1 + shift_y + size_y, 1 + shift_z:1 + shift_z + size_z]

def viscosity_of(padded_vel, prefactor_cells, yield_cells):
    gradient = []
    for comp_a in range(3):
        row_list = []
        for comp_b in range(3):
            step_up = UNIT_STEPS[comp_b]
            step_down = (-step_up[0], -step_up[1], -step_up[2])
            row_list.append(0.5 * (offset_view(padded_vel[comp_a], *step_up) - offset_view(padded_vel[comp_a], *step_down)))
        gradient.append(row_list)
    strain_sq = jnp.zeros(gradient[0][0].shape, jnp.float32)
    for comp_a in range(3):
        for comp_b in range(3):
            strain = 0.5 * (gradient[comp_a][comp_b] + gradient[comp_b][comp_a])
            strain_sq = strain_sq + strain * strain
    invariant = 0.5 * strain_sq + 1.0
    creeping = prefactor_cells * jnp.power(invariant, -1.0 / 3.0)
    plastic = yield_cells / (2.0 * jnp.sqrt(invariant))
    return jnp.minimum(creeping, plastic)

def restrict_dim(field, dim_index):
    coarse_len = (field.shape[dim_index] - 2) // 2

    def every_other(start):
        return lax.slice_in_dim(field, start, start + 2 * coarse_len - 1, 2, dim_index)
    return (every_other(0) + 3.0 * every_other(1) + 3.0 * every_other(2) + every_other(3)) * 0.125

def coarsen(padded):
    return restrict_dim(restrict_dim(restrict_dim(padded, 0), 1), 2)

def smooth_terms(padded_vel, padded_visc):
    centre = offset_view(padded_visc, 0, 0, 0)
    diagonal = jnp.zeros(centre.shape, jnp.float32)
    neighbours = jnp.zeros((3,) + centre.shape, jnp.float32)
    for offset in NEIGHBOUR_OFFSETS:
        face_visc = 0.5 * (centre + offset_view(padded_visc, *offset))
        diagonal = diagonal + face_visc
        neighbours = neighbours + face_visc[None] * offset_view(padded_vel, *offset)
    return (diagonal, neighbours)

def jacobi_sweep(padded_vel, padded_visc, forcing):
    diagonal, neighbours = smooth_terms(padded_vel, padded_visc)
    centre_vel = offset_view(padded_vel, 0, 0, 0)
    return centre_vel + RELAXATION * (forcing - (diagonal[None] * centre_vel - neighbours)) / diagonal[None]

def misfit(padded_vel, padded_visc, forcing):
    diagonal, neighbours = smooth_terms(padded_vel, padded_visc)
    centre_vel = offset_view(padded_vel, 0, 0, 0)
    return forcing - (diagonal[None] * centre_vel - neighbours)

def pad_vel(field):
    return jnp.pad(field, ((0, 0), (1, 1), (1, 1), (1, 1)))

def reference(velocity, forcing, phase_block, prefactor, yield_stress):
    cell_phase = jnp.repeat(jnp.repeat(jnp.repeat(phase_block, BLOCK, 0), BLOCK, 1), BLOCK, 2)
    prefactor_cells = prefactor[cell_phase]
    yield_cells = yield_stress[cell_phase]
    viscosity_field = viscosity_of(pad_vel(velocity), prefactor_cells, yield_cells)
    coarse_one = coarsen(jnp.pad(viscosity_field, 1))
    coarse_two = coarsen(jnp.pad(coarse_one, 1))
    coarse_three = coarsen(jnp.pad(coarse_two, 1))
    padded_visc = jnp.pad(viscosity_field, 1)
    current = velocity
    for sweep_index in range(SWEEPS):
        current = jacobi_sweep(pad_vel(current), padded_visc, forcing)
    misfit_field = misfit(pad_vel(current), padded_visc, forcing)
    residual_rms = jnp.sqrt(jnp.sum(misfit_field * misfit_field) / (3.0 * NX * NY * NZ))
    return (current, viscosity_field, coarse_one, coarse_two, coarse_three, misfit_field, residual_rms)
```

```python
import functools

import jax
import jax.numpy as jnp
import numpy as np
from jax import lax
from jax.experimental import pallas as pl
from jax.experimental.pallas import tpu as pltpu
from jax.sharding import PartitionSpec as P

BLOCK = 4
RELAXATION = 0.8
PAD = 8
GHOST = 64
UNROLL = 7
ONE_STAGE = 32
ROUNDS = 4
MESH = pl.DeviceIdType.MESH
HIGHEST = lax.Precision.HIGHEST


def coarse_matrices(length):
    def chain(low_edge, high_edge):
        field = np.eye(length)
        found = []
        first = 0
        for _ in range(3):
            count = length >> (len(found) + 1)
            out = np.zeros((length, count + 2))
            for k in range(-1, count + 1):
                for shift, weight in ((-1, 1.0), (0, 3.0), (1, 3.0), (2, 1.0)):
                    source = 2 * k + shift - first
                    if 0 <= source < field.shape[1]:
                        out[:, k + 1] += weight / 8.0 * field[:, source]
            if low_edge:
                out[:, 0] = 0.0
            if high_edge:
                out[:, -1] = 0.0
            placed = np.zeros((length, length))
            placed[:, :count] = out[:, 1:-1]
            placed[:, GHOST] = out[:, 0]
            placed[:, GHOST + 1] = out[:, -1]
            found.append(placed)
            field = out
            first = -1
        return np.stack(found)

    inner = chain(False, False)
    return np.stack([inner, inner - chain(True, False), inner - chain(False, True)]).astype(np.float32)


def kernel(
    sizes,
    vel_hbm,
    forc_hbm,
    mats_hbm,
    phase_hbm,
    pref_hbm,
    yield_hbm,
    smooth_ref,
    visc_ref,
    one_ref,
    two_ref,
    three_ref,
    misfit_ref,
    rms_ref,
    v0,
    v1,
    v2,
    visc,
    forc,
    mats,
    phase_ref,
    pref_ref,
    yield_ref,
    faces,
    z_faces,
    early,
    weight,
    diag,
    pref_cells,
    yield_cells,
    y_send,
    y_recv,
    z_send,
    z_recv,
    cx1,
    cx2,
    cx3,
    gx_send,
    gx_recv,
    t1,
    t2a,
    t2b,
    t3a,
    t3b,
    t3c,
    gy_send,
    gy_recv,
    gz_send,
    gz_recv,
    sums_xy,
    sums_z,
    local_sem,
    send_sem,
    recv_sem,
    plane_send,
    plane_recv,
    line_send,
    line_recv,
):
    nx, ny, nz, cx, cy, cz, phases = sizes
    ix, iy, iz = lax.axis_index("gx"), lax.axis_index("gy"), lax.axis_index("gz")
    rows = pl.ds(PAD, cy)

    vel_in = pltpu.make_async_copy(vel_hbm, v0.at[:, pl.ds(1, cx), rows, :], local_sem.at[0])
    forc_in = pltpu.make_async_copy(forc_hbm, forc, local_sem.at[1])
    mats_in = pltpu.make_async_copy(mats_hbm, mats, local_sem.at[2])
    vel_in.start()
    forc_in.start()
    mats_in.start()
    phase_in = pltpu.make_async_copy(phase_hbm, phase_ref, local_sem.at[3])
    phase_in.start()
    pref_in = pltpu.make_async_copy(pref_hbm, pref_ref, local_sem.at[4])
    pref_in.start()
    yield_in = pltpu.make_async_copy(yield_hbm, yield_ref, local_sem.at[5])
    yield_in.start()

    plane0 = jnp.zeros((3, cy, cz), jnp.float32)
    for buf in (v0, v1, v2):
        buf[:, 0, rows, :] = plane0
        buf[:, cx + 1, rows, :] = plane0
    row0 = jnp.zeros((3, cx, 1, cz), jnp.float32)
    visc[1 : cx + 1, PAD - 1 : PAD, :] = row0[0]
    visc[1 : cx + 1, PAD + cy : PAD + cy + 1, :] = row0[0]
    for buf in (v1, v2):
        buf[:, 1 : cx + 1, PAD - 1 : PAD, :] = row0
        buf[:, 1 : cx + 1, PAD + cy : PAD + cy + 1, :] = row0
    visc[0, rows, :] = plane0[0]
    visc[cx + 1, rows, :] = plane0[0]
    y_recv[...] = jnp.zeros(y_recv.shape, jnp.float32)
    z_recv[...] = jnp.zeros(z_recv.shape, jnp.float32)
    gx_recv[...] = jnp.zeros(gx_recv.shape, jnp.float32)
    gy_recv[...] = jnp.zeros(gy_recv.shape, jnp.float32)
    gz_recv[...] = jnp.zeros(gz_recv.shape, jnp.float32)

    barrier = pltpu.get_barrier_semaphore()
    me_xy = ix * ny + iy
    one_stage = nx * ny * nz <= ONE_STAGE
    plane_peers = []
    if one_stage:
        me_first = me_xy * nz + iz
        for k in range(1, nx * ny * nz):
            other = lax.rem(me_first + k, nx * ny * nz)
            plane_peers.append((other // (ny * nz), lax.rem(other // nz, ny), lax.rem(other, nz)))
        line_peers = []
    else:
        me_first = me_xy
        for k in range(1, nx * ny):
            other = lax.rem(me_xy + k, nx * ny)
            plane_peers.append((other // ny, lax.rem(other, ny), iz))
        line_peers = [(ix, iy, lax.rem(iz + k, nz)) for k in range(1, nz)]
    steps = [nx - 1, ny - 1, nz - 1] if one_stage else [nx - 1, ny - 1]
    if sum(steps) - max(steps) <= ROUNDS:
        greeted = [(lax.rem(ix + k, nx), iy, iz) for k in range(1, nx)]
        greeted += [(ix, lax.rem(iy + k, ny), iz) for k in range(1, ny)]
        greeted += [(ix, iy, lax.rem(iz + k, nz)) for k in range(1, nz)]
    else:
        greeted = plane_peers + line_peers
    for peer in greeted:
        pl.semaphore_signal(barrier, inc=1, device_id=peer, device_id_type=MESH)

    lane = lax.broadcasted_iota(jnp.int32, (cy, cz), 1)
    odd_lane = lax.rem(lane, 2) == 1
    first_lane = lane == 0
    last_lane = lane == cz - 1

    up_ids = (
        (lax.rem(ix + 1, nx), iy, iz),
        (ix, lax.rem(iy + 1, ny), iz),
        (ix, iy, lax.rem(iz + 1, nz)),
    )
    down_ids = (
        (lax.rem(ix + nx - 1, nx), iy, iz),
        (ix, lax.rem(iy + ny - 1, ny), iz),
        (ix, iy, lax.rem(iz + nz - 1, nz)),
    )
    has_up = (ix < nx - 1, iy < ny - 1, iz < nz - 1)
    has_down = (ix > 0, iy > 0, iz > 0)
    started = []

    def exchange(slot, dim, up_src, up_dst, down_src, down_dst):
        up = pltpu.make_async_remote_copy(
            up_src, up_dst, send_sem.at[slot, 0], recv_sem.at[slot, 0],
            device_id=up_ids[dim], device_id_type=MESH,
        )
        down = pltpu.make_async_remote_copy(
            down_src, down_dst, send_sem.at[slot, 1], recv_sem.at[slot, 1],
            device_id=down_ids[dim], device_id_type=MESH,
        )
        pl.when(has_up[dim])(up.start)
        pl.when(has_down[dim])(down.start)
        started.append((has_up[dim], up))
        started.append((has_down[dim], down))

        def wait():
            pl.when(has_down[dim])(up.wait_recv)
            pl.when(has_up[dim])(down.wait_recv)

        return wait

    def send_x(r, buf, vector):
        if vector:
            return exchange(
                3 * r, 0,
                buf.at[:, cx, rows, :], buf.at[:, 0, rows, :],
                buf.at[:, 1, rows, :], buf.at[:, cx + 1, rows, :],
            )
        return exchange(
            3 * r, 0,
            buf.at[cx, rows, :], buf.at[0, rows, :],
            buf.at[1, rows, :], buf.at[cx + 1, rows, :],
        )

    def send_yz(r):
        held = pl.ds(0, 1 if r == 1 else 3)
        return [
            exchange(
                3 * r + 1, 1,
                y_send.at[r, 0, held], y_recv.at[r, 0, held],
                y_send.at[r, 1, held], y_recv.at[r, 1, held],
            ),
            exchange(3 * r + 2, 2, z_send.at[r], z_recv.at[r, 0], z_send.at[r], z_recv.at[r, 1]),
        ]

    def pack(r, comp, i, value, packed):
        y_send[r, 0, comp, pl.ds(i, 1), :] = value[cy - 1 : cy, :]
        y_send[r, 1, comp, pl.ds(i, 1), :] = value[0:1, :]
        place = 2 * (comp * cx + i) + 1
        here = (lane == place) | (lane == place + 1)
        return jnp.where(here, pltpu.roll(value, place + 1, 1), packed)

    def unpack_y(r, buf, comps):
        def body(i, carry):
            for comp in range(comps):
                target = buf.at[comp, i + 1] if comps == 3 else buf.at[i + 1]
                target[PAD - 1 : PAD, :] = y_recv[r, 0, comp, pl.ds(i, 1), :]
                target[PAD + cy : PAD + cy + 1, :] = y_recv[r, 1, comp, pl.ds(i, 1), :]
            return carry

        lax.fori_loop(0, cx, body, 0)

    def merged_z(r):
        return jnp.where(odd_lane, z_recv[r, 0], pltpu.roll(z_recv[r, 1], cz - 2, 1))

    def along(plane_ref, centre, merged, place):
        edge = pltpu.roll(merged, cz - 1 - 2 * place, 1)
        return (
            plane_ref[PAD - 1 : PAD - 1 + cy, :],
            plane_ref[PAD + 1 : PAD + 1 + cy, :],
            jnp.where(first_lane, edge, pltpu.roll(centre, 1, 1)),
            jnp.where(last_lane, edge, pltpu.roll(centre, cz - 1, 1)),
        )

    def around(buf, comp, i, merged):
        centre = buf[comp, i + 1, rows, :]
        ym, yp, zm, zp = along(buf.at[comp, i + 1], centre, merged, comp * cx + i)
        return centre, (buf[comp, i, rows, :], buf[comp, i + 2, rows, :], ym, yp, zm, zp)

    vel_in.wait()

    def pack_first(i, packed):
        for comp in range(3):
            packed = pack(0, comp, i, v0[comp, i + 1, rows, :], packed)
        return packed

    nothing = jnp.zeros((cy, cz), jnp.float32)
    z_send[0] = lax.fori_loop(0, cx, pack_first, nothing, unroll=UNROLL)
    pl.semaphore_wait(barrier, len(greeted))
    waits = [send_x(0, v0, True)] + send_yz(0)

    phase_in.wait()
    pref_in.wait()
    yield_in.wait()
    blocks = phase_ref[...].astype(jnp.float32)
    n_rows, n_blocks = blocks.shape
    spread_z = lax.broadcasted_iota(jnp.int32, (n_blocks, cz), 1) // BLOCK
    spread_z = (spread_z == lax.broadcasted_iota(jnp.int32, (n_blocks, cz), 0)).astype(jnp.float32)
    spread_y = lax.broadcasted_iota(jnp.int32, (n_rows * BLOCK, n_rows), 0) // BLOCK
    spread_y = (
        spread_y == lax.broadcasted_iota(jnp.int32, (n_rows * BLOCK, n_rows), 1)
    ).astype(jnp.float32)
    cells = jnp.dot(blocks, spread_z, preferred_element_type=jnp.float32, precision=HIGHEST)
    cells = jnp.dot(spread_y, cells, preferred_element_type=jnp.float32, precision=HIGHEST)
    for bx in range(cx // BLOCK):
        phase = cells[bx * cy : (bx + 1) * cy, :]
        pref_value = jnp.zeros((cy, cz), jnp.float32)
        yield_value = jnp.zeros((cy, cz), jnp.float32)
        for p in range(phases):
            here = jnp.abs(phase - float(p)) < 0.5
            pref_value = jnp.where(here, pref_ref[p], pref_value)
            yield_value = jnp.where(here, yield_ref[p], yield_value)
        pref_cells[bx] = pref_value
        yield_cells[bx] = 0.5 * yield_value
    for buf in (cx1, cx2, cx3):
        for edge in (0, PAD + cy):
            buf[:, edge : edge + PAD, :] = jnp.zeros((buf.shape[0], PAD, cz), jnp.float32)
    for buf in (t1, t2a, t2b, t3a, t3b, t3c):
        buf[...] = jnp.zeros(buf.shape, jnp.float32)

    for wait in waits:
        wait()
    unpack_y(0, v0, 3)
    merged0 = merged_z(0)

    def ends_first(body, r, buf, vector, inner=None):
        packed = lax.fori_loop(0, 2, lambda t, carry: body(t * (cx - 1), carry), nothing)
        sent = send_x(r, buf, vector)
        z_send[r] = lax.fori_loop(1, cx - 1, inner or body, packed, unroll=UNROLL)
        return [sent] + send_yz(r)

    def visc_plane(i, packed):
        jump = []
        for comp in range(3):
            _, (xm, xp, ym, yp, zm, zp) = around(v0, comp, i, merged0)
            jump.append((xp - xm, yp - ym, zp - zm))
        straight = sum(jump[a][a] * jump[a][a] for a in range(3))
        skew = jnp.zeros((cy, cz), jnp.float32)
        for a, b in ((0, 1), (0, 2), (1, 2)):
            both = jump[a][b] + jump[b][a]
            skew = skew + both * both
        invariant = 1.0 + (0.125 * straight + 0.0625 * skew)
        creeping = pref_cells[i // BLOCK] * jnp.exp(jnp.log(invariant) * (-1.0 / 3.0))
        plastic = yield_cells[i // BLOCK] * lax.rsqrt(invariant)
        value = jnp.minimum(creeping, plastic)
        visc[i + 1, rows, :] = value
        visc_ref[i] = value
        return pack(1, 0, i, value, packed)

    waits = ends_first(visc_plane, 1, visc, False)

    def flag(condition):
        return jnp.where(condition, 1.0, 0.0).astype(jnp.float32)

    def restrict_planes(source, first, held, count, target, level):
        for k in range(-1, count + 1):
            total = None
            for shift, factor in ((-1, 0.125), (0, 0.375), (1, 0.375), (2, 0.125)):
                at = 2 * k + shift - first
                if 0 <= at < held:
                    term = factor * source[at, rows, :]
                    total = term if total is None else total + term
            if k == -1:
                total = total * flag(has_down[0])
                gx_send[1, level] = total
            if k == count:
                total = total * flag(has_up[0])
                gx_send[0, level] = total
            target[k + 1, rows, :] = total

    restrict_planes(visc.at[pl.ds(1, cx)], 0, cx, cx // 2, cx1, 0)
    restrict_planes(cx1, -1, cx // 2 + 2, cx // 4, cx2, 1)
    restrict_planes(cx2, -1, cx // 4 + 2, cx // 8, cx3, 2)
    wait_gx = exchange(12, 0, gx_send.at[0], gx_recv.at[0], gx_send.at[1], gx_recv.at[1])

    forc_in.wait()

    def early_one(i, carry):
        plane = visc.at[i + 1]
        centre = plane[rows, :]
        sides = (
            centre + visc[i, rows, :],
            centre + visc[i + 2, rows, :],
            centre + plane[PAD - 1 : PAD - 1 + cy, :],
            centre + plane[PAD + 1 : PAD + 1 + cy, :],
            centre + jnp.where(first_lane, 0.0, pltpu.roll(centre, 1, 1)),
            centre + jnp.where(last_lane, 0.0, pltpu.roll(centre, cz - 1, 1)),
        )
        for n, side in enumerate(sides):
            faces[n, i] = side
        diag[i] = (sides[0] + sides[1]) + (sides[2] + sides[3]) + (sides[4] + sides[5])
        for comp in range(3):
            _, near = around(v0, comp, i, merged0)
            flow = 2.0 * forc[comp, i]
            for n in range(6):
                flow = flow + sides[n] * near[n]
            early[comp, i] = flow
        return carry

    lax.fori_loop(1, cx - 1, early_one, 0, unroll=UNROLL)
    for wait in waits:
        wait()

    def late_one(i, carry):
        ends = ((0, 2, 0, PAD - 1), (1, 3, cy - 1, PAD + cy))
        for side, face, at, row in ends:
            halo = y_recv[1, side, 0, pl.ds(i, 1), :]
            faces[face, i, at : at + 1, :] = faces[face, i, at : at + 1, :] + halo
            diag[i, at : at + 1, :] = diag[i, at : at + 1, :] + halo
            for comp in range(3):
                near = v0[comp, i + 1, row : row + 1, :]
                early[comp, i, at : at + 1, :] = early[comp, i, at : at + 1, :] + halo * near
        return carry

    for i in (0, cx - 1):
        visc[i + 1, PAD - 1 : PAD, :] = y_recv[1, 0, 0, i : i + 1, :]
        visc[i + 1, PAD + cy : PAD + cy + 1, :] = y_recv[1, 1, 0, i : i + 1, :]
    lax.fori_loop(1, cx - 1, late_one, 0, unroll=UNROLL)
    merged1 = merged_z(1)

    def sweep_one_inner(i, packed):
        halo = pltpu.roll(merged1, cz - 1 - 2 * i, 1)
        halo = jnp.where(first_lane | last_lane, halo, 0.0)
        total = diag[i] + halo
        scale = RELAXATION / total
        diag[i] = total
        weight[i] = scale
        own = jnp.where(first_lane, faces[4, i], jnp.where(last_lane, faces[5, i], 0.0))
        z_faces[i] = own + halo
        for comp in range(3):
            edge = pltpu.roll(merged0, cz - 1 - 2 * (comp * cx + i), 1)
            flow = early[comp, i] + halo * edge
            value = (1.0 - RELAXATION) * v0[comp, i + 1, rows, :] + scale * flow
            v1[comp, i + 1, rows, :] = value
            packed = pack(2, comp, i, value, packed)
        return packed

    def sweep_one(i, packed):
        centre = visc[i + 1, rows, :]
        ym, yp, zm, zp = along(visc.at[i + 1], centre, merged1, i)
        sides = [centre + side for side in (visc[i, rows, :], visc[i + 2, rows, :], ym, yp, zm, zp)]
        total = (sides[0] + sides[1]) + (sides[2] + sides[3]) + (sides[4] + sides[5])
        scale = RELAXATION / total
        for n, side in enumerate(sides):
            faces[n, i] = side
        diag[i] = total
        weight[i] = scale
        z_faces[i] = jnp.where(first_lane, sides[4], jnp.where(last_lane, sides[5], 0.0))
        for comp in range(3):
            here, near = around(v0, comp, i, merged0)
            flow = sides[0] * near[0]
            for n in range(1, 6):
                flow = flow + sides[n] * near[n]
            value = (1.0 - RELAXATION) * here + scale * (2.0 * forc[comp, i] + flow)
            v1[comp, i + 1, rows, :] = value
            packed = pack(2, comp, i, value, packed)
        return packed

    waits = ends_first(sweep_one, 2, v1, True, sweep_one_inner)

    wait_gx()
    low_y, high_y = flag(has_down[1]), flag(has_up[1])
    gx_counts = (cx // 2, cx // 4, cx // 8)
    for level, buf in enumerate((cx1, cx2, cx3)):
        buf[1, rows, :] = buf[1, rows, :] + gx_recv[0, level]
        last = gx_counts[level]
        buf[last, rows, :] = buf[last, rows, :] + gx_recv[1, level]

    def restrict_rows(source, target, count):
        size = count + 2
        a, b, c, d = (source[pl.ds(PAD - 3 + s, size, stride=2), :] for s in range(4))
        target[PAD - 1 : PAD - 1 + size, :] = 0.125 * (a + d) + 0.375 * (b + c)
        target[PAD - 1 : PAD, :] = target[PAD - 1 : PAD, :] * low_y
        target[PAD + count : PAD + count + 1, :] = target[PAD + count : PAD + count + 1, :] * high_y

    row = 0
    ghost_rows = []
    for level, (buf, steps) in enumerate(((cx1, (t1,)), (cx2, (t2a, t2b)), (cx3, (t3a, t3b, t3c)))):
        for k in range(gx_counts[level]):
            source = buf.at[k + 1]
            for depth, target in enumerate(steps):
                restrict_rows(source, target.at[k], cy >> (depth + 1))
                source = target.at[k]
            count = cy >> len(steps)
            gy_send[1, row : row + 1, :] = source[PAD - 1 : PAD, :]
            gy_send[0, row : row + 1, :] = source[PAD + count : PAD + count + 1, :]
            ghost_rows.append((steps[-1], k, count, row))
            row += 1
    wait_gy = exchange(13, 1, gy_send.at[0], gy_recv.at[0], gy_send.at[1], gy_recv.at[1])

    def early_flow(buf):
        def body(i, carry):
            for comp in range(3):
                plane = buf.at[comp, i + 1]
                centre = plane[rows, :]
                low = jnp.where(first_lane, 0.0, pltpu.roll(centre, 1, 1))
                high = jnp.where(last_lane, 0.0, pltpu.roll(centre, cz - 1, 1))
                flow = 2.0 * forc[comp, i]
                flow = flow + faces[0, i] * buf[comp, i, rows, :]
                flow = flow + faces[1, i] * buf[comp, i + 2, rows, :]
                flow = flow + faces[2, i] * plane[PAD - 1 : PAD - 1 + cy, :]
                flow = flow + faces[3, i] * plane[PAD + 1 : PAD + 1 + cy, :]
                early[comp, i] = flow + (faces[4, i] * low + faces[5, i] * high)
            return carry

        lax.fori_loop(1, cx - 1, body, 0, unroll=UNROLL)

    def late_rows(r, buf):
        def body(i, carry):
            for comp in range(3):
                low = faces[2, i, 0:1, :] * y_recv[r, 0, comp, pl.ds(i, 1), :]
                high = faces[3, i, cy - 1 : cy, :] * y_recv[r, 1, comp, pl.ds(i, 1), :]
                early[comp, i, 0:1, :] = early[comp, i, 0:1, :] + low
                early[comp, i, cy - 1 : cy, :] = early[comp, i, cy - 1 : cy, :] + high
            return carry

        for i in (0, cx - 1):
            for comp in range(3):
                buf[comp, i + 1, PAD - 1 : PAD, :] = y_recv[r, 0, comp, i : i + 1, :]
                buf[comp, i + 1, PAD + cy : PAD + cy + 1, :] = y_recv[r, 1, comp, i : i + 1, :]
        lax.fori_loop(1, cx - 1, body, 0, unroll=UNROLL)

    def late(comp, i, merged):
        edge = pltpu.roll(merged, cz - 1 - 2 * (comp * cx + i), 1)
        return early[comp, i] + z_faces[i] * edge

    early_flow(v1)
    for wait in waits:
        wait()
    late_rows(2, v1)
    merged2 = merged_z(2)

    def flow_of(buf, comp, i, merged):
        here, near = around(buf, comp, i, merged)
        flow = faces[0, i] * near[0]
        for n in range(1, 6):
            flow = flow + faces[n, i] * near[n]
        return here, flow

    def sweep_two_inner(i, packed):
        for comp in range(3):
            value = (1.0 - RELAXATION) * v1[comp, i + 1, rows, :] + weight[i] * late(comp, i, merged2)
            v2[comp, i + 1, rows, :] = value
            smooth_ref[comp, i] = value
            packed = pack(3, comp, i, value, packed)
        return packed

    def sweep_two(i, packed):
        for comp in range(3):
            here, flow = flow_of(v1, comp, i, merged2)
            value = (1.0 - RELAXATION) * here + weight[i] * (2.0 * forc[comp, i] + flow)
            v2[comp, i + 1, rows, :] = value
            smooth_ref[comp, i] = value
            packed = pack(3, comp, i, value, packed)
        return packed

    waits = ends_first(sweep_two, 3, v2, True, sweep_two_inner)

    wait_gy()
    for buf, k, count, row in ghost_rows:
        buf[k, PAD : PAD + 1, :] = buf[k, PAD : PAD + 1, :] + gy_recv[0, row : row + 1, :]
        last = PAD + count - 1
        buf[k, last : last + 1, :] = buf[k, last : last + 1, :] + gy_recv[1, row : row + 1, :]
    mats_in.wait()
    off_low, off_high = 1.0 - flag(has_down[2]), 1.0 - flag(has_up[2])
    results = []
    groups = []
    lane8 = lax.broadcasted_iota(jnp.int32, (8, cz), 1)
    packed = jnp.zeros((8, cz), jnp.float32)
    for level, buf in enumerate((t1, t2b, t3c)):
        count = gx_counts[level]
        height = max(8, cy >> (level + 1))
        matrix = mats[0, level] - off_low * mats[1, level] - off_high * mats[2, level]
        data = buf[:, PAD : PAD + height, :].reshape(count * height, cz)
        result = jnp.dot(data, matrix, preferred_element_type=jnp.float32, precision=HIGHEST)
        for part in range(count * height // 8):
            g = len(groups)
            piece = result[8 * part : 8 * part + 8, :]
            groups.append((level, 8 * part // height, 8 * part % height, piece))
            shifted = pltpu.roll(piece, (2 * g - GHOST) % cz, 1)
            packed = jnp.where((lane8 == 2 * g) | (lane8 == 2 * g + 1), shifted, packed)
    gz_send[...] = packed
    wait_gz = exchange(14, 2, gz_send, gz_recv.at[0], gz_send, gz_recv.at[1])

    early_flow(v2)
    for wait in waits:
        wait()
    late_rows(3, v2)
    merged3 = merged_z(3)

    def misfit_plane(i, total):
        for comp in range(3):
            here, flow = flow_of(v2, comp, i, merged3)
            value = forc[comp, i] + 0.5 * (flow - diag[i] * here)
            misfit_ref[comp, i] = value
            total = total + value * value
        return total

    def misfit_inner(i, total):
        for comp in range(3):
            value = 0.5 * (late(comp, i, merged3) - diag[i] * v2[comp, i + 1, rows, :])
            misfit_ref[comp, i] = value
            total = total + value * value
        return total

    squares = lax.fori_loop(0, 2, lambda t, carry: misfit_plane(t * (cx - 1), carry), nothing)
    squares = lax.fori_loop(1, cx - 1, misfit_inner, squares, unroll=UNROLL)
    part = jnp.sum(squares, axis=0, keepdims=True)

    def gather(slots, mine, value, peers, sends, recvs):
        slots[mine] = value
        copies = []
        for k, peer in enumerate(peers):
            copy = pltpu.make_async_remote_copy(
                slots.at[mine], slots.at[mine], sends.at[k], recvs.at[k],
                device_id=peer, device_id_type=MESH,
            )
            copy.start()
            copies.append(copy)
        return copies

    def total_of(slots):
        total = slots[0]
        for n in range(1, slots.shape[0]):
            total = total + slots[n]
        return total

    plane_copies = gather(sums_xy, me_first, part, plane_peers, plane_send, plane_recv)

    wait_gz()
    low_part, high_part = gz_recv[0], gz_recv[1]
    for g, (level, k, at, piece) in enumerate(groups):
        width = cz >> (level + 1)
        height = cy >> (level + 1)
        piece = piece + jnp.where(lane8 == 0, pltpu.roll(low_part, (cz - 2 * g - 1) % cz, 1), 0.0)
        piece = piece + jnp.where(
            lane8 == width - 1, pltpu.roll(high_part, (width - 1 - 2 * g) % cz, 1), 0.0
        )
        target = (one_ref, two_ref, three_ref)[level]
        size = min(8, height - at)
        target[k, at : at + size, :] = piece[:size, :width]

    for copy in plane_copies:
        copy.wait()
    whole = total_of(sums_xy)
    if not one_stage:
        line_copies = gather(sums_z, iz, whole, line_peers, line_send, line_recv)
        for copy in line_copies:
            copy.wait()
        whole = total_of(sums_z)
    whole = jnp.sum(whole, axis=1, keepdims=True)
    cells_all = float(3 * cx * nx * cy * ny * cz * nz)
    rms_ref[...] = jnp.sqrt(whole / cells_all)

    for condition, copy in started:
        pl.when(condition)(copy.wait_send)


def writer(*refs):
    copies = [
        pltpu.make_async_copy(refs[n], refs[7 + n], refs[14].at[n]) for n in (0, 5, 1, 2, 3, 4, 6)
    ]
    for copy in copies:
        copy.start()
    for copy in copies:
        copy.wait()


def per_device(velocity, forcing, phase_block, prefactor, yield_stress):
    _, cx, cy, cz = velocity.shape
    nx, ny, nz = lax.axis_size("gx"), lax.axis_size("gy"), lax.axis_size("gz")
    f32 = jnp.float32
    sizes = (nx, ny, nz, cx, cy, cz, prefactor.shape[0])
    mats = jnp.asarray(coarse_matrices(cz))
    blocks = phase_block.reshape(phase_block.shape[0] * phase_block.shape[1], phase_block.shape[2])
    tall = cy + 2 * PAD
    firsts = nx * ny * nz if nx * ny * nz <= ONE_STAGE else nx * ny
    ghosts = cx // 2 + cx // 4 + cx // 8
    ghosts += -ghosts % 8
    hbm = pl.BlockSpec(memory_space=pltpu.HBM)
    vmem = pl.BlockSpec(memory_space=pltpu.VMEM)
    v = pltpu.VMEM
    field = v((3, cx + 2, tall, cz), f32)
    dma = pltpu.SemaphoreType.DMA
    operands = (velocity, forcing, mats, blocks, prefactor, yield_stress)
    outs = pl.pallas_call(
        functools.partial(kernel, sizes),
        out_shape=(
            jax.ShapeDtypeStruct(velocity.shape, f32),
            jax.ShapeDtypeStruct((cx, cy, cz), f32),
            jax.ShapeDtypeStruct((cx // 2, cy // 2, cz // 2), f32),
            jax.ShapeDtypeStruct((cx // 4, cy // 4, cz // 4), f32),
            jax.ShapeDtypeStruct((cx // 8, cy // 8, cz // 8), f32),
            jax.ShapeDtypeStruct(velocity.shape, f32),
            jax.ShapeDtypeStruct((1, 1), f32),
        ),
        in_specs=[hbm] * 6,
        out_specs=(vmem,) * 7,
        scratch_shapes=[
            field,
            field,
            field,
            v((cx + 2, tall, cz), f32),
            v((3, cx, cy, cz), f32),
            v(mats.shape, f32),
            v(blocks.shape, blocks.dtype),
            pltpu.SMEM(prefactor.shape, f32),
            pltpu.SMEM(yield_stress.shape, f32),
            v((6, cx, cy, cz), f32),
            v((cx, cy, cz), f32),
            v((3, cx, cy, cz), f32),
            v((cx, cy, cz), f32),
            v((cx, cy, cz), f32),
            v((cx // BLOCK, cy, cz), f32),
            v((cx // BLOCK, cy, cz), f32),
            v((4, 2, 3, cx, cz), f32),
            v((4, 2, 3, cx, cz), f32),
            v((4, cy, cz), f32),
            v((4, 2, cy, cz), f32),
            v((cx // 2 + 2, tall, cz), f32),
            v((cx // 4 + 2, tall, cz), f32),
            v((cx // 8 + 2, tall, cz), f32),
            v((2, 3, cy, cz), f32),
            v((2, 3, cy, cz), f32),
            v((cx // 2, tall, cz), f32),
            v((cx // 4, tall, cz), f32),
            v((cx // 4, tall, cz), f32),
            v((cx // 8, tall, cz), f32),
            v((cx // 8, tall, cz), f32),
            v((cx // 8, tall, cz), f32),
            v((2, ghosts, cz), f32),
            v((2, ghosts, cz), f32),
            v((8, cz), f32),
            v((2, 8, cz), f32),
            v((firsts, 1, cz), f32),
            v((nz, 1, cz), f32),
            dma((6,)),
            dma((15, 2)),
            dma((15, 2)),
            dma((firsts - 1,)),
            dma((firsts - 1,)),
            dma((nz - 1,)),
            dma((nz - 1,)),
        ],
        compiler_params=pltpu.CompilerParams(
            collective_id=0, has_side_effects=True, vmem_limit_bytes=40 * 1024 * 1024
        ),
    )(*(pltpu.with_memory_space_constraint(a, pltpu.HBM) for a in operands))
    outs = pl.pallas_call(
        writer,
        out_shape=tuple(jax.ShapeDtypeStruct(out.shape, f32) for out in outs),
        in_specs=[vmem] * 7,
        out_specs=(hbm,) * 7,
        scratch_shapes=[dma((7,))],
        compiler_params=pltpu.CompilerParams(vmem_limit_bytes=8 * 1024 * 1024),
    )(*outs)
    return outs[:6] + (outs[6].reshape(()),)


def solution(mesh):
    grid = P("gx", "gy", "gz")
    vector = P(None, "gx", "gy", "gz")
    return jax.shard_map(
        per_device,
        mesh=mesh,
        in_specs=(vector, vector, grid, P(), P()),
        out_specs=(vector, grid, grid, grid, grid, vector, P()),
        check_vma=False,
    )
```

```python
import functools

import jax
import jax.numpy as jnp
import numpy as np
from jax import lax
from jax.experimental import pallas as pl
from jax.experimental.pallas import tpu as pltpu
from jax.sharding import PartitionSpec as P

BLOCK = 4
RELAXATION = 0.8
PAD = 8
GHOST = 64
UNROLL = 4
VISC_UNROLL = 7
TILE = 8
AHEAD = 2
BEHIND = 2
ONE_STAGE = 32
ROUNDS = 4
MESH = pl.DeviceIdType.MESH
HIGHEST = lax.Precision.HIGHEST


def coarse_matrices(length):
    def chain(low_edge, high_edge):
        field = np.eye(length)
        found = []
        first = 0
        for _ in range(3):
            count = length >> (len(found) + 1)
            out = np.zeros((length, count + 2))
            for k in range(-1, count + 1):
                for shift, weight in ((-1, 1.0), (0, 3.0), (1, 3.0), (2, 1.0)):
                    source = 2 * k + shift - first
                    if 0 <= source < field.shape[1]:
                        out[:, k + 1] += weight / 8.0 * field[:, source]
            if low_edge:
                out[:, 0] = 0.0
            if high_edge:
                out[:, -1] = 0.0
            placed = np.zeros((length, length))
            placed[:, :count] = out[:, 1:-1]
            placed[:, GHOST] = out[:, 0]
            placed[:, GHOST + 1] = out[:, -1]
            found.append(placed)
            field = out
            first = -1
        return np.stack(found)

    inner = chain(False, False)
    return np.stack([inner, inner - chain(True, False), inner - chain(False, True)]).astype(np.float32)


def kernel(
    sizes,
    vel_hbm,
    forc_hbm,
    mats_hbm,
    phase_hbm,
    pref_hbm,
    yield_hbm,
    smooth_ref,
    visc_ref,
    one_ref,
    two_ref,
    three_ref,
    misfit_ref,
    rms_ref,
    v0,
    v1,
    v2,
    visc,
    forc,
    mats,
    phase_ref,
    pref_ref,
    yield_ref,
    faces,
    z_faces,
    z_scaled,
    early,
    weight,
    diag,
    pref_cells,
    yield_cells,
    x_send,
    x_recv,
    visc_x,
    y_send,
    y_recv,
    z_send,
    z_recv,
    cx1,
    cx2,
    cx3,
    gx_send,
    gx_recv,
    t1,
    t2a,
    t2b,
    t3a,
    t3b,
    t3c,
    gy_send,
    gy_recv,
    gz_send,
    gz_recv,
    sums_xy,
    sums_z,
    local_sem,
    send_sem,
    recv_sem,
    plane_send,
    plane_recv,
    line_send,
    line_recv,
):
    nx, ny, nz, cx, cy, cz, phases = sizes
    ix, iy, iz = lax.axis_index("gx"), lax.axis_index("gy"), lax.axis_index("gz")
    rows = pl.ds(PAD, cy)

    vel_in = pltpu.make_async_copy(vel_hbm, v0.at[:, pl.ds(1, cx), rows, :], local_sem.at[0])
    forc_in = pltpu.make_async_copy(forc_hbm, forc, local_sem.at[1])
    mats_in = pltpu.make_async_copy(mats_hbm, mats, local_sem.at[2])
    vel_in.start()
    phase_in = pltpu.make_async_copy(phase_hbm, phase_ref, local_sem.at[3])
    phase_in.start()
    pref_in = pltpu.make_async_copy(pref_hbm, pref_ref, local_sem.at[4])
    pref_in.start()
    yield_in = pltpu.make_async_copy(yield_hbm, yield_ref, local_sem.at[5])
    yield_in.start()

    plane0 = jnp.zeros((3, cy, cz), jnp.float32)
    for buf in (v0, v1, v2):
        buf[:, 0, rows, :] = plane0
        buf[:, cx + 1, rows, :] = plane0
    row0 = jnp.zeros((3, cx, 1, cz), jnp.float32)
    visc[1 : cx + 1, PAD - 1 : PAD, :] = row0[0]
    visc[1 : cx + 1, PAD + cy : PAD + cy + 1, :] = row0[0]
    for buf in (v1, v2):
        buf[:, 1 : cx + 1, PAD - 1 : PAD, :] = row0
        buf[:, 1 : cx + 1, PAD + cy : PAD + cy + 1, :] = row0
    visc[0, rows, :] = plane0[0]
    visc[cx + 1, rows, :] = plane0[0]
    x_recv[...] = jnp.zeros(x_recv.shape, jnp.float32)
    visc_x[...] = jnp.zeros(visc_x.shape, jnp.float32)
    y_recv[...] = jnp.zeros(y_recv.shape, jnp.float32)
    z_recv[...] = jnp.zeros(z_recv.shape, jnp.float32)
    gx_recv[...] = jnp.zeros(gx_recv.shape, jnp.float32)
    gy_recv[...] = jnp.zeros(gy_recv.shape, jnp.float32)
    gz_recv[...] = jnp.zeros(gz_recv.shape, jnp.float32)

    barrier = pltpu.get_barrier_semaphore()
    me_xy = ix * ny + iy
    one_stage = nx * ny * nz <= ONE_STAGE
    plane_peers = []
    if one_stage:
        me_first = me_xy * nz + iz
        for k in range(1, nx * ny * nz):
            other = lax.rem(me_first + k, nx * ny * nz)
            plane_peers.append((other // (ny * nz), lax.rem(other // nz, ny), lax.rem(other, nz)))
        line_peers = []
    else:
        me_first = me_xy
        for k in range(1, nx * ny):
            other = lax.rem(me_xy + k, nx * ny)
            plane_peers.append((other // ny, lax.rem(other, ny), iz))
        line_peers = [(ix, iy, lax.rem(iz + k, nz)) for k in range(1, nz)]
    steps = [nx - 1, ny - 1, nz - 1] if one_stage else [nx - 1, ny - 1]
    if sum(steps) - max(steps) <= ROUNDS:
        greeted = [(lax.rem(ix + k, nx), iy, iz) for k in range(1, nx)]
        greeted += [(ix, lax.rem(iy + k, ny), iz) for k in range(1, ny)]
        greeted += [(ix, iy, lax.rem(iz + k, nz)) for k in range(1, nz)]
    else:
        greeted = plane_peers + line_peers
    for peer in greeted:
        pl.semaphore_signal(barrier, inc=1, device_id=peer, device_id_type=MESH)

    lane = lax.broadcasted_iota(jnp.int32, (cy, cz), 1)
    odd_lane = lax.rem(lane, 2) == 1
    lane_pair = (lane - 1) // 2
    first_lane = lane == 0
    last_lane = lane == cz - 1
    end_lane = first_lane | last_lane

    up_ids = (
        (lax.rem(ix + 1, nx), iy, iz),
        (ix, lax.rem(iy + 1, ny), iz),
        (ix, iy, lax.rem(iz + 1, nz)),
    )
    down_ids = (
        (lax.rem(ix + nx - 1, nx), iy, iz),
        (ix, lax.rem(iy + ny - 1, ny), iz),
        (ix, iy, lax.rem(iz + nz - 1, nz)),
    )
    has_up = (ix < nx - 1, iy < ny - 1, iz < nz - 1)
    has_down = (ix > 0, iy > 0, iz > 0)
    started = []

    def exchange(slot, dim, up_src, up_dst, down_src, down_dst):
        up = pltpu.make_async_remote_copy(
            up_src, up_dst, send_sem.at[slot, 0], recv_sem.at[slot, 0],
            device_id=up_ids[dim], device_id_type=MESH,
        )
        down = pltpu.make_async_remote_copy(
            down_src, down_dst, send_sem.at[slot, 1], recv_sem.at[slot, 1],
            device_id=down_ids[dim], device_id_type=MESH,
        )
        pl.when(has_up[dim])(up.start)
        pl.when(has_down[dim])(down.start)
        started.append((has_up[dim], up))
        started.append((has_down[dim], down))

        def wait():
            pl.when(has_down[dim])(up.wait_recv)
            pl.when(has_up[dim])(down.wait_recv)

        return wait

    def send_x(r, last, low, first, high):
        return exchange(3 * r, 0, last, low, first, high)

    def send_yz(r):
        held = pl.ds(0, 1 if r == 1 else 3)
        return [
            exchange(
                3 * r + 1, 1,
                y_send.at[r, 0, held], y_recv.at[r, 0, held],
                y_send.at[r, 1, held], y_recv.at[r, 1, held],
            ),
            exchange(3 * r + 2, 2, z_send.at[r], z_recv.at[r, 0], z_send.at[r], z_recv.at[r, 1]),
        ]

    def pack(r, comp, i, value, packed):
        y_send[r, 0, comp, pl.ds(i, 1), :] = value[cy - 1 : cy, :]
        y_send[r, 1, comp, pl.ds(i, 1), :] = value[0:1, :]
        place = 2 * (comp * cx + i) + 1
        return jnp.where(lane_pair == comp * cx + i, pltpu.roll(value, place + 1, 1), packed)

    def unpack_y(r, buf, comps):
        def body(i, carry):
            for comp in range(comps):
                target = buf.at[comp, i + 1] if comps == 3 else buf.at[i + 1]
                target[PAD - 1 : PAD, :] = y_recv[r, 0, comp, pl.ds(i, 1), :]
                target[PAD + cy : PAD + cy + 1, :] = y_recv[r, 1, comp, pl.ds(i, 1), :]
            return carry

        lax.fori_loop(0, cx, body, 0)

    def merged_z(r):
        return jnp.where(odd_lane, z_recv[r, 0], pltpu.roll(z_recv[r, 1], cz - 2, 1))

    def along(plane_ref, centre, merged, place):
        edge = pltpu.roll(merged, cz - 1 - 2 * place, 1)
        return (
            plane_ref[PAD - 1 : PAD - 1 + cy, :],
            plane_ref[PAD + 1 : PAD + 1 + cy, :],
            jnp.where(first_lane, edge, pltpu.roll(centre, 1, 1)),
            jnp.where(last_lane, edge, pltpu.roll(centre, cz - 1, 1)),
        )

    def around(buf, comp, i, merged):
        centre = buf[comp, i + 1, rows, :]
        ym, yp, zm, zp = along(buf.at[comp, i + 1], centre, merged, comp * cx + i)
        return centre, (buf[comp, i, rows, :], buf[comp, i + 2, rows, :], ym, yp, zm, zp)

    vel_in.wait()
    forc_in.start()
    mats_in.start()

    nothing = jnp.zeros((cy, cz), jnp.float32)
    packed = nothing
    for i in range(cx):
        for comp in range(3):
            packed = pack(0, comp, i, v0[comp, i + 1, rows, :], packed)
    z_send[0] = packed
    pl.semaphore_wait(barrier, len(greeted))
    waits = [send_x(0, v0.at[:, cx, rows, :], v0.at[:, 0, rows, :], v0.at[:, 1, rows, :], v0.at[:, cx + 1, rows, :])] + send_yz(0)

    phase_in.wait()
    pref_in.wait()
    yield_in.wait()
    blocks = phase_ref[...].astype(jnp.float32)
    n_rows, n_blocks = blocks.shape
    spread_z = lax.broadcasted_iota(jnp.int32, (n_blocks, cz), 1) // BLOCK
    spread_z = (spread_z == lax.broadcasted_iota(jnp.int32, (n_blocks, cz), 0)).astype(jnp.float32)
    spread_y = lax.broadcasted_iota(jnp.int32, (n_rows * BLOCK, n_rows), 0) // BLOCK
    spread_y = (
        spread_y == lax.broadcasted_iota(jnp.int32, (n_rows * BLOCK, n_rows), 1)
    ).astype(jnp.float32)
    cells = jnp.dot(blocks, spread_z, preferred_element_type=jnp.float32, precision=HIGHEST)
    cells = jnp.dot(spread_y, cells, preferred_element_type=jnp.float32, precision=HIGHEST)
    for bx in range(cx // BLOCK):
        phase = cells[bx * cy : (bx + 1) * cy, :]
        pref_value = jnp.zeros((cy, cz), jnp.float32)
        yield_value = jnp.zeros((cy, cz), jnp.float32)
        for p in range(phases):
            here = jnp.abs(phase - float(p)) < 0.5
            pref_value = jnp.where(here, pref_ref[p], pref_value)
            yield_value = jnp.where(here, yield_ref[p], yield_value)
        pref_cells[bx] = pref_value
        yield_cells[bx] = 0.5 * yield_value
    for buf in (cx1, cx2, cx3):
        for edge in (0, PAD + cy):
            buf[:, edge : edge + PAD, :] = jnp.zeros((buf.shape[0], PAD, cz), jnp.float32)
    for buf in (t1, t2a, t2b, t3a, t3b, t3c):
        buf[...] = jnp.zeros(buf.shape, jnp.float32)

    for wait in waits:
        wait()
    unpack_y(0, v0, 3)
    merged0 = merged_z(0)

    order = [0, cx - 1] + list(range(1, cx - 1))

    def shell_pass(edge, value_of, r, send_ends, vector=True):
        comps = 3 if vector else 1
        packed = nothing
        edges, rolled = {}, {}
        sent = None
        for t in range(cx + AHEAD + BEHIND):
            if t < cx:
                edges[t] = edge(order[t])
            n = t - AHEAD
            if 0 <= n < cx:
                i = order[n]
                moved = []
                for comp, value in enumerate(value_of(i, edges.pop(n))):
                    if r is not None:
                        y_send[r, 0, comp, pl.ds(i, 1), :] = value[cy - 1 : cy, :]
                        y_send[r, 1, comp, pl.ds(i, 1), :] = value[0:1, :]
                        moved.append((comp * cx + i, pltpu.roll(value, 2 * (comp * cx + i) + 2, 1)))
                rolled[n] = moved
                if n == 1 and send_ends is not None:
                    sent = send_ends()
            n = t - AHEAD - BEHIND
            if 0 <= n < cx:
                for place, value in rolled.pop(n):
                    packed = jnp.where(lane_pair == place, value, packed)
        if r is None:
            return None
        z_send[r] = packed
        return [sent] + send_yz(r)

    def edge_of(merged, place):
        return pltpu.roll(merged, cz - 1 - 2 * place, 1)

    def visc_plane(i, carry):
        packed, held, at = carry
        out = []
        centres = [v0[comp, i + 1, rows, :] for comp in range(3)]
        edges = [edge_of(merged0, comp * cx + i) for comp in range(3)]
        lows = [pltpu.roll(centre, 1, 1) for centre in centres]
        highs = [pltpu.roll(centre, cz - 1, 1) for centre in centres]
        moved = pltpu.roll(held, 2 * at + 2, 1)
        packed = jnp.where(lane_pair == at, moved, packed)
        jump = []
        for comp in range(3):
            plane = v0.at[comp, i + 1]
            below = jnp.where(first_lane, edges[comp], lows[comp])
            above = jnp.where(last_lane, edges[comp], highs[comp])
            jump.append((
                v0[comp, i + 2, rows, :] - v0[comp, i, rows, :],
                plane[PAD + 1 : PAD + 1 + cy, :] - plane[PAD - 1 : PAD - 1 + cy, :],
                above - below,
            ))
        straight = sum(jump[a][a] * jump[a][a] for a in range(3))
        skew = None
        for a, b in ((0, 1), (0, 2), (1, 2)):
            both = jump[a][b] + jump[b][a]
            skew = both * both if skew is None else skew + both * both
        invariant = 1.0 + (0.125 * straight + 0.0625 * skew)
        creeping = pref_cells[i // BLOCK] * jnp.exp(jnp.log(invariant) * (-1.0 / 3.0))
        plastic = yield_cells[i // BLOCK] * lax.rsqrt(invariant)
        value = jnp.minimum(creeping, plastic)
        visc[i + 1, rows, :] = value
        visc_ref[i] = value
        y_send[1, 0, 0, pl.ds(i, 1), :] = value[cy - 1 : cy, :]
        y_send[1, 1, 0, pl.ds(i, 1), :] = value[0:1, :]
        return packed, value, i

    carry = visc_plane(cx - 1, visc_plane(0, (nothing, nothing, 0)))
    sent = send_x(1, visc.at[cx, rows, :], visc_x.at[0], visc.at[1, rows, :], visc_x.at[1])
    packed, held, at = lax.fori_loop(1, cx - 1, visc_plane, carry, unroll=VISC_UNROLL)
    z_send[1] = jnp.where(lane_pair == at, pltpu.roll(held, 2 * at + 2, 1), packed)
    waits = [sent] + send_yz(1)

    def flag(condition):
        return jnp.where(condition, 1.0, 0.0).astype(jnp.float32)

    def restrict_planes(source, first, held, count, target, level):
        for k in range(-1, count + 1):
            total = None
            for shift, factor in ((-1, 0.125), (0, 0.375), (1, 0.375), (2, 0.125)):
                at = 2 * k + shift - first
                if 0 <= at < held:
                    term = factor * source[at, rows, :]
                    total = term if total is None else total + term
            if k == -1:
                total = total * flag(has_down[0])
                gx_send[1, level] = total
            if k == count:
                total = total * flag(has_up[0])
                gx_send[0, level] = total
            target[k + 1, rows, :] = total

    restrict_planes(visc.at[pl.ds(1, cx)], 0, cx, cx // 2, cx1, 0)
    restrict_planes(cx1, -1, cx // 2 + 2, cx // 4, cx2, 1)
    restrict_planes(cx2, -1, cx // 4 + 2, cx // 8, cx3, 2)
    wait_gx = exchange(12, 0, gx_send.at[0], gx_recv.at[0], gx_send.at[1], gx_recv.at[1])

    forc_in.wait()

    def early_one(i, carry):
        plane = visc.at[i + 1]
        centre = plane[rows, :]
        sides = (
            centre + visc[i, rows, :],
            centre + visc[i + 2, rows, :],
            centre + plane[PAD - 1 : PAD - 1 + cy, :],
            centre + plane[PAD + 1 : PAD + 1 + cy, :],
            centre + jnp.where(first_lane, 0.0, pltpu.roll(centre, 1, 1)),
            centre + jnp.where(last_lane, 0.0, pltpu.roll(centre, cz - 1, 1)),
        )
        for n in range(4):
            faces[n, i] = sides[n]
        faces[4, i] = jnp.where(first_lane, 0.0, sides[4])
        faces[5, i] = jnp.where(last_lane, 0.0, sides[5])
        diag[i] = (sides[0] + sides[1]) + (sides[2] + sides[3]) + (sides[4] + sides[5])
        for comp in range(3):
            _, near = around(v0, comp, i, merged0)
            flow = 2.0 * forc[comp, i]
            for n in range(6):
                flow = flow + sides[n] * near[n]
            early[comp, i] = flow
        return carry

    lax.fori_loop(0, cx, early_one, 0, unroll=UNROLL)
    for wait in waits:
        wait()
    merged1 = merged_z(1)

    for side, i, face, halo_plane in ((0, 0, 0, 0), (1, cx - 1, 1, cx + 1)):
        halo = visc_x[side]
        faces[face, i] = faces[face, i] + halo
        diag[i] = diag[i] + halo
        for comp in range(3):
            early[comp, i] = early[comp, i] + halo * v0[comp, halo_plane, rows, :]

    def late_one(i, carry):
        ends = ((0, 2, 0, PAD - 1), (1, 3, cy - 1, PAD + cy))
        for side, face, at, row in ends:
            halo = y_recv[1, side, 0, pl.ds(i, 1), :]
            faces[face, i, at : at + 1, :] = faces[face, i, at : at + 1, :] + halo
            diag[i, at : at + 1, :] = diag[i, at : at + 1, :] + halo
            for comp in range(3):
                near = v0[comp, i + 1, row : row + 1, :]
                early[comp, i, at : at + 1, :] = early[comp, i, at : at + 1, :] + halo * near
        return carry

    lax.fori_loop(0, cx, late_one, 0, unroll=UNROLL)

    def edges_one(i):
        return [edge_of(merged1, i)] + [edge_of(merged0, comp * cx + i) for comp in range(3)]

    def values_one(i, edges):
        halo = jnp.where(end_lane, edges[0], 0.0)
        total = diag[i] + halo
        scale = RELAXATION / total
        diag[i] = total
        weight[i] = scale
        z_faces[i] = jnp.where(end_lane, visc[i + 1, rows, :] + halo, 0.0)
        for comp in range(3):
            flow = early[comp, i] + halo * edges[1 + comp]
            value = (1.0 - RELAXATION) * v0[comp, i + 1, rows, :] + scale * flow
            v1[comp, i + 1, rows, :] = value
            keep_end(2, comp, i, value)
            yield value

    def send_ends(r):
        s = r - 2
        return lambda: send_x(r, x_send.at[s, 0], x_recv.at[s, 0], x_send.at[s, 1], x_recv.at[s, 1])

    def keep_end(r, comp, i, value):
        if i == cx - 1:
            x_send[r - 2, 0, comp] = value
        if i == 0:
            x_send[r - 2, 1, comp] = value

    waits = shell_pass(edges_one, values_one, 2, send_ends(2))

    wait_gx()
    low_y, high_y = flag(has_down[1]), flag(has_up[1])
    gx_counts = (cx // 2, cx // 4, cx // 8)
    for level, buf in enumerate((cx1, cx2, cx3)):
        buf[1, rows, :] = buf[1, rows, :] + gx_recv[0, level]
        last = gx_counts[level]
        buf[last, rows, :] = buf[last, rows, :] + gx_recv[1, level]

    def restrict_rows(source, target, count):
        size = count + 2
        a, b, c, d = (source[pl.ds(PAD - 3 + s, size, stride=2), :] for s in range(4))
        target[PAD - 1 : PAD - 1 + size, :] = 0.125 * (a + d) + 0.375 * (b + c)
        target[PAD - 1 : PAD, :] = target[PAD - 1 : PAD, :] * low_y
        target[PAD + count : PAD + count + 1, :] = target[PAD + count : PAD + count + 1, :] * high_y

    row = 0
    ghost_rows = []
    for level, (buf, steps) in enumerate(((cx1, (t1,)), (cx2, (t2a, t2b)), (cx3, (t3a, t3b, t3c)))):
        for k in range(gx_counts[level]):
            source = buf.at[k + 1]
            for depth, target in enumerate(steps):
                restrict_rows(source, target.at[k], cy >> (depth + 1))
                source = target.at[k]
            count = cy >> len(steps)
            gy_send[1, row : row + 1, :] = source[PAD - 1 : PAD, :]
            gy_send[0, row : row + 1, :] = source[PAD + count : PAD + count + 1, :]
            ghost_rows.append((steps[-1], k, count, row))
            row += 1
    wait_gy = exchange(13, 1, gy_send.at[0], gy_recv.at[0], gy_send.at[1], gy_recv.at[1])

    def around_inner(buf, comp, i):
        plane = buf.at[comp, i + 1]
        centre = plane[rows, :]
        return centre, (
            buf[comp, i, rows, :],
            buf[comp, i + 2, rows, :],
            plane[PAD - 1 : PAD - 1 + cy, :],
            plane[PAD + 1 : PAD + 1 + cy, :],
            pltpu.roll(centre, 1, 1),
            pltpu.roll(centre, cz - 1, 1),
        )

    def flow_inner(buf, comp, i):
        centre, near = around_inner(buf, comp, i)
        flow = 2.0 * forc[comp, i]
        for n in range(6):
            flow = flow + faces[n, i] * near[n]
        return centre, flow

    def early_two(i, carry):
        z_scaled[i] = weight[i] * z_faces[i]
        for comp in range(3):
            centre, flow = flow_inner(v1, comp, i)
            early[comp, i] = (1.0 - RELAXATION) * centre + weight[i] * flow
        return carry

    def late_ends(r, scaled):
        for side, i, face in ((0, 0, 0), (1, cx - 1, 1)):
            factor = faces[face, i]
            if scaled:
                factor = factor * weight[i]
            for comp in range(3):
                early[comp, i] = early[comp, i] + factor * x_recv[r - 2, side, comp]

        def body(i, carry):
            for side, face, at in ((0, 2, 0), (1, 3, cy - 1)):
                factor = faces[face, i, at : at + 1, :]
                if scaled:
                    factor = factor * weight[i, at : at + 1, :]
                for comp in range(3):
                    halo = y_recv[r, side, comp, pl.ds(i, 1), :]
                    early[comp, i, at : at + 1, :] = early[comp, i, at : at + 1, :] + factor * halo
            return carry

        lax.fori_loop(0, cx, body, 0, unroll=UNROLL)

    lax.fori_loop(0, cx, early_two, 0, unroll=UNROLL)
    for wait in waits:
        wait()
    merged2 = merged_z(2)
    late_ends(2, True)

    def edges_two(i):
        return [edge_of(merged2, comp * cx + i) for comp in range(3)]

    def values_two(i, edges):
        factor = z_scaled[i]
        for comp in range(3):
            value = early[comp, i] + factor * edges[comp]
            v2[comp, i + 1, rows, :] = value
            keep_end(3, comp, i, value)
            yield value

    waits = shell_pass(edges_two, values_two, 3, send_ends(3))

    wait_gy()
    for buf, k, count, row in ghost_rows:
        buf[k, PAD : PAD + 1, :] = buf[k, PAD : PAD + 1, :] + gy_recv[0, row : row + 1, :]
        last = PAD + count - 1
        buf[k, last : last + 1, :] = buf[k, last : last + 1, :] + gy_recv[1, row : row + 1, :]
    mats_in.wait()
    off_low, off_high = 1.0 - flag(has_down[2]), 1.0 - flag(has_up[2])
    results = []
    groups = []
    lane8 = lax.broadcasted_iota(jnp.int32, (8, cz), 1)
    packed = jnp.zeros((8, cz), jnp.float32)
    for level, buf in enumerate((t1, t2b, t3c)):
        count = gx_counts[level]
        height = max(8, cy >> (level + 1))
        matrix = mats[0, level] - off_low * mats[1, level] - off_high * mats[2, level]
        data = buf[:, PAD : PAD + height, :].reshape(count * height, cz)
        result = jnp.dot(data, matrix, preferred_element_type=jnp.float32, precision=HIGHEST)
        for part in range(count * height // 8):
            g = len(groups)
            piece = result[8 * part : 8 * part + 8, :]
            groups.append((level, 8 * part // height, 8 * part % height, piece))
            shifted = pltpu.roll(piece, (2 * g - GHOST) % cz, 1)
            packed = jnp.where((lane8 == 2 * g) | (lane8 == 2 * g + 1), shifted, packed)
    gz_send[...] = packed
    wait_gz = exchange(14, 2, gz_send, gz_recv.at[0], gz_send, gz_recv.at[1])

    def early_misfit(i, carry):
        for comp in range(3):
            centre, flow = flow_inner(v2, comp, i)
            smooth_ref[comp, i] = centre
            early[comp, i] = flow - diag[i] * centre
        return carry

    lax.fori_loop(0, cx, early_misfit, 0, unroll=UNROLL)
    for wait in waits:
        wait()
    merged3 = merged_z(3)
    late_ends(3, False)
    squares = []

    def edges_three(i):
        return [edge_of(merged3, comp * cx + i) for comp in range(3)]

    def values_three(i, edges):
        total = None
        for comp in range(3):
            value = 0.5 * (early[comp, i] + z_faces[i] * edges[comp])
            misfit_ref[comp, i] = value
            total = value * value if total is None else total + value * value
            yield value
        squares.append(total if not squares else squares[-1] + total)

    shell_pass(edges_three, values_three, None, None)
    part = jnp.sum(squares[-1], axis=0, keepdims=True)

    def gather(slots, mine, value, peers, sends, recvs):
        slots[mine] = value
        copies = []
        for k, peer in enumerate(peers):
            copy = pltpu.make_async_remote_copy(
                slots.at[mine], slots.at[mine], sends.at[k], recvs.at[k],
                device_id=peer, device_id_type=MESH,
            )
            copy.start()
            copies.append(copy)
        return copies

    def total_of(slots):
        parts = [slots[n] for n in range(slots.shape[0])]
        while len(parts) > 1:
            parts = [sum(parts[n : n + 2]) for n in range(0, len(parts), 2)]
        return parts[0]

    plane_copies = gather(sums_xy, me_first, part, plane_peers, plane_send, plane_recv)

    wait_gz()
    low_part, high_part = gz_recv[0], gz_recv[1]
    for g, (level, k, at, piece) in enumerate(groups):
        width = cz >> (level + 1)
        height = cy >> (level + 1)
        piece = piece + jnp.where(lane8 == 0, pltpu.roll(low_part, (cz - 2 * g - 1) % cz, 1), 0.0)
        piece = piece + jnp.where(
            lane8 == width - 1, pltpu.roll(high_part, (width - 1 - 2 * g) % cz, 1), 0.0
        )
        target = (one_ref, two_ref, three_ref)[level]
        size = min(8, height - at)
        target[k, at : at + size, :] = piece[:size, :width]

    for condition, copy in started:
        pl.when(condition)(copy.wait_send)
    for copy in plane_copies:
        copy.wait()
    whole = total_of(sums_xy)
    if not one_stage:
        line_copies = gather(sums_z, iz, whole, line_peers, line_send, line_recv)
        for copy in line_copies:
            copy.wait()
        whole = total_of(sums_z)
    whole = jnp.sum(whole, axis=1, keepdims=True)
    cells_all = float(3 * cx * nx * cy * ny * cz * nz)
    rms_ref[...] = jnp.sqrt(whole / cells_all)


def writer(*refs):
    copies = [
        pltpu.make_async_copy(refs[n], refs[7 + n], refs[14].at[n]) for n in (0, 5, 1, 2, 3, 4, 6)
    ]
    for copy in copies:
        copy.start()
    for copy in copies:
        copy.wait()


def per_device(velocity, forcing, phase_block, prefactor, yield_stress):
    _, cx, cy, cz = velocity.shape
    nx, ny, nz = lax.axis_size("gx"), lax.axis_size("gy"), lax.axis_size("gz")
    f32 = jnp.float32
    sizes = (nx, ny, nz, cx, cy, cz, prefactor.shape[0])
    mats = jnp.asarray(coarse_matrices(cz))
    blocks = phase_block.reshape(phase_block.shape[0] * phase_block.shape[1], phase_block.shape[2])
    tall = cy + 2 * PAD
    firsts = nx * ny * nz if nx * ny * nz <= ONE_STAGE else nx * ny
    ghosts = cx // 2 + cx // 4 + cx // 8
    ghosts += -ghosts % 8
    hbm = pl.BlockSpec(memory_space=pltpu.HBM)
    vmem = pl.BlockSpec(memory_space=pltpu.VMEM)
    v = pltpu.VMEM
    field = v((3, cx + 2, tall, cz), f32)
    dma = pltpu.SemaphoreType.DMA
    operands = (velocity, forcing, mats, blocks, prefactor, yield_stress)
    outs = pl.pallas_call(
        functools.partial(kernel, sizes),
        out_shape=(
            jax.ShapeDtypeStruct(velocity.shape, f32),
            jax.ShapeDtypeStruct((cx, cy, cz), f32),
            jax.ShapeDtypeStruct((cx // 2, cy // 2, cz // 2), f32),
            jax.ShapeDtypeStruct((cx // 4, cy // 4, cz // 4), f32),
            jax.ShapeDtypeStruct((cx // 8, cy // 8, cz // 8), f32),
            jax.ShapeDtypeStruct(velocity.shape, f32),
            jax.ShapeDtypeStruct((1, 1), f32),
        ),
        in_specs=[hbm] * 6,
        out_specs=(vmem,) * 7,
        scratch_shapes=[
            field,
            field,
            field,
            v((cx + 2, tall, cz), f32),
            v((3, cx, cy, cz), f32),
            v(mats.shape, f32),
            v(blocks.shape, blocks.dtype),
            pltpu.SMEM(prefactor.shape, f32),
            pltpu.SMEM(yield_stress.shape, f32),
            v((6, cx, cy, cz), f32),
            v((cx, cy, cz), f32),
            v((cx, cy, cz), f32),
            v((3, cx, cy, cz), f32),
            v((cx, cy, cz), f32),
            v((cx, cy, cz), f32),
            v((cx // BLOCK, cy, cz), f32),
            v((cx // BLOCK, cy, cz), f32),
            v((2, 2, 3, cy, cz), f32),
            v((2, 2, 3, cy, cz), f32),
            v((2, cy, cz), f32),
            v((4, 2, 3, cx, cz), f32),
            v((4, 2, 3, cx, cz), f32),
            v((4, cy, cz), f32),
            v((4, 2, cy, cz), f32),
            v((cx // 2 + 2, tall, cz), f32),
            v((cx // 4 + 2, tall, cz), f32),
            v((cx // 8 + 2, tall, cz), f32),
            v((2, 3, cy, cz), f32),
            v((2, 3, cy, cz), f32),
            v((cx // 2, tall, cz), f32),
            v((cx // 4, tall, cz), f32),
            v((cx // 4, tall, cz), f32),
            v((cx // 8, tall, cz), f32),
            v((cx // 8, tall, cz), f32),
            v((cx // 8, tall, cz), f32),
            v((2, ghosts, cz), f32),
            v((2, ghosts, cz), f32),
            v((8, cz), f32),
            v((2, 8, cz), f32),
            v((firsts, 1, cz), f32),
            v((nz, 1, cz), f32),
            dma((6,)),
            dma((15, 2)),
            dma((15, 2)),
            dma((firsts - 1,)),
            dma((firsts - 1,)),
            dma((nz - 1,)),
            dma((nz - 1,)),
        ],
        compiler_params=pltpu.CompilerParams(
            collective_id=0, has_side_effects=True, vmem_limit_bytes=40 * 1024 * 1024
        ),
    )(*(pltpu.with_memory_space_constraint(a, pltpu.HBM) for a in operands))
    outs = pl.pallas_call(
        writer,
        out_shape=tuple(jax.ShapeDtypeStruct(out.shape, f32) for out in outs),
        in_specs=[vmem] * 7,
        out_specs=(hbm,) * 7,
        scratch_shapes=[dma((7,))],
        compiler_params=pltpu.CompilerParams(vmem_limit_bytes=8 * 1024 * 1024),
    )(*outs)
    return outs[:6] + (outs[6].reshape(()),)


def solution(mesh):
    grid = P("gx", "gy", "gz")
    vector = P(None, "gx", "gy", "gz")
    return jax.shard_map(
        per_device,
        mesh=mesh,
        in_specs=(vector, vector, grid, P(), P()),
        out_specs=(vector, grid, grid, grid, grid, vector, P()),
        check_vma=False,
    )
```

```python
import functools

import jax
import jax.numpy as jnp
import numpy as np
from jax import lax
from jax.experimental import pallas as pl
from jax.experimental.pallas import tpu as pltpu
from jax.sharding import PartitionSpec as P

BLOCK = 4
RELAXATION = 0.8
PAD = 8
GHOST = 64
UNROLL = 4
STAGES = (2, 0, 2)
STAGES_VISC = (2, 2, 2)
ONE_STAGE = 32
ROUNDS = 4
MESH = pl.DeviceIdType.MESH
HIGHEST = lax.Precision.HIGHEST


def coarse_matrices(length):
    def chain(low_edge, high_edge):
        field = np.eye(length)
        found = []
        first = 0
        for _ in range(3):
            count = length >> (len(found) + 1)
            out = np.zeros((length, count + 2))
            for k in range(-1, count + 1):
                for shift, weight in ((-1, 1.0), (0, 3.0), (1, 3.0), (2, 1.0)):
                    source = 2 * k + shift - first
                    if 0 <= source < field.shape[1]:
                        out[:, k + 1] += weight / 8.0 * field[:, source]
            if low_edge:
                out[:, 0] = 0.0
            if high_edge:
                out[:, -1] = 0.0
            placed = np.zeros((length, length))
            placed[:, :count] = out[:, 1:-1]
            placed[:, GHOST] = out[:, 0]
            placed[:, GHOST + 1] = out[:, -1]
            found.append(placed)
            field = out
            first = -1
        return np.stack(found)

    inner = chain(False, False)
    return np.stack([inner, inner - chain(True, False), inner - chain(False, True)]).astype(np.float32)


def kernel(
    sizes,
    vel_hbm,
    forc_hbm,
    mats_hbm,
    phase_hbm,
    pref_hbm,
    yield_hbm,
    smooth_ref,
    visc_ref,
    one_ref,
    two_ref,
    three_ref,
    misfit_ref,
    rms_ref,
    v0,
    v1,
    v2,
    visc,
    forc,
    mats,
    phase_ref,
    pref_ref,
    yield_ref,
    faces,
    z_faces,
    z_scaled,
    early,
    weight,
    diag,
    pref_cells,
    yield_cells,
    x_send,
    x_recv,
    visc_x,
    y_send,
    y_recv,
    z_send,
    z_recv,
    cx1,
    cx2,
    cx3,
    gx_send,
    gx_recv,
    t1,
    t2a,
    t2b,
    t3a,
    t3b,
    t3c,
    gy_send,
    gy_recv,
    gz_send,
    gz_recv,
    sums_xy,
    sums_z,
    local_sem,
    send_sem,
    recv_sem,
    plane_sem,
    line_sem,
):
    nx, ny, nz, cx, cy, cz, phases = sizes
    ix, iy, iz = lax.axis_index("gx"), lax.axis_index("gy"), lax.axis_index("gz")
    rows = pl.ds(PAD, cy)

    ends_in = [
        pltpu.make_async_copy(vel_hbm.at[:, cx - 1], x_send.at[0, 0], local_sem.at[0]),
        pltpu.make_async_copy(vel_hbm.at[:, 0], x_send.at[0, 1], local_sem.at[1]),
    ]
    vel_in = [
        pltpu.make_async_copy(vel_hbm.at[comp], v0.at[comp, pl.ds(1, cx), rows, :], local_sem.at[2 + comp])
        for comp in range(3)
    ]
    forc_in = pltpu.make_async_copy(forc_hbm, forc, local_sem.at[5])
    mats_in = pltpu.make_async_copy(mats_hbm, mats, local_sem.at[6])
    phase_in = pltpu.make_async_copy(phase_hbm, phase_ref, local_sem.at[7])
    pref_in = pltpu.make_async_copy(pref_hbm, pref_ref, local_sem.at[8])
    yield_in = pltpu.make_async_copy(yield_hbm, yield_ref, local_sem.at[9])
    for copy in ends_in + vel_in:
        copy.start()

    barrier = pltpu.get_barrier_semaphore()
    one_stage = nx * ny * nz <= ONE_STAGE
    me_xy = ix * ny + iy
    me_first = me_xy * nz + iz if one_stage else me_xy

    def first_peers():
        if one_stage:
            others = [lax.rem(me_first + k, nx * ny * nz) for k in range(1, nx * ny * nz)]
            return [(o // (ny * nz), lax.rem(o // nz, ny), lax.rem(o, nz)) for o in others]
        others = [lax.rem(me_first + k, nx * ny) for k in range(1, nx * ny)]
        return [(o // ny, lax.rem(o, ny), iz) for o in others]

    line_peers = [] if one_stage else [(ix, iy, lax.rem(iz + k, nz)) for k in range(1, nz)]
    steps = [nx - 1, ny - 1, nz - 1] if one_stage else [nx - 1, ny - 1]
    if sum(steps) - max(steps) <= ROUNDS:
        greeted = [(lax.rem(ix + k, nx), iy, iz) for k in range(1, nx)]
        greeted += [(ix, lax.rem(iy + k, ny), iz) for k in range(1, ny)]
        greeted += [(ix, iy, lax.rem(iz + k, nz)) for k in range(1, nz)]
    else:
        greeted = first_peers() + line_peers
    for peer in greeted:
        pl.semaphore_signal(barrier, inc=1, device_id=peer, device_id_type=MESH)
    for copy in (phase_in, pref_in, yield_in):
        copy.start()

    has_up = (ix < nx - 1, iy < ny - 1, iz < nz - 1)
    has_down = (ix > 0, iy > 0, iz > 0)

    def clear(ref):
        ref[...] = jnp.zeros(ref.shape, jnp.float32)

    for side, present in ((0, has_down), (1, has_up)):
        @pl.when(jnp.logical_not(present[0]))
        def _():
            for r in range(3):
                clear(x_recv.at[r, side])
            clear(visc_x.at[side])
            clear(gx_recv.at[side])

        @pl.when(jnp.logical_not(present[1]))
        def _():
            for r in range(4):
                clear(y_recv.at[r, side])
            clear(gy_recv.at[side])

        @pl.when(jnp.logical_not(present[2]))
        def _():
            for r in range(4):
                clear(z_recv.at[r, side])
            clear(gz_recv.at[side])

    for buf in [v.at[comp] for v in (v0, v1, v2) for comp in range(3)] + [visc]:
        clear(buf.at[0, rows])
        clear(buf.at[cx + 1, rows])
        clear(buf.at[pl.ds(1, cx), pl.ds(PAD - 1, 1)])
        clear(buf.at[pl.ds(1, cx), pl.ds(PAD + cy, 1)])

    lane = lax.broadcasted_iota(jnp.int32, (cy, cz), 1)
    odd_lane = lax.rem(lane, 2) == 1
    lane_pair = (lane - 1) // 2
    first_lane = lane == 0
    last_lane = lane == cz - 1
    end_lane = first_lane | last_lane

    up_ids = (
        (lax.rem(ix + 1, nx), iy, iz),
        (ix, lax.rem(iy + 1, ny), iz),
        (ix, iy, lax.rem(iz + 1, nz)),
    )
    down_ids = (
        (lax.rem(ix + nx - 1, nx), iy, iz),
        (ix, lax.rem(iy + ny - 1, ny), iz),
        (ix, iy, lax.rem(iz + nz - 1, nz)),
    )
    started = []

    def exchange(slot, dim, up_src, up_dst, down_src, down_dst):
        up = pltpu.make_async_remote_copy(
            up_src, up_dst, send_sem.at[slot, 0], recv_sem.at[slot, 0],
            device_id=up_ids[dim], device_id_type=MESH,
        )
        down = pltpu.make_async_remote_copy(
            down_src, down_dst, send_sem.at[slot, 1], recv_sem.at[slot, 1],
            device_id=down_ids[dim], device_id_type=MESH,
        )
        pl.when(has_up[dim])(up.start)
        pl.when(has_down[dim])(down.start)
        started.append((has_up[dim], up))
        started.append((has_down[dim], down))

        def wait():
            pl.when(has_down[dim])(up.wait_recv)
            pl.when(has_up[dim])(down.wait_recv)

        return wait

    def send_x(r, last, low, first, high):
        return exchange(3 * r, 0, last, low, first, high)

    def send_yz(r):
        held = pl.ds(0, 1 if r == 1 else 3)
        return [
            exchange(
                3 * r + 1, 1,
                y_send.at[r, 0, held], y_recv.at[r, 0, held],
                y_send.at[r, 1, held], y_recv.at[r, 1, held],
            ),
            exchange(3 * r + 2, 2, z_send.at[r], z_recv.at[r, 0], z_send.at[r], z_recv.at[r, 1]),
        ]

    def pack(r, comp, i, value, packed):
        y_send[r, 0, comp, pl.ds(i, 1), :] = value[cy - 1 : cy, :]
        y_send[r, 1, comp, pl.ds(i, 1), :] = value[0:1, :]
        place = 2 * (comp * cx + i) + 1
        return jnp.where(lane_pair == comp * cx + i, pltpu.roll(value, place + 1, 1), packed)

    def unpack_y(r, buf, comps):
        def body(i, carry):
            for comp in range(comps):
                target = buf.at[comp, i + 1] if comps == 3 else buf.at[i + 1]
                target[PAD - 1 : PAD, :] = y_recv[r, 0, comp, pl.ds(i, 1), :]
                target[PAD + cy : PAD + cy + 1, :] = y_recv[r, 1, comp, pl.ds(i, 1), :]
            return carry

        lax.fori_loop(0, cx, body, 0)

    def merged_z(r):
        return jnp.where(odd_lane, z_recv[r, 0], pltpu.roll(z_recv[r, 1], cz - 2, 1))

    def along(plane_ref, centre, merged, place):
        edge = pltpu.roll(merged, cz - 1 - 2 * place, 1)
        return (
            plane_ref[PAD - 1 : PAD - 1 + cy, :],
            plane_ref[PAD + 1 : PAD + 1 + cy, :],
            jnp.where(first_lane, edge, pltpu.roll(centre, 1, 1)),
            jnp.where(last_lane, edge, pltpu.roll(centre, cz - 1, 1)),
        )

    def around(buf, comp, i, merged):
        centre = buf[comp, i + 1, rows, :]
        ym, yp, zm, zp = along(buf.at[comp, i + 1], centre, merged, comp * cx + i)
        return centre, (buf[comp, i, rows, :], buf[comp, i + 2, rows, :], ym, yp, zm, zp)

    for copy in ends_in:
        copy.wait()
    pl.semaphore_wait(barrier, len(greeted))
    waits = [send_x(0, x_send.at[0, 0], x_recv.at[0, 0], x_send.at[0, 1], x_recv.at[0, 1])]
    nothing = jnp.zeros((cy, cz), jnp.float32)
    packed = nothing
    for comp in range(3):
        vel_in[comp].wait()
        for i in range(cx):
            packed = pack(0, comp, i, v0[comp, i + 1, rows, :], packed)
    z_send[0] = packed
    waits += send_yz(0)
    forc_in.start()
    mats_in.start()

    phase_in.wait()
    pref_in.wait()
    yield_in.wait()
    blocks = phase_ref[...].astype(jnp.float32)
    n_rows, n_blocks = blocks.shape
    spread_z = lax.broadcasted_iota(jnp.int32, (n_blocks, cz), 1) // BLOCK
    spread_z = (spread_z == lax.broadcasted_iota(jnp.int32, (n_blocks, cz), 0)).astype(jnp.float32)
    spread_y = lax.broadcasted_iota(jnp.int32, (n_rows * BLOCK, n_rows), 0) // BLOCK
    spread_y = (
        spread_y == lax.broadcasted_iota(jnp.int32, (n_rows * BLOCK, n_rows), 1)
    ).astype(jnp.float32)
    cells = jnp.dot(blocks, spread_z, preferred_element_type=jnp.float32, precision=HIGHEST)
    cells = jnp.dot(spread_y, cells, preferred_element_type=jnp.float32, precision=HIGHEST)
    for bx in range(cx // BLOCK):
        phase = cells[bx * cy : (bx + 1) * cy, :]
        pref_value = jnp.zeros((cy, cz), jnp.float32)
        yield_value = jnp.zeros((cy, cz), jnp.float32)
        for p in range(phases):
            here = jnp.abs(phase - float(p)) < 0.5
            pref_value = jnp.where(here, pref_ref[p], pref_value)
            yield_value = jnp.where(here, yield_ref[p], yield_value)
        pref_cells[bx] = pref_value
        yield_cells[bx] = 0.5 * yield_value
    for buf in (cx1, cx2, cx3):
        for edge in (0, PAD + cy):
            buf[:, edge : edge + PAD, :] = jnp.zeros((buf.shape[0], PAD, cz), jnp.float32)
    for buf in (t1, t2a, t2b, t3a, t3b, t3c):
        buf[...] = jnp.zeros(buf.shape, jnp.float32)

    along_x, along_y, along_z = (0, 3, 4), (3, 1, 5), (4, 5, 2)

    def early_strain(i, carry):
        found = {}
        for comp in range(3):
            plane = v0.at[comp, i + 1]
            centre = plane[rows, :]
            low = jnp.where(first_lane, 0.0, pltpu.roll(centre, 1, 1))
            high = jnp.where(last_lane, 0.0, pltpu.roll(centre, cz - 1, 1))
            for n, jump in (
                (along_x[comp], v0[comp, i + 2, rows, :] - v0[comp, i, rows, :]),
                (along_y[comp], plane[PAD + 1 : PAD + 1 + cy, :] - plane[PAD - 1 : PAD - 1 + cy, :]),
                (along_z[comp], high - low),
            ):
                found[n] = found[n] + jump if n in found else jump
        for n in range(6):
            faces[n, i] = found[n]
        return carry

    lax.fori_loop(0, cx, early_strain, 0, unroll=UNROLL)
    for wait in waits:
        wait()
    merged0 = merged_z(0)
    signed0 = jnp.where(odd_lane, -merged0, merged0)
    for comp in range(3):
        n = along_x[comp]
        faces[n, 0] = faces[n, 0] - x_recv[0, 0, comp]
        faces[n, cx - 1] = faces[n, cx - 1] + x_recv[0, 1, comp]

    def late_strain(i, carry):
        for comp in range(3):
            n = along_y[comp]
            faces[n, i, 0:1, :] = faces[n, i, 0:1, :] - y_recv[0, 0, comp, pl.ds(i, 1), :]
            faces[n, i, cy - 1 : cy, :] = faces[n, i, cy - 1 : cy, :] + y_recv[0, 1, comp, pl.ds(i, 1), :]
        return carry

    lax.fori_loop(0, cx, late_strain, 0, unroll=UNROLL)

    order = [0, cx - 1] + list(range(1, cx - 1))

    def shell_pass(edge, value_of, r, send_ends, stages):
        ahead, hold, behind = stages
        packed = nothing
        edges, values, rolled = {}, {}, {}
        sent = None
        for t in range(cx + ahead + hold + behind):
            if t < cx:
                edges[t] = edge(order[t])
            n = t - ahead
            if 0 <= n < cx:
                i = order[n]
                values[n] = []
                for comp, value in enumerate(value_of(i, edges.pop(n))):
                    if r is not None:
                        y_send[r, 0, comp, pl.ds(i, 1), :] = value[cy - 1 : cy, :]
                        y_send[r, 1, comp, pl.ds(i, 1), :] = value[0:1, :]
                        values[n].append((comp * cx + i, value))
                if n == 1 and send_ends is not None:
                    sent = send_ends()
            n = t - ahead - hold
            if 0 <= n < cx:
                rolled[n] = [(place, pltpu.roll(value, 2 * place + 2, 1)) for place, value in values.pop(n)]
            n = t - ahead - hold - behind
            if 0 <= n < cx:
                for place, value in rolled.pop(n):
                    packed = jnp.where(lane_pair == place, value, packed)
        if r is None:
            return None
        z_send[r] = packed
        return [sent] + send_yz(r)

    def edge_of(merged, place):
        return pltpu.roll(merged, cz - 1 - 2 * place, 1)

    def edges_visc(i):
        return [edge_of(signed0, comp * cx + i) for comp in range(3)]

    def values_visc(i, edges):
        strain = [faces[n, i] for n in range(6)]
        for comp in range(3):
            n = along_z[comp]
            strain[n] = strain[n] + jnp.where(end_lane, edges[comp], 0.0)
        squared = [term * term for term in strain]
        straight = squared[0] + squared[1] + squared[2]
        skew = squared[3] + squared[4] + squared[5]
        invariant = 1.0 + (0.125 * straight + 0.0625 * skew)
        creeping = pref_cells[i // BLOCK] * jnp.exp(jnp.log(invariant) * (-1.0 / 3.0))
        plastic = yield_cells[i // BLOCK] * lax.rsqrt(invariant)
        value = jnp.minimum(creeping, plastic)
        visc[i + 1, rows, :] = value
        yield value

    def send_visc():
        return send_x(1, visc.at[cx, rows, :], visc_x.at[0], visc.at[1, rows, :], visc_x.at[1])

    waits = shell_pass(edges_visc, values_visc, 1, send_visc, STAGES_VISC)
    for comp in range(3):
        v0[comp, 0, rows, :] = x_recv[0, 0, comp]
        v0[comp, cx + 1, rows, :] = x_recv[0, 1, comp]
    unpack_y(0, v0, 3)

    def flag(condition):
        return jnp.where(condition, 1.0, 0.0).astype(jnp.float32)

    def restrict_planes(source, first, held, count, target, level):
        for k in range(-1, count + 1):
            total = None
            for shift, factor in ((-1, 0.125), (0, 0.375), (1, 0.375), (2, 0.125)):
                at = 2 * k + shift - first
                if 0 <= at < held:
                    term = factor * source[at, rows, :]
                    total = term if total is None else total + term
            if k == -1:
                total = total * flag(has_down[0])
                gx_send[1, level] = total
            if k == count:
                total = total * flag(has_up[0])
                gx_send[0, level] = total
            target[k + 1, rows, :] = total

    restrict_planes(visc.at[pl.ds(1, cx)], 0, cx, cx // 2, cx1, 0)
    restrict_planes(cx1, -1, cx // 2 + 2, cx // 4, cx2, 1)
    restrict_planes(cx2, -1, cx // 4 + 2, cx // 8, cx3, 2)
    wait_gx = exchange(12, 0, gx_send.at[0], gx_recv.at[0], gx_send.at[1], gx_recv.at[1])

    forc_in.wait()

    def early_one(i, carry):
        plane = visc.at[i + 1]
        centre = plane[rows, :]
        visc_ref[i] = centre
        sides = (
            centre + visc[i, rows, :],
            centre + visc[i + 2, rows, :],
            centre + plane[PAD - 1 : PAD - 1 + cy, :],
            centre + plane[PAD + 1 : PAD + 1 + cy, :],
            centre + jnp.where(first_lane, 0.0, pltpu.roll(centre, 1, 1)),
            centre + jnp.where(last_lane, 0.0, pltpu.roll(centre, cz - 1, 1)),
        )
        for n in range(4):
            faces[n, i] = sides[n]
        faces[4, i] = jnp.where(first_lane, 0.0, sides[4])
        faces[5, i] = jnp.where(last_lane, 0.0, sides[5])
        diag[i] = (sides[0] + sides[1]) + (sides[2] + sides[3]) + (sides[4] + sides[5])
        for comp in range(3):
            _, near = around(v0, comp, i, merged0)
            flow = 2.0 * forc[comp, i]
            for n in range(6):
                flow = flow + sides[n] * near[n]
            early[comp, i] = flow
        return carry

    lax.fori_loop(0, cx, early_one, 0, unroll=UNROLL)
    for wait in waits:
        wait()
    merged1 = merged_z(1)

    for side, i, face, halo_plane in ((0, 0, 0, 0), (1, cx - 1, 1, cx + 1)):
        halo = visc_x[side]
        faces[face, i] = faces[face, i] + halo
        diag[i] = diag[i] + halo
        for comp in range(3):
            early[comp, i] = early[comp, i] + halo * v0[comp, halo_plane, rows, :]

    def late_one(i, carry):
        ends = ((0, 2, 0, PAD - 1), (1, 3, cy - 1, PAD + cy))
        for side, face, at, row in ends:
            halo = y_recv[1, side, 0, pl.ds(i, 1), :]
            faces[face, i, at : at + 1, :] = faces[face, i, at : at + 1, :] + halo
            diag[i, at : at + 1, :] = diag[i, at : at + 1, :] + halo
            for comp in range(3):
                near = v0[comp, i + 1, row : row + 1, :]
                early[comp, i, at : at + 1, :] = early[comp, i, at : at + 1, :] + halo * near
        return carry

    lax.fori_loop(0, cx, late_one, 0, unroll=UNROLL)

    def edges_one(i):
        return [edge_of(merged1, i)] + [edge_of(merged0, comp * cx + i) for comp in range(3)]

    def values_one(i, edges):
        halo = jnp.where(end_lane, edges[0], 0.0)
        total = diag[i] + halo
        scale = RELAXATION / total
        diag[i] = total
        weight[i] = scale
        z_faces[i] = jnp.where(end_lane, visc[i + 1, rows, :] + halo, 0.0)
        for comp in range(3):
            flow = early[comp, i] + halo * edges[1 + comp]
            value = (1.0 - RELAXATION) * v0[comp, i + 1, rows, :] + scale * flow
            v1[comp, i + 1, rows, :] = value
            keep_end(2, comp, i, value)
            yield value

    def send_ends(r):
        s = r - 1
        return lambda: send_x(r, x_send.at[s, 0], x_recv.at[s, 0], x_send.at[s, 1], x_recv.at[s, 1])

    def keep_end(r, comp, i, value):
        if i == cx - 1:
            x_send[r - 1, 0, comp] = value
        if i == 0:
            x_send[r - 1, 1, comp] = value

    waits = shell_pass(edges_one, values_one, 2, send_ends(2), STAGES)

    wait_gx()
    low_y, high_y = flag(has_down[1]), flag(has_up[1])
    gx_counts = (cx // 2, cx // 4, cx // 8)
    for level, buf in enumerate((cx1, cx2, cx3)):
        buf[1, rows, :] = buf[1, rows, :] + gx_recv[0, level]
        last = gx_counts[level]
        buf[last, rows, :] = buf[last, rows, :] + gx_recv[1, level]

    def restrict_rows(source, target, count):
        size = count + 2
        a, b, c, d = (source[pl.ds(PAD - 3 + s, size, stride=2), :] for s in range(4))
        target[PAD - 1 : PAD - 1 + size, :] = 0.125 * (a + d) + 0.375 * (b + c)
        target[PAD - 1 : PAD, :] = target[PAD - 1 : PAD, :] * low_y
        target[PAD + count : PAD + count + 1, :] = target[PAD + count : PAD + count + 1, :] * high_y

    row = 0
    ghost_rows = []
    for level, (buf, steps) in enumerate(((cx1, (t1,)), (cx2, (t2a, t2b)), (cx3, (t3a, t3b, t3c)))):
        for k in range(gx_counts[level]):
            source = buf.at[k + 1]
            for depth, target in enumerate(steps):
                restrict_rows(source, target.at[k], cy >> (depth + 1))
                source = target.at[k]
            count = cy >> len(steps)
            gy_send[1, row : row + 1, :] = source[PAD - 1 : PAD, :]
            gy_send[0, row : row + 1, :] = source[PAD + count : PAD + count + 1, :]
            ghost_rows.append((steps[-1], k, count, row))
            row += 1
    wait_gy = exchange(13, 1, gy_send.at[0], gy_recv.at[0], gy_send.at[1], gy_recv.at[1])

    def around_inner(buf, comp, i):
        plane = buf.at[comp, i + 1]
        centre = plane[rows, :]
        return centre, (
            buf[comp, i, rows, :],
            buf[comp, i + 2, rows, :],
            plane[PAD - 1 : PAD - 1 + cy, :],
            plane[PAD + 1 : PAD + 1 + cy, :],
            pltpu.roll(centre, 1, 1),
            pltpu.roll(centre, cz - 1, 1),
        )

    def flow_inner(buf, comp, i):
        centre, near = around_inner(buf, comp, i)
        flow = 2.0 * forc[comp, i]
        for n in range(6):
            flow = flow + faces[n, i] * near[n]
        return centre, flow

    def early_two(i, carry):
        z_scaled[i] = weight[i] * z_faces[i]
        for comp in range(3):
            centre, flow = flow_inner(v1, comp, i)
            early[comp, i] = (1.0 - RELAXATION) * centre + weight[i] * flow
        return carry

    def late_ends(r, scaled):
        for side, i, face in ((0, 0, 0), (1, cx - 1, 1)):
            factor = faces[face, i]
            if scaled:
                factor = factor * weight[i]
            for comp in range(3):
                early[comp, i] = early[comp, i] + factor * x_recv[r - 1, side, comp]

        def body(i, carry):
            for side, face, at in ((0, 2, 0), (1, 3, cy - 1)):
                factor = faces[face, i, at : at + 1, :]
                if scaled:
                    factor = factor * weight[i, at : at + 1, :]
                for comp in range(3):
                    halo = y_recv[r, side, comp, pl.ds(i, 1), :]
                    early[comp, i, at : at + 1, :] = early[comp, i, at : at + 1, :] + factor * halo
            return carry

        lax.fori_loop(0, cx, body, 0, unroll=UNROLL)

    lax.fori_loop(0, cx, early_two, 0, unroll=UNROLL)
    for wait in waits:
        wait()
    merged2 = merged_z(2)
    late_ends(2, True)

    def edges_two(i):
        return [edge_of(merged2, comp * cx + i) for comp in range(3)]

    def values_two(i, edges):
        factor = z_scaled[i]
        for comp in range(3):
            value = early[comp, i] + factor * edges[comp]
            v2[comp, i + 1, rows, :] = value
            keep_end(3, comp, i, value)
            yield value

    waits = shell_pass(edges_two, values_two, 3, send_ends(3), STAGES)

    wait_gy()
    for buf, k, count, row in ghost_rows:
        buf[k, PAD : PAD + 1, :] = buf[k, PAD : PAD + 1, :] + gy_recv[0, row : row + 1, :]
        last = PAD + count - 1
        buf[k, last : last + 1, :] = buf[k, last : last + 1, :] + gy_recv[1, row : row + 1, :]
    mats_in.wait()
    off_low, off_high = 1.0 - flag(has_down[2]), 1.0 - flag(has_up[2])
    results = []
    groups = []
    lane8 = lax.broadcasted_iota(jnp.int32, (8, cz), 1)
    packed = jnp.zeros((8, cz), jnp.float32)
    for level, buf in enumerate((t1, t2b, t3c)):
        count = gx_counts[level]
        height = max(8, cy >> (level + 1))
        matrix = mats[0, level] - off_low * mats[1, level] - off_high * mats[2, level]
        data = buf[:, PAD : PAD + height, :].reshape(count * height, cz)
        result = jnp.dot(data, matrix, preferred_element_type=jnp.float32, precision=HIGHEST)
        for part in range(count * height // 8):
            g = len(groups)
            piece = result[8 * part : 8 * part + 8, :]
            groups.append((level, 8 * part // height, 8 * part % height, piece))
            shifted = pltpu.roll(piece, (2 * g - GHOST) % cz, 1)
            packed = jnp.where((lane8 == 2 * g) | (lane8 == 2 * g + 1), shifted, packed)
    gz_send[...] = packed
    wait_gz = exchange(14, 2, gz_send, gz_recv.at[0], gz_send, gz_recv.at[1])

    def early_misfit(i, carry):
        for comp in range(3):
            centre, flow = flow_inner(v2, comp, i)
            smooth_ref[comp, i] = centre
            early[comp, i] = flow - diag[i] * centre
        return carry

    lax.fori_loop(0, cx, early_misfit, 0, unroll=UNROLL)
    for wait in waits:
        wait()
    merged3 = merged_z(3)
    late_ends(3, False)
    squares = []

    def edges_three(i):
        return [edge_of(merged3, comp * cx + i) for comp in range(3)]

    def values_three(i, edges):
        total = None
        for comp in range(3):
            value = 0.5 * (early[comp, i] + z_faces[i] * edges[comp])
            misfit_ref[comp, i] = value
            total = value * value if total is None else total + value * value
            yield value
        squares.append(total if not squares else squares[-1] + total)

    shell_pass(edges_three, values_three, None, None, STAGES)
    part = jnp.sum(squares[-1], axis=0, keepdims=True)

    def gather(slots, mine, value, peers, sems):
        slots[mine] = value
        for peer in peers:
            pltpu.make_async_remote_copy(
                slots.at[mine], slots.at[mine], sems.at[0], sems.at[1],
                device_id=peer, device_id_type=MESH,
            ).start()
        others = slots.at[pl.ds(0, len(peers))]
        return pltpu.make_async_remote_copy(
            others, others, sems.at[0], sems.at[1], device_id=peers[0], device_id_type=MESH
        )

    def total_of(slots):
        parts = [slots[n] for n in range(slots.shape[0])]
        while len(parts) > 1:
            parts = [sum(parts[n : n + 2]) for n in range(0, len(parts), 2)]
        return parts[0]

    plane_copies = gather(sums_xy, me_first, part, first_peers(), plane_sem)

    wait_gz()
    low_part, high_part = gz_recv[0], gz_recv[1]
    for g, (level, k, at, piece) in enumerate(groups):
        width = cz >> (level + 1)
        height = cy >> (level + 1)
        piece = piece + jnp.where(lane8 == 0, pltpu.roll(low_part, (cz - 2 * g - 1) % cz, 1), 0.0)
        piece = piece + jnp.where(
            lane8 == width - 1, pltpu.roll(high_part, (width - 1 - 2 * g) % cz, 1), 0.0
        )
        target = (one_ref, two_ref, three_ref)[level]
        size = min(8, height - at)
        target[k, at : at + size, :] = piece[:size, :width]

    for condition, copy in started:
        pl.when(condition)(copy.wait_send)
    plane_copies.wait()
    whole = total_of(sums_xy)
    if not one_stage:
        gather(sums_z, iz, whole, line_peers, line_sem).wait()
        whole = total_of(sums_z)
    whole = jnp.sum(whole, axis=1, keepdims=True)
    cells_all = float(3 * cx * nx * cy * ny * cz * nz)
    rms_ref[...] = jnp.sqrt(whole / cells_all)


def writer(*refs):
    copies = [
        pltpu.make_async_copy(refs[n], refs[7 + n], refs[14].at[n]) for n in (0, 5, 1, 2, 3, 4, 6)
    ]
    for copy in copies:
        copy.start()
    for copy in copies:
        copy.wait()


def per_device(velocity, forcing, phase_block, prefactor, yield_stress):
    _, cx, cy, cz = velocity.shape
    nx, ny, nz = lax.axis_size("gx"), lax.axis_size("gy"), lax.axis_size("gz")
    f32 = jnp.float32
    sizes = (nx, ny, nz, cx, cy, cz, prefactor.shape[0])
    mats = jnp.asarray(coarse_matrices(cz))
    blocks = phase_block.reshape(phase_block.shape[0] * phase_block.shape[1], phase_block.shape[2])
    tall = cy + 2 * PAD
    firsts = nx * ny * nz if nx * ny * nz <= ONE_STAGE else nx * ny
    ghosts = cx // 2 + cx // 4 + cx // 8
    ghosts += -ghosts % 8
    hbm = pl.BlockSpec(memory_space=pltpu.HBM)
    vmem = pl.BlockSpec(memory_space=pltpu.VMEM)
    v = pltpu.VMEM
    field = v((3, cx + 2, tall, cz), f32)
    dma = pltpu.SemaphoreType.DMA
    operands = (velocity, forcing, mats, blocks, prefactor, yield_stress)
    outs = pl.pallas_call(
        functools.partial(kernel, sizes),
        out_shape=(
            jax.ShapeDtypeStruct(velocity.shape, f32),
            jax.ShapeDtypeStruct((cx, cy, cz), f32),
            jax.ShapeDtypeStruct((cx // 2, cy // 2, cz // 2), f32),
            jax.ShapeDtypeStruct((cx // 4, cy // 4, cz // 4), f32),
            jax.ShapeDtypeStruct((cx // 8, cy // 8, cz // 8), f32),
            jax.ShapeDtypeStruct(velocity.shape, f32),
            jax.ShapeDtypeStruct((1, 1), f32),
        ),
        in_specs=[hbm] * 6,
        out_specs=(vmem,) * 7,
        scratch_shapes=[
            field,
            field,
            field,
            v((cx + 2, tall, cz), f32),
            v((3, cx, cy, cz), f32),
            v(mats.shape, f32),
            v(blocks.shape, blocks.dtype),
            pltpu.SMEM(prefactor.shape, f32),
            pltpu.SMEM(yield_stress.shape, f32),
            v((6, cx, cy, cz), f32),
            v((cx, cy, cz), f32),
            v((cx, cy, cz), f32),
            v((3, cx, cy, cz), f32),
            v((cx, cy, cz), f32),
            v((cx, cy, cz), f32),
            v((cx // BLOCK, cy, cz), f32),
            v((cx // BLOCK, cy, cz), f32),
            v((3, 2, 3, cy, cz), f32),
            v((3, 2, 3, cy, cz), f32),
            v((2, cy, cz), f32),
            v((4, 2, 3, cx, cz), f32),
            v((4, 2, 3, cx, cz), f32),
            v((4, cy, cz), f32),
            v((4, 2, cy, cz), f32),
            v((cx // 2 + 2, tall, cz), f32),
            v((cx // 4 + 2, tall, cz), f32),
            v((cx // 8 + 2, tall, cz), f32),
            v((2, 3, cy, cz), f32),
            v((2, 3, cy, cz), f32),
            v((cx // 2, tall, cz), f32),
            v((cx // 4, tall, cz), f32),
            v((cx // 4, tall, cz), f32),
            v((cx // 8, tall, cz), f32),
            v((cx // 8, tall, cz), f32),
            v((cx // 8, tall, cz), f32),
            v((2, ghosts, cz), f32),
            v((2, ghosts, cz), f32),
            v((8, cz), f32),
            v((2, 8, cz), f32),
            v((firsts, 1, cz), f32),
            v((nz, 1, cz), f32),
            dma((10,)),
            dma((15, 2)),
            dma((15, 2)),
            dma((2,)),
            dma((2,)),
        ],
        compiler_params=pltpu.CompilerParams(
            collective_id=0, has_side_effects=True, vmem_limit_bytes=40 * 1024 * 1024
        ),
    )(*(pltpu.with_memory_space_constraint(a, pltpu.HBM) for a in operands))
    outs = pl.pallas_call(
        writer,
        out_shape=tuple(jax.ShapeDtypeStruct(out.shape, f32) for out in outs),
        in_specs=[vmem] * 7,
        out_specs=(hbm,) * 7,
        scratch_shapes=[dma((7,))],
        compiler_params=pltpu.CompilerParams(vmem_limit_bytes=8 * 1024 * 1024),
    )(*outs)
    return outs[:6] + (outs[6].reshape(()),)


def solution(mesh):
    grid = P("gx", "gy", "gz")
    vector = P(None, "gx", "gy", "gz")
    return jax.shard_map(
        per_device,
        mesh=mesh,
        in_specs=(vector, vector, grid, P(), P()),
        out_specs=(vector, grid, grid, grid, grid, vector, P()),
        check_vma=False,
    )
```

```python
import functools

import jax
import jax.numpy as jnp
import numpy as np
from jax import lax
from jax.experimental import pallas as pl
from jax.experimental.pallas import tpu as pltpu
from jax.sharding import PartitionSpec as P

BLOCK = 4
RELAXATION = 0.8
PAD = 8
GHOST = 64
UNROLL = 4
STAGES = (3, 0, 1)
STAGES_VISC = (2, 2, 2)
ONE_STAGE = 32
ROUNDS = 4
MESH = pl.DeviceIdType.MESH
HIGHEST = lax.Precision.HIGHEST


def coarse_matrices(length):
    def chain(low_edge, high_edge):
        field = np.eye(length)
        found = []
        first = 0
        for _ in range(3):
            count = length >> (len(found) + 1)
            out = np.zeros((length, count + 2))
            for k in range(-1, count + 1):
                for shift, weight in ((-1, 1.0), (0, 3.0), (1, 3.0), (2, 1.0)):
                    source = 2 * k + shift - first
                    if 0 <= source < field.shape[1]:
                        out[:, k + 1] += weight / 8.0 * field[:, source]
            if low_edge:
                out[:, 0] = 0.0
            if high_edge:
                out[:, -1] = 0.0
            placed = np.zeros((length, length))
            placed[:, :count] = out[:, 1:-1]
            placed[:, GHOST] = out[:, 0]
            placed[:, GHOST + 1] = out[:, -1]
            found.append(placed)
            field = out
            first = -1
        return np.stack(found)

    inner = chain(False, False)
    return np.stack([inner, inner - chain(True, False), inner - chain(False, True)]).astype(np.float32)


def kernel(
    sizes,
    vel_hbm,
    forc_hbm,
    mats_hbm,
    phase_hbm,
    pref_hbm,
    yield_hbm,
    smooth_ref,
    visc_ref,
    one_ref,
    two_ref,
    three_ref,
    misfit_ref,
    rms_ref,
    v0,
    v1,
    v2,
    visc,
    forc,
    mats,
    phase_ref,
    pref_ref,
    yield_ref,
    faces,
    z_faces,
    z_scaled,
    early,
    weight,
    diag,
    pref_cells,
    yield_cells,
    x_send,
    x_recv,
    visc_x,
    y_send,
    y_recv,
    z_send,
    z_recv,
    cx1,
    cx2,
    cx3,
    gx_send,
    gx_recv,
    t1,
    t2a,
    t2b,
    t3a,
    t3b,
    t3c,
    gy_send,
    gy_recv,
    gz_send,
    gz_recv,
    sums_xy,
    sums_z,
    local_sem,
    send_sem,
    recv_sem,
    plane_sem,
    line_sem,
    hello_sem,
):
    nx, ny, nz, cx, cy, cz, phases = sizes
    ix, iy, iz = lax.axis_index("gx"), lax.axis_index("gy"), lax.axis_index("gz")
    rows = pl.ds(PAD, cy)

    ends_in = [
        pltpu.make_async_copy(vel_hbm.at[:, cx - 1], x_send.at[0, 0], local_sem.at[0]),
        pltpu.make_async_copy(vel_hbm.at[:, 0], x_send.at[0, 1], local_sem.at[1]),
    ]
    vel_in = [
        pltpu.make_async_copy(vel_hbm.at[comp], v0.at[comp, pl.ds(1, cx), rows, :], local_sem.at[2 + comp])
        for comp in range(3)
    ]
    forc_in = pltpu.make_async_copy(forc_hbm, forc, local_sem.at[5])
    mats_in = pltpu.make_async_copy(mats_hbm, mats, local_sem.at[6])
    phase_in = pltpu.make_async_copy(phase_hbm, phase_ref, local_sem.at[7])
    pref_in = pltpu.make_async_copy(pref_hbm, pref_ref, local_sem.at[8])
    yield_in = pltpu.make_async_copy(yield_hbm, yield_ref, local_sem.at[9])
    for copy in ends_in + vel_in:
        copy.start()

    barrier = pltpu.get_barrier_semaphore()
    one_stage = nx * ny * nz <= ONE_STAGE
    me_xy = ix * ny + iy
    me_first = me_xy * nz + iz if one_stage else me_xy

    def first_peers():
        if one_stage:
            others = [lax.rem(me_first + k, nx * ny * nz) for k in range(1, nx * ny * nz)]
            return [(o // (ny * nz), lax.rem(o // nz, ny), lax.rem(o, nz)) for o in others]
        others = [lax.rem(me_first + k, nx * ny) for k in range(1, nx * ny)]
        return [(o // ny, lax.rem(o, ny), iz) for o in others]

    line_peers = [] if one_stage else [(ix, iy, lax.rem(iz + k, nz)) for k in range(1, nz)]
    has_up = (ix < nx - 1, iy < ny - 1, iz < nz - 1)
    has_down = (ix > 0, iy > 0, iz > 0)
    up_ids = (
        (lax.rem(ix + 1, nx), iy, iz),
        (ix, lax.rem(iy + 1, ny), iz),
        (ix, iy, lax.rem(iz + 1, nz)),
    )
    down_ids = (
        (lax.rem(ix + nx - 1, nx), iy, iz),
        (ix, lax.rem(iy + ny - 1, ny), iz),
        (ix, iy, lax.rem(iz + nz - 1, nz)),
    )
    z_line = [(ix, iy, lax.rem(iz + k, nz)) for k in range(1, nz)]
    steps = [nx - 1, ny - 1, nz - 1] if one_stage else [nx - 1, ny - 1]
    near_only = one_stage and steps[0] + steps[1] <= ROUNDS and steps[2] <= ROUNDS
    if near_only:
        met = 0
        for there, peer in list(zip(has_up, up_ids)) + list(zip(has_down, down_ids)):
            met = met + there.astype(jnp.int32)

            @pl.when(there)
            def _():
                pl.semaphore_signal(barrier, inc=1, device_id=peer, device_id_type=MESH)
    else:
        if sum(steps) - max(steps) <= ROUNDS:
            greeted = [(lax.rem(ix + k, nx), iy, iz) for k in range(1, nx)]
            greeted += [(ix, lax.rem(iy + k, ny), iz) for k in range(1, ny)]
            greeted += z_line
        else:
            greeted = first_peers() + line_peers
        met = len(greeted)
        for peer in greeted:
            pl.semaphore_signal(barrier, inc=1, device_id=peer, device_id_type=MESH)
    for copy in (phase_in, pref_in, yield_in):
        copy.start()

    def clear(ref):
        ref[...] = jnp.zeros(ref.shape, jnp.float32)

    for side, present in ((0, has_down), (1, has_up)):
        @pl.when(jnp.logical_not(present[0]))
        def _():
            for r in range(3):
                clear(x_recv.at[r, side])
            clear(visc_x.at[side])
            clear(gx_recv.at[side])

        @pl.when(jnp.logical_not(present[1]))
        def _():
            for r in range(4):
                clear(y_recv.at[r, side])
            clear(gy_recv.at[side])

        @pl.when(jnp.logical_not(present[2]))
        def _():
            for r in range(4):
                clear(z_recv.at[r, side])
            clear(gz_recv.at[side])

    for buf in [v.at[comp] for v in (v0, v1, v2) for comp in range(3)] + [visc]:
        clear(buf.at[0, rows])
        clear(buf.at[cx + 1, rows])
        clear(buf.at[pl.ds(1, cx), pl.ds(PAD - 1, 1)])
        clear(buf.at[pl.ds(1, cx), pl.ds(PAD + cy, 1)])

    lane = lax.broadcasted_iota(jnp.int32, (cy, cz), 1)
    odd_lane = lax.rem(lane, 2) == 1
    lane_pair = (lane - 1) // 2
    first_lane = lane == 0
    last_lane = lane == cz - 1
    end_lane = first_lane | last_lane

    started = []

    def exchange(slot, dim, up_src, up_dst, down_src, down_dst):
        up = pltpu.make_async_remote_copy(
            up_src, up_dst, send_sem.at[slot, 0], recv_sem.at[slot, 0],
            device_id=up_ids[dim], device_id_type=MESH,
        )
        down = pltpu.make_async_remote_copy(
            down_src, down_dst, send_sem.at[slot, 1], recv_sem.at[slot, 1],
            device_id=down_ids[dim], device_id_type=MESH,
        )
        pl.when(has_up[dim])(up.start)
        pl.when(has_down[dim])(down.start)
        started.append((has_up[dim], up))
        started.append((has_down[dim], down))

        def wait():
            pl.when(has_down[dim])(up.wait_recv)
            pl.when(has_up[dim])(down.wait_recv)

        return wait

    def send_x(r, last, low, first, high):
        return exchange(3 * r, 0, last, low, first, high)

    def send_yz(r):
        held = pl.ds(0, 1 if r == 1 else 3)
        return [
            exchange(
                3 * r + 1, 1,
                y_send.at[r, 0, held], y_recv.at[r, 0, held],
                y_send.at[r, 1, held], y_recv.at[r, 1, held],
            ),
            exchange(3 * r + 2, 2, z_send.at[r], z_recv.at[r, 0], z_send.at[r], z_recv.at[r, 1]),
        ]

    def pack(r, comp, i, value, packed):
        y_send[r, 0, comp, pl.ds(i, 1), :] = value[cy - 1 : cy, :]
        y_send[r, 1, comp, pl.ds(i, 1), :] = value[0:1, :]
        place = 2 * (comp * cx + i) + 1
        return jnp.where(lane_pair == comp * cx + i, pltpu.roll(value, place + 1, 1), packed)

    def unpack_y(r, buf, comps):
        def body(i, carry):
            for comp in range(comps):
                target = buf.at[comp, i + 1] if comps == 3 else buf.at[i + 1]
                target[PAD - 1 : PAD, :] = y_recv[r, 0, comp, pl.ds(i, 1), :]
                target[PAD + cy : PAD + cy + 1, :] = y_recv[r, 1, comp, pl.ds(i, 1), :]
            return carry

        lax.fori_loop(0, cx, body, 0)

    def merged_z(r):
        return jnp.where(odd_lane, z_recv[r, 0], pltpu.roll(z_recv[r, 1], cz - 2, 1))

    def along(plane_ref, centre, merged, place):
        edge = pltpu.roll(merged, cz - 1 - 2 * place, 1)
        return (
            plane_ref[PAD - 1 : PAD - 1 + cy, :],
            plane_ref[PAD + 1 : PAD + 1 + cy, :],
            jnp.where(first_lane, edge, pltpu.roll(centre, 1, 1)),
            jnp.where(last_lane, edge, pltpu.roll(centre, cz - 1, 1)),
        )

    def around(buf, comp, i, merged):
        centre = buf[comp, i + 1, rows, :]
        ym, yp, zm, zp = along(buf.at[comp, i + 1], centre, merged, comp * cx + i)
        return centre, (buf[comp, i, rows, :], buf[comp, i + 2, rows, :], ym, yp, zm, zp)

    for copy in ends_in:
        copy.wait()
    pl.semaphore_wait(barrier, met)
    waits = [send_x(0, x_send.at[0, 0], x_recv.at[0, 0], x_send.at[0, 1], x_recv.at[0, 1])]
    nothing = jnp.zeros((cy, cz), jnp.float32)
    packed = nothing
    for comp in range(3):
        vel_in[comp].wait()
        for i in range(cx):
            packed = pack(0, comp, i, v0[comp, i + 1, rows, :], packed)
    z_send[0] = packed
    waits += send_yz(0)
    forc_in.start()
    mats_in.start()

    phase_in.wait()
    pref_in.wait()
    yield_in.wait()
    blocks = phase_ref[...].astype(jnp.float32)
    n_rows, n_blocks = blocks.shape
    spread_z = lax.broadcasted_iota(jnp.int32, (n_blocks, cz), 1) // BLOCK
    spread_z = (spread_z == lax.broadcasted_iota(jnp.int32, (n_blocks, cz), 0)).astype(jnp.float32)
    spread_y = lax.broadcasted_iota(jnp.int32, (n_rows * BLOCK, n_rows), 0) // BLOCK
    spread_y = (
        spread_y == lax.broadcasted_iota(jnp.int32, (n_rows * BLOCK, n_rows), 1)
    ).astype(jnp.float32)
    cells = jnp.dot(blocks, spread_z, preferred_element_type=jnp.float32, precision=HIGHEST)
    cells = jnp.dot(spread_y, cells, preferred_element_type=jnp.float32, precision=HIGHEST)
    for bx in range(cx // BLOCK):
        phase = cells[bx * cy : (bx + 1) * cy, :]
        pref_value = jnp.zeros((cy, cz), jnp.float32)
        yield_value = jnp.zeros((cy, cz), jnp.float32)
        for p in range(phases):
            here = jnp.abs(phase - float(p)) < 0.5
            pref_value = jnp.where(here, pref_ref[p], pref_value)
            yield_value = jnp.where(here, yield_ref[p], yield_value)
        pref_cells[bx] = pref_value
        yield_cells[bx] = 0.5 * yield_value
    for buf in (cx1, cx2, cx3):
        for edge in (0, PAD + cy):
            buf[:, edge : edge + PAD, :] = jnp.zeros((buf.shape[0], PAD, cz), jnp.float32)
    for buf in (t1, t2a, t2b, t3a, t3b, t3c):
        buf[...] = jnp.zeros(buf.shape, jnp.float32)

    along_x, along_y, along_z = (0, 3, 4), (3, 1, 5), (4, 5, 2)

    def early_strain(i, carry):
        found = {}
        for comp in range(3):
            plane = v0.at[comp, i + 1]
            centre = plane[rows, :]
            low = jnp.where(first_lane, 0.0, pltpu.roll(centre, 1, 1))
            high = jnp.where(last_lane, 0.0, pltpu.roll(centre, cz - 1, 1))
            for n, jump in (
                (along_x[comp], v0[comp, i + 2, rows, :] - v0[comp, i, rows, :]),
                (along_y[comp], plane[PAD + 1 : PAD + 1 + cy, :] - plane[PAD - 1 : PAD - 1 + cy, :]),
                (along_z[comp], high - low),
            ):
                found[n] = found[n] + jump if n in found else jump
        for n in range(6):
            faces[n, i] = found[n]
        return carry

    lax.fori_loop(0, cx, early_strain, 0, unroll=UNROLL)
    for wait in waits:
        wait()
    merged0 = merged_z(0)
    signed0 = jnp.where(odd_lane, -merged0, merged0)
    for comp in range(3):
        n = along_x[comp]
        faces[n, 0] = faces[n, 0] - x_recv[0, 0, comp]
        faces[n, cx - 1] = faces[n, cx - 1] + x_recv[0, 1, comp]

    def late_strain(i):
        for comp in range(3):
            n = along_y[comp]
            faces[n, i, 0:1, :] = faces[n, i, 0:1, :] - y_recv[0, 0, comp, pl.ds(i, 1), :]
            faces[n, i, cy - 1 : cy, :] = faces[n, i, cy - 1 : cy, :] + y_recv[0, 1, comp, pl.ds(i, 1), :]

    order = [0, cx - 1] + list(range(1, cx - 1))

    def shell_pass(fix, edge, value_of, r, send_ends, stages):
        ahead, hold, behind = stages
        packed = nothing
        edges, values, rolled = {}, {}, {}
        sent = None
        for t in range(cx + ahead + hold + behind):
            if t < cx:
                edges[t] = edge(order[t])
                fix(order[t])
            n = t - ahead
            if 0 <= n < cx:
                i = order[n]
                values[n] = []
                for comp, value in enumerate(value_of(i, edges.pop(n))):
                    if r is not None:
                        y_send[r, 0, comp, pl.ds(i, 1), :] = value[cy - 1 : cy, :]
                        y_send[r, 1, comp, pl.ds(i, 1), :] = value[0:1, :]
                        values[n].append((comp * cx + i, value))
                if n == 1 and send_ends is not None:
                    sent = send_ends()
            n = t - ahead - hold
            if 0 <= n < cx:
                rolled[n] = [(place, pltpu.roll(value, 2 * place + 2, 1)) for place, value in values.pop(n)]
            n = t - ahead - hold - behind
            if 0 <= n < cx:
                for place, value in rolled.pop(n):
                    packed = jnp.where(lane_pair == place, value, packed)
        if r is None:
            return None
        z_send[r] = packed
        return [sent] + send_yz(r)

    def edge_of(merged, place):
        return pltpu.roll(merged, cz - 1 - 2 * place, 1)

    def edges_visc(i):
        return [edge_of(signed0, comp * cx + i) for comp in range(3)]

    def values_visc(i, edges):
        strain = [faces[n, i] for n in range(6)]
        for comp in range(3):
            n = along_z[comp]
            strain[n] = strain[n] + jnp.where(end_lane, edges[comp], 0.0)
        squared = [term * term for term in strain]
        straight = squared[0] + squared[1] + squared[2]
        skew = squared[3] + squared[4] + squared[5]
        invariant = 1.0 + (0.125 * straight + 0.0625 * skew)
        creeping = pref_cells[i // BLOCK] * jnp.exp(jnp.log(invariant) * (-1.0 / 3.0))
        plastic = yield_cells[i // BLOCK] * lax.rsqrt(invariant)
        value = jnp.minimum(creeping, plastic)
        visc[i + 1, rows, :] = value
        yield value

    def send_visc():
        return send_x(1, visc.at[cx, rows, :], visc_x.at[0], visc.at[1, rows, :], visc_x.at[1])

    waits = shell_pass(late_strain, edges_visc, values_visc, 1, send_visc, STAGES_VISC)
    for comp in range(3):
        v0[comp, 0, rows, :] = x_recv[0, 0, comp]
        v0[comp, cx + 1, rows, :] = x_recv[0, 1, comp]
    unpack_y(0, v0, 3)

    def flag(condition):
        return jnp.where(condition, 1.0, 0.0).astype(jnp.float32)

    def restrict_planes(source, first, held, count, target, level):
        for k in range(-1, count + 1):
            total = None
            for shift, factor in ((-1, 0.125), (0, 0.375), (1, 0.375), (2, 0.125)):
                at = 2 * k + shift - first
                if 0 <= at < held:
                    term = factor * source[at, rows, :]
                    total = term if total is None else total + term
            if k == -1:
                total = total * flag(has_down[0])
                gx_send[1, level] = total
            if k == count:
                total = total * flag(has_up[0])
                gx_send[0, level] = total
            target[k + 1, rows, :] = total

    restrict_planes(visc.at[pl.ds(1, cx)], 0, cx, cx // 2, cx1, 0)
    restrict_planes(cx1, -1, cx // 2 + 2, cx // 4, cx2, 1)
    restrict_planes(cx2, -1, cx // 4 + 2, cx // 8, cx3, 2)
    wait_gx = exchange(12, 0, gx_send.at[0], gx_recv.at[0], gx_send.at[1], gx_recv.at[1])

    forc_in.wait()

    def early_one(i, carry):
        plane = visc.at[i + 1]
        centre = plane[rows, :]
        visc_ref[i] = centre
        sides = (
            centre + visc[i, rows, :],
            centre + visc[i + 2, rows, :],
            centre + plane[PAD - 1 : PAD - 1 + cy, :],
            centre + plane[PAD + 1 : PAD + 1 + cy, :],
            centre + jnp.where(first_lane, 0.0, pltpu.roll(centre, 1, 1)),
            centre + jnp.where(last_lane, 0.0, pltpu.roll(centre, cz - 1, 1)),
        )
        for n in range(4):
            faces[n, i] = sides[n]
        faces[4, i] = jnp.where(first_lane, 0.0, sides[4])
        faces[5, i] = jnp.where(last_lane, 0.0, sides[5])
        diag[i] = (sides[0] + sides[1]) + (sides[2] + sides[3]) + (sides[4] + sides[5])
        for comp in range(3):
            _, near = around(v0, comp, i, merged0)
            flow = 2.0 * forc[comp, i]
            for n in range(6):
                flow = flow + sides[n] * near[n]
            early[comp, i] = flow
        return carry

    lax.fori_loop(0, cx, early_one, 0, unroll=UNROLL)
    for wait in waits:
        wait()
    merged1 = merged_z(1)

    for side, i, face, halo_plane in ((0, 0, 0, 0), (1, cx - 1, 1, cx + 1)):
        halo = visc_x[side]
        faces[face, i] = faces[face, i] + halo
        diag[i] = diag[i] + halo
        for comp in range(3):
            early[comp, i] = early[comp, i] + halo * v0[comp, halo_plane, rows, :]

    def late_one(i):
        ends = ((0, 2, 0, PAD - 1), (1, 3, cy - 1, PAD + cy))
        for side, face, at, row in ends:
            halo = y_recv[1, side, 0, pl.ds(i, 1), :]
            faces[face, i, at : at + 1, :] = faces[face, i, at : at + 1, :] + halo
            diag[i, at : at + 1, :] = diag[i, at : at + 1, :] + halo
            for comp in range(3):
                near = v0[comp, i + 1, row : row + 1, :]
                early[comp, i, at : at + 1, :] = early[comp, i, at : at + 1, :] + halo * near

    def edges_one(i):
        return [edge_of(merged1, i)] + [edge_of(merged0, comp * cx + i) for comp in range(3)]

    def values_one(i, edges):
        halo = jnp.where(end_lane, edges[0], 0.0)
        total = diag[i] + halo
        scale = RELAXATION / total
        diag[i] = total
        weight[i] = scale
        z_faces[i] = jnp.where(end_lane, visc[i + 1, rows, :] + halo, 0.0)
        for comp in range(3):
            flow = early[comp, i] + halo * edges[1 + comp]
            value = (1.0 - RELAXATION) * v0[comp, i + 1, rows, :] + scale * flow
            v1[comp, i + 1, rows, :] = value
            keep_end(2, comp, i, value)
            yield value

    def send_ends(r):
        s = r - 1
        return lambda: send_x(r, x_send.at[s, 0], x_recv.at[s, 0], x_send.at[s, 1], x_recv.at[s, 1])

    def keep_end(r, comp, i, value):
        if i == cx - 1:
            x_send[r - 1, 0, comp] = value
        if i == 0:
            x_send[r - 1, 1, comp] = value

    waits = shell_pass(late_one, edges_one, values_one, 2, send_ends(2), STAGES)

    wait_gx()
    low_y, high_y = flag(has_down[1]), flag(has_up[1])
    gx_counts = (cx // 2, cx // 4, cx // 8)
    for level, buf in enumerate((cx1, cx2, cx3)):
        buf[1, rows, :] = buf[1, rows, :] + gx_recv[0, level]
        last = gx_counts[level]
        buf[last, rows, :] = buf[last, rows, :] + gx_recv[1, level]

    def restrict_rows(source, target, count):
        size = count + 2
        a, b, c, d = (source[pl.ds(PAD - 3 + s, size, stride=2), :] for s in range(4))
        target[PAD - 1 : PAD - 1 + size, :] = 0.125 * (a + d) + 0.375 * (b + c)
        target[PAD - 1 : PAD, :] = target[PAD - 1 : PAD, :] * low_y
        target[PAD + count : PAD + count + 1, :] = target[PAD + count : PAD + count + 1, :] * high_y

    row = 0
    ghost_rows = []
    for level, (buf, steps) in enumerate(((cx1, (t1,)), (cx2, (t2a, t2b)), (cx3, (t3a, t3b, t3c)))):
        for k in range(gx_counts[level]):
            source = buf.at[k + 1]
            for depth, target in enumerate(steps):
                restrict_rows(source, target.at[k], cy >> (depth + 1))
                source = target.at[k]
            count = cy >> len(steps)
            gy_send[1, row : row + 1, :] = source[PAD - 1 : PAD, :]
            gy_send[0, row : row + 1, :] = source[PAD + count : PAD + count + 1, :]
            ghost_rows.append((steps[-1], k, count, row))
            row += 1
    wait_gy = exchange(13, 1, gy_send.at[0], gy_recv.at[0], gy_send.at[1], gy_recv.at[1])

    def around_inner(buf, comp, i):
        plane = buf.at[comp, i + 1]
        centre = plane[rows, :]
        return centre, (
            buf[comp, i, rows, :],
            buf[comp, i + 2, rows, :],
            plane[PAD - 1 : PAD - 1 + cy, :],
            plane[PAD + 1 : PAD + 1 + cy, :],
            pltpu.roll(centre, 1, 1),
            pltpu.roll(centre, cz - 1, 1),
        )

    def flow_inner(buf, comp, i):
        centre, near = around_inner(buf, comp, i)
        flow = 2.0 * forc[comp, i]
        for n in range(6):
            flow = flow + faces[n, i] * near[n]
        return centre, flow

    def early_two(i, carry):
        z_scaled[i] = weight[i] * z_faces[i]
        for comp in range(3):
            centre, flow = flow_inner(v1, comp, i)
            early[comp, i] = (1.0 - RELAXATION) * centre + weight[i] * flow
        return carry

    def late_planes(r, scaled):
        for side, i, face in ((0, 0, 0), (1, cx - 1, 1)):
            factor = faces[face, i]
            if scaled:
                factor = factor * weight[i]
            for comp in range(3):
                early[comp, i] = early[comp, i] + factor * x_recv[r - 1, side, comp]

    def late_rows(r, scaled):
        def fix(i):
            for side, face, at in ((0, 2, 0), (1, 3, cy - 1)):
                factor = faces[face, i, at : at + 1, :]
                if scaled:
                    factor = factor * weight[i, at : at + 1, :]
                for comp in range(3):
                    halo = y_recv[r, side, comp, pl.ds(i, 1), :]
                    early[comp, i, at : at + 1, :] = early[comp, i, at : at + 1, :] + factor * halo

        return fix

    lax.fori_loop(0, cx, early_two, 0, unroll=UNROLL)
    for wait in waits:
        wait()
    merged2 = merged_z(2)
    late_planes(2, True)

    def edges_two(i):
        return [edge_of(merged2, comp * cx + i) for comp in range(3)]

    def values_two(i, edges):
        factor = z_scaled[i]
        for comp in range(3):
            value = early[comp, i] + factor * edges[comp]
            v2[comp, i + 1, rows, :] = value
            keep_end(3, comp, i, value)
            yield value

    waits = shell_pass(late_rows(2, True), edges_two, values_two, 3, send_ends(3), STAGES)

    wait_gy()
    for buf, k, count, row in ghost_rows:
        buf[k, PAD : PAD + 1, :] = buf[k, PAD : PAD + 1, :] + gy_recv[0, row : row + 1, :]
        last = PAD + count - 1
        buf[k, last : last + 1, :] = buf[k, last : last + 1, :] + gy_recv[1, row : row + 1, :]
    mats_in.wait()
    off_low, off_high = 1.0 - flag(has_down[2]), 1.0 - flag(has_up[2])
    results = []
    groups = []
    lane8 = lax.broadcasted_iota(jnp.int32, (8, cz), 1)
    packed = jnp.zeros((8, cz), jnp.float32)
    for level, buf in enumerate((t1, t2b, t3c)):
        count = gx_counts[level]
        height = max(8, cy >> (level + 1))
        matrix = mats[0, level] - off_low * mats[1, level] - off_high * mats[2, level]
        data = buf[:, PAD : PAD + height, :].reshape(count * height, cz)
        result = jnp.dot(data, matrix, preferred_element_type=jnp.float32, precision=HIGHEST)
        for part in range(count * height // 8):
            g = len(groups)
            piece = result[8 * part : 8 * part + 8, :]
            groups.append((level, 8 * part // height, 8 * part % height, piece))
            shifted = pltpu.roll(piece, (2 * g - GHOST) % cz, 1)
            packed = jnp.where((lane8 == 2 * g) | (lane8 == 2 * g + 1), shifted, packed)
    gz_send[...] = packed
    wait_gz = exchange(14, 2, gz_send, gz_recv.at[0], gz_send, gz_recv.at[1])

    def early_misfit(i, carry):
        for comp in range(3):
            centre, flow = flow_inner(v2, comp, i)
            smooth_ref[comp, i] = centre
            early[comp, i] = flow - diag[i] * centre
        return carry

    if near_only:
        for peer in z_line:
            pl.semaphore_signal(hello_sem, inc=1, device_id=peer, device_id_type=MESH)
    lax.fori_loop(0, cx, early_misfit, 0, unroll=UNROLL)
    for wait in waits:
        wait()
    merged3 = merged_z(3)
    late_planes(3, False)
    squares = []

    def edges_three(i):
        return [edge_of(merged3, comp * cx + i) for comp in range(3)]

    def values_three(i, edges):
        total = None
        for comp in range(3):
            value = 0.5 * (early[comp, i] + z_faces[i] * edges[comp])
            misfit_ref[comp, i] = value
            total = value * value if total is None else total + value * value
            yield value
        squares.append(total if not squares else squares[-1] + total)

    shell_pass(late_rows(3, False), edges_three, values_three, None, None, STAGES)
    part = jnp.sum(squares[-1], axis=0, keepdims=True)

    def gather(slots, mine, value, peers, sems):
        slots[mine] = value
        for peer in peers:
            pltpu.make_async_remote_copy(
                slots.at[mine], slots.at[mine], sems.at[0], sems.at[1],
                device_id=peer, device_id_type=MESH,
            ).start()
        others = slots.at[pl.ds(0, len(peers))]
        return pltpu.make_async_remote_copy(
            others, others, sems.at[0], sems.at[1], device_id=peers[0], device_id_type=MESH
        )

    def total_of(slots):
        parts = [slots[n] for n in range(slots.shape[0])]
        while len(parts) > 1:
            parts = [sum(parts[n : n + 2]) for n in range(0, len(parts), 2)]
        return parts[0]

    if near_only:
        pl.semaphore_wait(hello_sem, nz - 1)
    plane_copies = gather(sums_xy, me_first, part, first_peers(), plane_sem)

    wait_gz()
    low_part, high_part = gz_recv[0], gz_recv[1]
    for g, (level, k, at, piece) in enumerate(groups):
        width = cz >> (level + 1)
        height = cy >> (level + 1)
        piece = piece + jnp.where(lane8 == 0, pltpu.roll(low_part, (cz - 2 * g - 1) % cz, 1), 0.0)
        piece = piece + jnp.where(
            lane8 == width - 1, pltpu.roll(high_part, (width - 1 - 2 * g) % cz, 1), 0.0
        )
        target = (one_ref, two_ref, three_ref)[level]
        size = min(8, height - at)
        target[k, at : at + size, :] = piece[:size, :width]

    for condition, copy in started:
        pl.when(condition)(copy.wait_send)
    plane_copies.wait()
    whole = total_of(sums_xy)
    if not one_stage:
        gather(sums_z, iz, whole, line_peers, line_sem).wait()
        whole = total_of(sums_z)
    whole = jnp.sum(whole, axis=1, keepdims=True)
    cells_all = float(3 * cx * nx * cy * ny * cz * nz)
    rms_ref[...] = jnp.sqrt(whole / cells_all)


def writer(*refs):
    copies = [
        pltpu.make_async_copy(refs[n], refs[7 + n], refs[14].at[n]) for n in (0, 5, 1, 2, 3, 4, 6)
    ]
    for copy in copies:
        copy.start()
    for copy in copies:
        copy.wait()


def per_device(velocity, forcing, phase_block, prefactor, yield_stress):
    _, cx, cy, cz = velocity.shape
    nx, ny, nz = lax.axis_size("gx"), lax.axis_size("gy"), lax.axis_size("gz")
    f32 = jnp.float32
    sizes = (nx, ny, nz, cx, cy, cz, prefactor.shape[0])
    mats = jnp.asarray(coarse_matrices(cz))
    blocks = phase_block.reshape(phase_block.shape[0] * phase_block.shape[1], phase_block.shape[2])
    tall = cy + 2 * PAD
    firsts = nx * ny * nz if nx * ny * nz <= ONE_STAGE else nx * ny
    ghosts = cx // 2 + cx // 4 + cx // 8
    ghosts += -ghosts % 8
    hbm = pl.BlockSpec(memory_space=pltpu.HBM)
    vmem = pl.BlockSpec(memory_space=pltpu.VMEM)
    v = pltpu.VMEM
    field = v((3, cx + 2, tall, cz), f32)
    dma = pltpu.SemaphoreType.DMA
    operands = (velocity, forcing, mats, blocks, prefactor, yield_stress)
    outs = pl.pallas_call(
        functools.partial(kernel, sizes),
        out_shape=(
            jax.ShapeDtypeStruct(velocity.shape, f32),
            jax.ShapeDtypeStruct((cx, cy, cz), f32),
            jax.ShapeDtypeStruct((cx // 2, cy // 2, cz // 2), f32),
            jax.ShapeDtypeStruct((cx // 4, cy // 4, cz // 4), f32),
            jax.ShapeDtypeStruct((cx // 8, cy // 8, cz // 8), f32),
            jax.ShapeDtypeStruct(velocity.shape, f32),
            jax.ShapeDtypeStruct((1, 1), f32),
        ),
        in_specs=[hbm] * 6,
        out_specs=(vmem,) * 7,
        scratch_shapes=[
            field,
            field,
            field,
            v((cx + 2, tall, cz), f32),
            v((3, cx, cy, cz), f32),
            v(mats.shape, f32),
            v(blocks.shape, blocks.dtype),
            pltpu.SMEM(prefactor.shape, f32),
            pltpu.SMEM(yield_stress.shape, f32),
            v((6, cx, cy, cz), f32),
            v((cx, cy, cz), f32),
            v((cx, cy, cz), f32),
            v((3, cx, cy, cz), f32),
            v((cx, cy, cz), f32),
            v((cx, cy, cz), f32),
            v((cx // BLOCK, cy, cz), f32),
            v((cx // BLOCK, cy, cz), f32),
            v((3, 2, 3, cy, cz), f32),
            v((3, 2, 3, cy, cz), f32),
            v((2, cy, cz), f32),
            v((4, 2, 3, cx, cz), f32),
            v((4, 2, 3, cx, cz), f32),
            v((4, cy, cz), f32),
            v((4, 2, cy, cz), f32),
            v((cx // 2 + 2, tall, cz), f32),
            v((cx // 4 + 2, tall, cz), f32),
            v((cx // 8 + 2, tall, cz), f32),
            v((2, 3, cy, cz), f32),
            v((2, 3, cy, cz), f32),
            v((cx // 2, tall, cz), f32),
            v((cx // 4, tall, cz), f32),
            v((cx // 4, tall, cz), f32),
            v((cx // 8, tall, cz), f32),
            v((cx // 8, tall, cz), f32),
            v((cx // 8, tall, cz), f32),
            v((2, ghosts, cz), f32),
            v((2, ghosts, cz), f32),
            v((8, cz), f32),
            v((2, 8, cz), f32),
            v((firsts, 1, cz), f32),
            v((nz, 1, cz), f32),
            dma((10,)),
            dma((15, 2)),
            dma((15, 2)),
            dma((2,)),
            dma((2,)),
            pltpu.SemaphoreType.REGULAR,
        ],
        compiler_params=pltpu.CompilerParams(
            collective_id=0, has_side_effects=True, vmem_limit_bytes=40 * 1024 * 1024
        ),
    )(*(pltpu.with_memory_space_constraint(a, pltpu.HBM) for a in operands))
    outs = pl.pallas_call(
        writer,
        out_shape=tuple(jax.ShapeDtypeStruct(out.shape, f32) for out in outs),
        in_specs=[vmem] * 7,
        out_specs=(hbm,) * 7,
        scratch_shapes=[dma((7,))],
        compiler_params=pltpu.CompilerParams(vmem_limit_bytes=8 * 1024 * 1024),
    )(*outs)
    return outs[:6] + (outs[6].reshape(()),)


def solution(mesh):
    grid = P("gx", "gy", "gz")
    vector = P(None, "gx", "gy", "gz")
    return jax.shard_map(
        per_device,
        mesh=mesh,
        in_specs=(vector, vector, grid, P(), P()),
        out_specs=(vector, grid, grid, grid, grid, vector, P()),
        check_vma=False,
    )
```

```python
import functools

import jax
import jax.numpy as jnp
import numpy as np
from jax import lax
from jax.experimental import pallas as pl
from jax.experimental.pallas import tpu as pltpu
from jax.sharding import PartitionSpec as P

BLOCK = 4
RELAXATION = 0.8
PAD = 8
GHOST = 64
UNROLL = 4
STAGES = (3, 0, 1)
STAGES_VISC = (2, 2, 2)
ONE_STAGE = 32
ROUNDS = 4
MESH = pl.DeviceIdType.MESH
HIGHEST = lax.Precision.HIGHEST


def coarse_matrices(length):
    def chain(low_edge, high_edge):
        field = np.eye(length)
        found = []
        first = 0
        for _ in range(3):
            count = length >> (len(found) + 1)
            out = np.zeros((length, count + 2))
            for k in range(-1, count + 1):
                for shift, weight in ((-1, 1.0), (0, 3.0), (1, 3.0), (2, 1.0)):
                    source = 2 * k + shift - first
                    if 0 <= source < field.shape[1]:
                        out[:, k + 1] += weight / 8.0 * field[:, source]
            if low_edge:
                out[:, 0] = 0.0
            if high_edge:
                out[:, -1] = 0.0
            placed = np.zeros((length, length))
            placed[:, :count] = out[:, 1:-1]
            placed[:, GHOST] = out[:, 0]
            placed[:, GHOST + 1] = out[:, -1]
            found.append(placed)
            field = out
            first = -1
        return np.stack(found)

    inner = chain(False, False)
    return np.stack([inner, inner - chain(True, False), inner - chain(False, True)]).astype(np.float32)


def kernel(
    sizes,
    vel_hbm,
    forc_hbm,
    mats_hbm,
    phase_hbm,
    pref_hbm,
    yield_hbm,
    smooth_ref,
    visc_ref,
    one_ref,
    two_ref,
    three_ref,
    misfit_ref,
    rms_ref,
    v0,
    v1,
    v2,
    visc,
    forc,
    mats,
    phase_ref,
    pref_ref,
    yield_ref,
    faces,
    z_faces,
    z_scaled,
    edge0,
    early,
    weight,
    diag,
    pref_cells,
    yield_cells,
    x_send,
    x_recv,
    visc_x,
    y_send,
    y_recv,
    z_send,
    z_recv,
    cx1,
    cx2,
    cx3,
    gx_send,
    gx_recv,
    t1,
    t2a,
    t2b,
    t3a,
    t3b,
    t3c,
    gy_send,
    gy_recv,
    gz_send,
    gz_recv,
    sums_xy,
    sums_z,
    local_sem,
    send_sem,
    recv_sem,
    plane_sem,
    line_sem,
    hello_sem,
):
    nx, ny, nz, cx, cy, cz, phases = sizes
    ix, iy, iz = lax.axis_index("gx"), lax.axis_index("gy"), lax.axis_index("gz")
    rows = pl.ds(PAD, cy)

    ends_in = [
        pltpu.make_async_copy(vel_hbm.at[:, cx - 1], x_send.at[0, 0], local_sem.at[0]),
        pltpu.make_async_copy(vel_hbm.at[:, 0], x_send.at[0, 1], local_sem.at[1]),
    ]
    vel_in = [
        pltpu.make_async_copy(vel_hbm.at[comp], v0.at[comp, pl.ds(1, cx), rows, :], local_sem.at[2 + comp])
        for comp in range(3)
    ]
    forc_in = pltpu.make_async_copy(forc_hbm, forc, local_sem.at[5])
    mats_in = pltpu.make_async_copy(mats_hbm, mats, local_sem.at[6])
    phase_in = pltpu.make_async_copy(phase_hbm, phase_ref, local_sem.at[7])
    pref_in = pltpu.make_async_copy(pref_hbm, pref_ref, local_sem.at[8])
    yield_in = pltpu.make_async_copy(yield_hbm, yield_ref, local_sem.at[9])
    for copy in ends_in + vel_in:
        copy.start()

    barrier = pltpu.get_barrier_semaphore()
    one_stage = nx * ny * nz <= ONE_STAGE
    me_xy = ix * ny + iy
    me_first = me_xy * nz + iz if one_stage else me_xy

    def first_peers():
        if one_stage:
            others = [lax.rem(me_first + k, nx * ny * nz) for k in range(1, nx * ny * nz)]
            return [(o // (ny * nz), lax.rem(o // nz, ny), lax.rem(o, nz)) for o in others]
        others = [lax.rem(me_first + k, nx * ny) for k in range(1, nx * ny)]
        return [(o // ny, lax.rem(o, ny), iz) for o in others]

    line_peers = [] if one_stage else [(ix, iy, lax.rem(iz + k, nz)) for k in range(1, nz)]
    has_up = (ix < nx - 1, iy < ny - 1, iz < nz - 1)
    has_down = (ix > 0, iy > 0, iz > 0)
    up_ids = (
        (lax.rem(ix + 1, nx), iy, iz),
        (ix, lax.rem(iy + 1, ny), iz),
        (ix, iy, lax.rem(iz + 1, nz)),
    )
    down_ids = (
        (lax.rem(ix + nx - 1, nx), iy, iz),
        (ix, lax.rem(iy + ny - 1, ny), iz),
        (ix, iy, lax.rem(iz + nz - 1, nz)),
    )
    z_line = [(ix, iy, lax.rem(iz + k, nz)) for k in range(1, nz)]
    steps = [nx - 1, ny - 1, nz - 1] if one_stage else [nx - 1, ny - 1]
    near_only = one_stage and steps[0] + steps[1] <= ROUNDS and steps[2] <= ROUNDS
    if near_only:
        met = 0
        for there, peer in list(zip(has_up, up_ids)) + list(zip(has_down, down_ids)):
            met = met + there.astype(jnp.int32)

            @pl.when(there)
            def _():
                pl.semaphore_signal(barrier, inc=1, device_id=peer, device_id_type=MESH)
    else:
        if sum(steps) - max(steps) <= ROUNDS:
            greeted = [(lax.rem(ix + k, nx), iy, iz) for k in range(1, nx)]
            greeted += [(ix, lax.rem(iy + k, ny), iz) for k in range(1, ny)]
            greeted += z_line
        else:
            greeted = first_peers() + line_peers
        met = len(greeted)
        for peer in greeted:
            pl.semaphore_signal(barrier, inc=1, device_id=peer, device_id_type=MESH)
    for copy in (phase_in, pref_in, yield_in):
        copy.start()

    def clear(ref):
        ref[...] = jnp.zeros(ref.shape, jnp.float32)

    for side, present in ((0, has_down), (1, has_up)):
        @pl.when(jnp.logical_not(present[0]))
        def _():
            for r in range(3):
                clear(x_recv.at[r, side])
            clear(visc_x.at[side])
            clear(gx_recv.at[side])

        @pl.when(jnp.logical_not(present[1]))
        def _():
            for r in range(4):
                clear(y_recv.at[r, side])
            clear(gy_recv.at[side])

        @pl.when(jnp.logical_not(present[2]))
        def _():
            for r in range(4):
                clear(z_recv.at[r, side])
            clear(gz_recv.at[side])

    for buf in [v.at[comp] for v in (v0, v1, v2) for comp in range(3)] + [visc]:
        clear(buf.at[0, rows])
        clear(buf.at[cx + 1, rows])
        clear(buf.at[pl.ds(1, cx), pl.ds(PAD - 1, 1)])
        clear(buf.at[pl.ds(1, cx), pl.ds(PAD + cy, 1)])

    lane = lax.broadcasted_iota(jnp.int32, (cy, cz), 1)
    odd_lane = lax.rem(lane, 2) == 1
    lane_pair = (lane - 1) // 2
    first_lane = lane == 0
    last_lane = lane == cz - 1
    end_lane = first_lane | last_lane

    started = []

    def exchange(slot, dim, up_src, up_dst, down_src, down_dst):
        up = pltpu.make_async_remote_copy(
            up_src, up_dst, send_sem.at[slot, 0], recv_sem.at[slot, 0],
            device_id=up_ids[dim], device_id_type=MESH,
        )
        down = pltpu.make_async_remote_copy(
            down_src, down_dst, send_sem.at[slot, 1], recv_sem.at[slot, 1],
            device_id=down_ids[dim], device_id_type=MESH,
        )
        pl.when(has_up[dim])(up.start)
        pl.when(has_down[dim])(down.start)
        started.append((has_up[dim], up))
        started.append((has_down[dim], down))

        def wait():
            pl.when(has_down[dim])(up.wait_recv)
            pl.when(has_up[dim])(down.wait_recv)

        return wait

    def send_x(r, last, low, first, high):
        return exchange(3 * r, 0, last, low, first, high)

    def send_yz(r):
        held = pl.ds(0, 1 if r == 1 else 3)
        return [
            exchange(
                3 * r + 1, 1,
                y_send.at[r, 0, held], y_recv.at[r, 0, held],
                y_send.at[r, 1, held], y_recv.at[r, 1, held],
            ),
            exchange(3 * r + 2, 2, z_send.at[r], z_recv.at[r, 0], z_send.at[r], z_recv.at[r, 1]),
        ]

    def pack(r, comp, i, value, packed):
        y_send[r, 0, comp, pl.ds(i, 1), :] = value[cy - 1 : cy, :]
        y_send[r, 1, comp, pl.ds(i, 1), :] = value[0:1, :]
        place = 2 * (comp * cx + i) + 1
        return jnp.where(lane_pair == comp * cx + i, pltpu.roll(value, place + 1, 1), packed)

    def unpack_y(r, buf, comps):
        def body(i, carry):
            for comp in range(comps):
                target = buf.at[comp, i + 1] if comps == 3 else buf.at[i + 1]
                target[PAD - 1 : PAD, :] = y_recv[r, 0, comp, pl.ds(i, 1), :]
                target[PAD + cy : PAD + cy + 1, :] = y_recv[r, 1, comp, pl.ds(i, 1), :]
            return carry

        lax.fori_loop(0, cx, body, 0)

    def halos_z(r):
        low, high = z_recv[r, 0], z_recv[r, 1]
        return jnp.where(odd_lane, low, high), jnp.where(odd_lane, low, pltpu.roll(high, cz - 2, 1))

    for copy in ends_in:
        copy.wait()
    pl.semaphore_wait(barrier, met)
    waits = [send_x(0, x_send.at[0, 0], x_recv.at[0, 0], x_send.at[0, 1], x_recv.at[0, 1])]
    nothing = jnp.zeros((cy, cz), jnp.float32)
    packed = nothing
    for copy in vel_in:
        copy.wait()
    for comp in range(3):
        for i in range(cx):
            packed = pack(0, comp, i, v0[comp, i + 1, rows, :], packed)
    z_send[0] = packed
    waits += send_yz(0)
    forc_in.start()
    mats_in.start()

    phase_in.wait()
    pref_in.wait()
    yield_in.wait()
    blocks = phase_ref[...].astype(jnp.float32)
    n_rows, n_blocks = blocks.shape
    spread_z = lax.broadcasted_iota(jnp.int32, (n_blocks, cz), 1) // BLOCK
    spread_z = (spread_z == lax.broadcasted_iota(jnp.int32, (n_blocks, cz), 0)).astype(jnp.float32)
    spread_y = lax.broadcasted_iota(jnp.int32, (n_rows * BLOCK, n_rows), 0) // BLOCK
    spread_y = (
        spread_y == lax.broadcasted_iota(jnp.int32, (n_rows * BLOCK, n_rows), 1)
    ).astype(jnp.float32)
    cells = jnp.dot(blocks, spread_z, preferred_element_type=jnp.float32, precision=HIGHEST)
    cells = jnp.dot(spread_y, cells, preferred_element_type=jnp.float32, precision=HIGHEST)
    for bx in range(cx // BLOCK):
        phase = cells[bx * cy : (bx + 1) * cy, :]
        pref_value = jnp.zeros((cy, cz), jnp.float32)
        yield_value = jnp.zeros((cy, cz), jnp.float32)
        for p in range(phases):
            here = jnp.abs(phase - float(p)) < 0.5
            pref_value = jnp.where(here, pref_ref[p], pref_value)
            yield_value = jnp.where(here, yield_ref[p], yield_value)
        pref_cells[bx] = pref_value
        yield_cells[bx] = 0.5 * yield_value
    for buf in (cx1, cx2, cx3):
        for edge in (0, PAD + cy):
            buf[:, edge : edge + PAD, :] = jnp.zeros((buf.shape[0], PAD, cz), jnp.float32)
    for buf in (t1, t2a, t2b, t3a, t3b, t3c):
        buf[...] = jnp.zeros(buf.shape, jnp.float32)

    along_x, along_y, along_z = (0, 3, 4), (3, 1, 5), (4, 5, 2)

    def early_strain(i, carry):
        found = {}
        for comp in range(3):
            plane = v0.at[comp, i + 1]
            centre = plane[rows, :]
            low = jnp.where(first_lane, 0.0, pltpu.roll(centre, 1, 1))
            high = jnp.where(last_lane, 0.0, pltpu.roll(centre, cz - 1, 1))
            for n, jump in (
                (along_x[comp], v0[comp, i + 2, rows, :] - v0[comp, i, rows, :]),
                (along_y[comp], plane[PAD + 1 : PAD + 1 + cy, :] - plane[PAD - 1 : PAD - 1 + cy, :]),
                (along_z[comp], high - low),
            ):
                found[n] = found[n] + jump if n in found else jump
        for n in range(6):
            faces[n, i] = found[n]
        return carry

    lax.fori_loop(0, cx, early_strain, 0, unroll=UNROLL)
    for wait in waits:
        wait()
    halos0 = halos_z(0)
    merged0 = halos0[1]
    signed0 = [jnp.where(odd_lane, -halo, halo) for halo in halos0]
    for comp in range(3):
        n = along_x[comp]
        faces[n, 0] = faces[n, 0] - x_recv[0, 0, comp]
        faces[n, cx - 1] = faces[n, cx - 1] + x_recv[0, 1, comp]

    def late_strain(i):
        for comp in range(3):
            n = along_y[comp]
            faces[n, i, 0:1, :] = faces[n, i, 0:1, :] - y_recv[0, 0, comp, pl.ds(i, 1), :]
            faces[n, i, cy - 1 : cy, :] = faces[n, i, cy - 1 : cy, :] + y_recv[0, 1, comp, pl.ds(i, 1), :]

    order = [0, cx - 1] + list(range(1, cx - 1))

    def shell_pass(fix, edge, value_of, r, send_ends, stages):
        ahead, hold, behind = stages
        packed = nothing
        edges, values, rolled = {}, {}, {}
        sent = None
        for t in range(cx + ahead + hold + behind):
            if t < cx:
                edges[t] = edge(order[t])
                fix(order[t])
            n = t - ahead
            if 0 <= n < cx:
                i = order[n]
                values[n] = []
                for comp, value in enumerate(value_of(i, edges.pop(n))):
                    if r is not None:
                        y_send[r, 0, comp, pl.ds(i, 1), :] = value[cy - 1 : cy, :]
                        y_send[r, 1, comp, pl.ds(i, 1), :] = value[0:1, :]
                        values[n].append((comp * cx + i, value))
                if n == 1 and send_ends is not None:
                    sent = send_ends()
            n = t - ahead - hold
            if 0 <= n < cx:
                rolled[n] = [(place, pltpu.roll(value, 2 * place + 2, 1)) for place, value in values.pop(n)]
            n = t - ahead - hold - behind
            if 0 <= n < cx:
                for place, value in rolled.pop(n):
                    packed = jnp.where(lane_pair == place, value, packed)
        if r is None:
            return None
        z_send[r] = packed
        return [sent] + send_yz(r)

    def edge_of(merged, place):
        return pltpu.roll(merged, cz - 1 - 2 * place, 1)

    def edge_at(halos, i, place):
        mixed, merged = halos
        if i in (0, cx - 1):
            return jnp.where(first_lane, edge_of(mixed, place), edge_of(mixed, place + 1))
        return edge_of(merged, place)

    def edges_visc(i):
        return [edge_at(signed0, i, comp * cx + i) for comp in range(3)]

    def values_visc(i, edges):
        strain = [faces[n, i] for n in range(6)]
        for comp in range(3):
            n = along_z[comp]
            strain[n] = strain[n] + jnp.where(end_lane, edges[comp], 0.0)
        squared = [term * term for term in strain]
        straight = squared[0] + squared[1] + squared[2]
        skew = squared[3] + squared[4] + squared[5]
        invariant = 1.0 + (0.125 * straight + 0.0625 * skew)
        creeping = pref_cells[i // BLOCK] * jnp.exp(jnp.log(invariant) * (-1.0 / 3.0))
        plastic = yield_cells[i // BLOCK] * lax.rsqrt(invariant)
        value = jnp.minimum(creeping, plastic)
        visc[i + 1, rows, :] = value
        yield value

    def send_visc():
        return send_x(1, visc.at[cx, rows, :], visc_x.at[0], visc.at[1, rows, :], visc_x.at[1])

    waits = shell_pass(late_strain, edges_visc, values_visc, 1, send_visc, STAGES_VISC)
    for comp in range(3):
        v0[comp, 0, rows, :] = x_recv[0, 0, comp]
        v0[comp, cx + 1, rows, :] = x_recv[0, 1, comp]
    unpack_y(0, v0, 3)

    def flag(condition):
        return jnp.where(condition, 1.0, 0.0).astype(jnp.float32)

    def restrict_planes(source, first, held, count, target, level):
        for k in range(-1, count + 1):
            total = None
            for shift, factor in ((-1, 0.125), (0, 0.375), (1, 0.375), (2, 0.125)):
                at = 2 * k + shift - first
                if 0 <= at < held:
                    term = factor * source[at, rows, :]
                    total = term if total is None else total + term
            if k == -1:
                total = total * flag(has_down[0])
                gx_send[1, level] = total
            if k == count:
                total = total * flag(has_up[0])
                gx_send[0, level] = total
            target[k + 1, rows, :] = total

    restrict_planes(visc.at[pl.ds(1, cx)], 0, cx, cx // 2, cx1, 0)
    restrict_planes(cx1, -1, cx // 2 + 2, cx // 4, cx2, 1)
    restrict_planes(cx2, -1, cx // 4 + 2, cx // 8, cx3, 2)
    wait_gx = exchange(12, 0, gx_send.at[0], gx_recv.at[0], gx_send.at[1], gx_recv.at[1])

    forc_in.wait()

    def early_one(i, carry):
        plane = visc.at[i + 1]
        centre = plane[rows, :]
        visc_ref[i] = centre
        sides = (
            centre + visc[i, rows, :],
            centre + visc[i + 2, rows, :],
            centre + plane[PAD - 1 : PAD - 1 + cy, :],
            centre + plane[PAD + 1 : PAD + 1 + cy, :],
            centre + jnp.where(first_lane, 0.0, pltpu.roll(centre, 1, 1)),
            centre + jnp.where(last_lane, 0.0, pltpu.roll(centre, cz - 1, 1)),
        )
        for n in range(4):
            faces[n, i] = sides[n]
        faces[4, i] = jnp.where(first_lane, 0.0, sides[4])
        faces[5, i] = jnp.where(last_lane, 0.0, sides[5])
        diag[i] = (sides[0] + sides[1]) + (sides[2] + sides[3]) + (sides[4] + sides[5])
        for comp in range(3):
            plane = v0.at[comp, i + 1]
            centre = plane[rows, :]
            edge = edge_of(merged0, comp * cx + i)
            edge0[comp, i] = edge
            near = (
                v0[comp, i, rows, :],
                v0[comp, i + 2, rows, :],
                plane[PAD - 1 : PAD - 1 + cy, :],
                plane[PAD + 1 : PAD + 1 + cy, :],
                jnp.where(first_lane, edge, pltpu.roll(centre, 1, 1)),
                jnp.where(last_lane, edge, pltpu.roll(centre, cz - 1, 1)),
            )
            flow = 2.0 * forc[comp, i]
            for n in range(6):
                flow = flow + sides[n] * near[n]
            early[comp, i] = flow
        return carry

    lax.fori_loop(0, cx, early_one, 0, unroll=UNROLL)
    for wait in waits:
        wait()
    halos1 = halos_z(1)

    for side, i, face, halo_plane in ((0, 0, 0, 0), (1, cx - 1, 1, cx + 1)):
        halo = visc_x[side]
        faces[face, i] = faces[face, i] + halo
        diag[i] = diag[i] + halo
        for comp in range(3):
            early[comp, i] = early[comp, i] + halo * v0[comp, halo_plane, rows, :]

    def late_one(i):
        ends = ((0, 2, 0, PAD - 1), (1, 3, cy - 1, PAD + cy))
        for side, face, at, row in ends:
            halo = y_recv[1, side, 0, pl.ds(i, 1), :]
            faces[face, i, at : at + 1, :] = faces[face, i, at : at + 1, :] + halo
            diag[i, at : at + 1, :] = diag[i, at : at + 1, :] + halo
            for comp in range(3):
                near = v0[comp, i + 1, row : row + 1, :]
                early[comp, i, at : at + 1, :] = early[comp, i, at : at + 1, :] + halo * near

    def edges_one(i):
        return [edge_at(halos1, i, i)]

    def values_one(i, edges):
        halo = jnp.where(end_lane, edges[0], 0.0)
        total = diag[i] + halo
        scale = RELAXATION / total
        diag[i] = total
        weight[i] = scale
        z_faces[i] = jnp.where(end_lane, visc[i + 1, rows, :] + halo, 0.0)
        for comp in range(3):
            flow = early[comp, i] + halo * edge0[comp, i]
            value = (1.0 - RELAXATION) * v0[comp, i + 1, rows, :] + scale * flow
            v1[comp, i + 1, rows, :] = value
            keep_end(2, comp, i, value)
            yield value

    def send_ends(r):
        s = r - 1
        return lambda: send_x(r, x_send.at[s, 0], x_recv.at[s, 0], x_send.at[s, 1], x_recv.at[s, 1])

    def keep_end(r, comp, i, value):
        if i == cx - 1:
            x_send[r - 1, 0, comp] = value
        if i == 0:
            x_send[r - 1, 1, comp] = value

    waits = shell_pass(late_one, edges_one, values_one, 2, send_ends(2), STAGES)

    wait_gx()
    low_y, high_y = flag(has_down[1]), flag(has_up[1])
    gx_counts = (cx // 2, cx // 4, cx // 8)
    for level, buf in enumerate((cx1, cx2, cx3)):
        buf[1, rows, :] = buf[1, rows, :] + gx_recv[0, level]
        last = gx_counts[level]
        buf[last, rows, :] = buf[last, rows, :] + gx_recv[1, level]

    def restrict_rows(source, target, count):
        size = count + 2
        a, b, c, d = (source[pl.ds(PAD - 3 + s, size, stride=2), :] for s in range(4))
        target[PAD - 1 : PAD - 1 + size, :] = 0.125 * (a + d) + 0.375 * (b + c)
        target[PAD - 1 : PAD, :] = target[PAD - 1 : PAD, :] * low_y
        target[PAD + count : PAD + count + 1, :] = target[PAD + count : PAD + count + 1, :] * high_y

    row = 0
    ghost_rows = []
    for level, (buf, steps) in enumerate(((cx1, (t1,)), (cx2, (t2a, t2b)), (cx3, (t3a, t3b, t3c)))):
        for k in range(gx_counts[level]):
            source = buf.at[k + 1]
            for depth, target in enumerate(steps):
                restrict_rows(source, target.at[k], cy >> (depth + 1))
                source = target.at[k]
            count = cy >> len(steps)
            gy_send[1, row : row + 1, :] = source[PAD - 1 : PAD, :]
            gy_send[0, row : row + 1, :] = source[PAD + count : PAD + count + 1, :]
            ghost_rows.append((steps[-1], k, count, row))
            row += 1
    wait_gy = exchange(13, 1, gy_send.at[0], gy_recv.at[0], gy_send.at[1], gy_recv.at[1])

    def around_inner(buf, comp, i):
        plane = buf.at[comp, i + 1]
        centre = plane[rows, :]
        return centre, (
            buf[comp, i, rows, :],
            buf[comp, i + 2, rows, :],
            plane[PAD - 1 : PAD - 1 + cy, :],
            plane[PAD + 1 : PAD + 1 + cy, :],
            pltpu.roll(centre, 1, 1),
            pltpu.roll(centre, cz - 1, 1),
        )

    def flow_inner(buf, comp, i):
        centre, near = around_inner(buf, comp, i)
        flow = 2.0 * forc[comp, i]
        for n in range(6):
            flow = flow + faces[n, i] * near[n]
        return centre, flow

    def early_two(i, carry):
        z_scaled[i] = weight[i] * z_faces[i]
        for comp in range(3):
            centre, flow = flow_inner(v1, comp, i)
            early[comp, i] = (1.0 - RELAXATION) * centre + weight[i] * flow
        return carry

    def late_planes(r, scaled):
        for side, i, face in ((0, 0, 0), (1, cx - 1, 1)):
            factor = faces[face, i]
            if scaled:
                factor = factor * weight[i]
            for comp in range(3):
                early[comp, i] = early[comp, i] + factor * x_recv[r - 1, side, comp]

    def late_rows(r, scaled):
        def fix(i):
            for side, face, at in ((0, 2, 0), (1, 3, cy - 1)):
                factor = faces[face, i, at : at + 1, :]
                if scaled:
                    factor = factor * weight[i, at : at + 1, :]
                for comp in range(3):
                    halo = y_recv[r, side, comp, pl.ds(i, 1), :]
                    early[comp, i, at : at + 1, :] = early[comp, i, at : at + 1, :] + factor * halo

        return fix

    lax.fori_loop(0, cx, early_two, 0, unroll=UNROLL)
    for wait in waits:
        wait()
    halos2 = halos_z(2)
    late_planes(2, True)

    def edges_two(i):
        return [edge_at(halos2, i, comp * cx + i) for comp in range(3)]

    def values_two(i, edges):
        factor = z_scaled[i]
        for comp in range(3):
            value = early[comp, i] + factor * edges[comp]
            v2[comp, i + 1, rows, :] = value
            keep_end(3, comp, i, value)
            yield value

    waits = shell_pass(late_rows(2, True), edges_two, values_two, 3, send_ends(3), STAGES)

    wait_gy()
    for buf, k, count, row in ghost_rows:
        buf[k, PAD : PAD + 1, :] = buf[k, PAD : PAD + 1, :] + gy_recv[0, row : row + 1, :]
        last = PAD + count - 1
        buf[k, last : last + 1, :] = buf[k, last : last + 1, :] + gy_recv[1, row : row + 1, :]
    mats_in.wait()
    off_low, off_high = 1.0 - flag(has_down[2]), 1.0 - flag(has_up[2])
    results = []
    groups = []
    lane8 = lax.broadcasted_iota(jnp.int32, (8, cz), 1)
    packed = jnp.zeros((8, cz), jnp.float32)
    for level, buf in enumerate((t1, t2b, t3c)):
        count = gx_counts[level]
        height = max(8, cy >> (level + 1))
        matrix = mats[0, level] - off_low * mats[1, level] - off_high * mats[2, level]
        data = buf[:, PAD : PAD + height, :].reshape(count * height, cz)
        result = jnp.dot(data, matrix, preferred_element_type=jnp.float32, precision=HIGHEST)
        for part in range(count * height // 8):
            g = len(groups)
            piece = result[8 * part : 8 * part + 8, :]
            groups.append((level, 8 * part // height, 8 * part % height, piece))
            shifted = pltpu.roll(piece, (2 * g - GHOST) % cz, 1)
            packed = jnp.where((lane8 == 2 * g) | (lane8 == 2 * g + 1), shifted, packed)
    gz_send[...] = packed
    wait_gz = exchange(14, 2, gz_send, gz_recv.at[0], gz_send, gz_recv.at[1])

    def early_misfit(i, carry):
        for comp in range(3):
            centre, flow = flow_inner(v2, comp, i)
            smooth_ref[comp, i] = centre
            early[comp, i] = flow - diag[i] * centre
        return carry

    if near_only:
        for peer in z_line:
            pl.semaphore_signal(hello_sem, inc=1, device_id=peer, device_id_type=MESH)
    lax.fori_loop(0, cx, early_misfit, 0, unroll=UNROLL)
    for wait in waits:
        wait()
    halos3 = halos_z(3)
    late_planes(3, False)
    squares = []

    def edges_three(i):
        return [edge_of(halos3[1], comp * cx + i) for comp in range(3)]

    def values_three(i, edges):
        total = None
        for comp in range(3):
            value = 0.5 * (early[comp, i] + z_faces[i] * edges[comp])
            misfit_ref[comp, i] = value
            total = value * value if total is None else total + value * value
            yield value
        squares.append(total if not squares else squares[-1] + total)

    shell_pass(late_rows(3, False), edges_three, values_three, None, None, STAGES)
    part = jnp.sum(squares[-1], axis=0, keepdims=True)

    def gather(slots, mine, value, peers, sems):
        slots[mine] = value
        for peer in peers:
            pltpu.make_async_remote_copy(
                slots.at[mine], slots.at[mine], sems.at[0], sems.at[1],
                device_id=peer, device_id_type=MESH,
            ).start()
        others = slots.at[pl.ds(0, len(peers))]
        return pltpu.make_async_remote_copy(
            others, others, sems.at[0], sems.at[1], device_id=peers[0], device_id_type=MESH
        )

    def total_of(slots):
        parts = [slots[n] for n in range(slots.shape[0])]
        while len(parts) > 1:
            parts = [sum(parts[n : n + 2]) for n in range(0, len(parts), 2)]
        return parts[0]

    if near_only:
        pl.semaphore_wait(hello_sem, nz - 1)
    plane_copies = gather(sums_xy, me_first, part, first_peers(), plane_sem)

    wait_gz()
    low_part, high_part = gz_recv[0], gz_recv[1]
    for g, (level, k, at, piece) in enumerate(groups):
        width = cz >> (level + 1)
        height = cy >> (level + 1)
        piece = piece + jnp.where(lane8 == 0, pltpu.roll(low_part, (cz - 2 * g - 1) % cz, 1), 0.0)
        piece = piece + jnp.where(
            lane8 == width - 1, pltpu.roll(high_part, (width - 1 - 2 * g) % cz, 1), 0.0
        )
        target = (one_ref, two_ref, three_ref)[level]
        size = min(8, height - at)
        target[k, at : at + size, :] = piece[:size, :width]

    for condition, copy in started:
        pl.when(condition)(copy.wait_send)
    plane_copies.wait()
    whole = total_of(sums_xy)
    if not one_stage:
        gather(sums_z, iz, whole, line_peers, line_sem).wait()
        whole = total_of(sums_z)
    rms_ref[...] = jnp.broadcast_to(whole, rms_ref.shape)


def writer(cells_all, *refs):
    rms, sems = refs[14], refs[15]
    copies = [pltpu.make_async_copy(refs[n], refs[7 + n], sems.at[n]) for n in (0, 5, 1, 2, 3, 4)]
    copies.append(pltpu.make_async_copy(rms, refs[13], sems.at[6]))
    for copy in copies[:6]:
        copy.start()
    whole = jnp.sum(refs[6][0:1, :], axis=1, keepdims=True)
    rms[...] = jnp.sqrt(whole / cells_all)
    copies[6].start()
    for copy in copies:
        copy.wait()


def per_device(velocity, forcing, phase_block, prefactor, yield_stress):
    _, cx, cy, cz = velocity.shape
    nx, ny, nz = lax.axis_size("gx"), lax.axis_size("gy"), lax.axis_size("gz")
    f32 = jnp.float32
    sizes = (nx, ny, nz, cx, cy, cz, prefactor.shape[0])
    mats = jnp.asarray(coarse_matrices(cz))
    blocks = phase_block.reshape(phase_block.shape[0] * phase_block.shape[1], phase_block.shape[2])
    tall = cy + 2 * PAD
    firsts = nx * ny * nz if nx * ny * nz <= ONE_STAGE else nx * ny
    ghosts = cx // 2 + cx // 4 + cx // 8
    ghosts += -ghosts % 8
    hbm = pl.BlockSpec(memory_space=pltpu.HBM)
    vmem = pl.BlockSpec(memory_space=pltpu.VMEM)
    v = pltpu.VMEM
    field = v((3, cx + 2, tall, cz), f32)
    dma = pltpu.SemaphoreType.DMA
    operands = (velocity, forcing, mats, blocks, prefactor, yield_stress)
    outs = pl.pallas_call(
        functools.partial(kernel, sizes),
        out_shape=(
            jax.ShapeDtypeStruct(velocity.shape, f32),
            jax.ShapeDtypeStruct((cx, cy, cz), f32),
            jax.ShapeDtypeStruct((cx // 2, cy // 2, cz // 2), f32),
            jax.ShapeDtypeStruct((cx // 4, cy // 4, cz // 4), f32),
            jax.ShapeDtypeStruct((cx // 8, cy // 8, cz // 8), f32),
            jax.ShapeDtypeStruct(velocity.shape, f32),
            jax.ShapeDtypeStruct((8, cz), f32),
        ),
        in_specs=[hbm] * 6,
        out_specs=(vmem,) * 7,
        scratch_shapes=[
            field,
            field,
            field,
            v((cx + 2, tall, cz), f32),
            v((3, cx, cy, cz), f32),
            v(mats.shape, f32),
            v(blocks.shape, blocks.dtype),
            pltpu.SMEM(prefactor.shape, f32),
            pltpu.SMEM(yield_stress.shape, f32),
            v((6, cx, cy, cz), f32),
            v((cx, cy, cz), f32),
            v((cx, cy, cz), f32),
            v((3, cx, cy, cz), f32),
            v((3, cx, cy, cz), f32),
            v((cx, cy, cz), f32),
            v((cx, cy, cz), f32),
            v((cx // BLOCK, cy, cz), f32),
            v((cx // BLOCK, cy, cz), f32),
            v((3, 2, 3, cy, cz), f32),
            v((3, 2, 3, cy, cz), f32),
            v((2, cy, cz), f32),
            v((4, 2, 3, cx, cz), f32),
            v((4, 2, 3, cx, cz), f32),
            v((4, cy, cz), f32),
            v((4, 2, cy, cz), f32),
            v((cx // 2 + 2, tall, cz), f32),
            v((cx // 4 + 2, tall, cz), f32),
            v((cx // 8 + 2, tall, cz), f32),
            v((2, 3, cy, cz), f32),
            v((2, 3, cy, cz), f32),
            v((cx // 2, tall, cz), f32),
            v((cx // 4, tall, cz), f32),
            v((cx // 4, tall, cz), f32),
            v((cx // 8, tall, cz), f32),
            v((cx // 8, tall, cz), f32),
            v((cx // 8, tall, cz), f32),
            v((2, ghosts, cz), f32),
            v((2, ghosts, cz), f32),
            v((8, cz), f32),
            v((2, 8, cz), f32),
            v((firsts, 1, cz), f32),
            v((nz, 1, cz), f32),
            dma((10,)),
            dma((15, 2)),
            dma((15, 2)),
            dma((2,)),
            dma((2,)),
            pltpu.SemaphoreType.REGULAR,
        ],
        compiler_params=pltpu.CompilerParams(
            collective_id=0, has_side_effects=True, vmem_limit_bytes=40 * 1024 * 1024
        ),
    )(*(pltpu.with_memory_space_constraint(a, pltpu.HBM) for a in operands))
    outs = pl.pallas_call(
        functools.partial(writer, float(3 * cx * nx * cy * ny * cz * nz)),
        out_shape=tuple(jax.ShapeDtypeStruct(out.shape, f32) for out in outs[:6])
        + (jax.ShapeDtypeStruct((1, 1), f32),),
        in_specs=[vmem] * 7,
        out_specs=(hbm,) * 7,
        scratch_shapes=[v((1, 1), f32), dma((7,))],
        compiler_params=pltpu.CompilerParams(vmem_limit_bytes=8 * 1024 * 1024),
    )(*outs)
    return outs[:6] + (outs[6].reshape(()),)


def solution(mesh):
    grid = P("gx", "gy", "gz")
    vector = P(None, "gx", "gy", "gz")
    return jax.shard_map(
        per_device,
        mesh=mesh,
        in_specs=(vector, vector, grid, P(), P()),
        out_specs=(vector, grid, grid, grid, grid, vector, P()),
        check_vma=False,
    )
```

```python
import functools

import jax
import jax.numpy as jnp
import numpy as np
from jax import lax
from jax.experimental import pallas as pl
from jax.experimental.pallas import tpu as pltpu
from jax.sharding import PartitionSpec as P

BLOCK = 4
RELAXATION = 0.8
PAD = 8
GHOST = 64
UNROLL = 4
STAGES = (3, 0, 1)
STAGES_VISC = (2, 2, 2)
ONE_STAGE = 32
ROUNDS = 4
MESH = pl.DeviceIdType.MESH
HIGHEST = lax.Precision.HIGHEST


def coarse_matrices(length):
    def chain(low_edge, high_edge):
        field = np.eye(length)
        found = []
        first = 0
        for _ in range(3):
            count = length >> (len(found) + 1)
            out = np.zeros((length, count + 2))
            for k in range(-1, count + 1):
                for shift, weight in ((-1, 1.0), (0, 3.0), (1, 3.0), (2, 1.0)):
                    source = 2 * k + shift - first
                    if 0 <= source < field.shape[1]:
                        out[:, k + 1] += weight / 8.0 * field[:, source]
            if low_edge:
                out[:, 0] = 0.0
            if high_edge:
                out[:, -1] = 0.0
            placed = np.zeros((length, length))
            placed[:, :count] = out[:, 1:-1]
            placed[:, GHOST] = out[:, 0]
            placed[:, GHOST + 1] = out[:, -1]
            found.append(placed)
            field = out
            first = -1
        return np.stack(found)

    inner = chain(False, False)
    return np.stack([inner, inner - chain(True, False), inner - chain(False, True)]).astype(np.float32)


def kernel(
    sizes,
    vel_hbm,
    forc_hbm,
    mats_hbm,
    phase_hbm,
    pref_hbm,
    yield_hbm,
    smooth_ref,
    visc_ref,
    one_ref,
    two_ref,
    three_ref,
    misfit_ref,
    rms_ref,
    v0,
    v1,
    v2,
    visc,
    forc,
    mats,
    phase_ref,
    pref_ref,
    yield_ref,
    faces,
    z_faces,
    z_scaled,
    edge0,
    early,
    weight,
    diag,
    pref_cells,
    yield_cells,
    x_send,
    x_recv,
    visc_x,
    y_send,
    y_recv,
    z_send,
    z_recv,
    cx1,
    cx2,
    cx3,
    gx_send,
    gx_recv,
    t1,
    t2a,
    t2b,
    t3a,
    t3b,
    t3c,
    gy_send,
    gy_recv,
    gz_send,
    gz_recv,
    sums_xy,
    sums_z,
    local_sem,
    send_sem,
    recv_sem,
    plane_sem,
    line_sem,
    hello_sem,
):
    nx, ny, nz, cx, cy, cz, phases = sizes
    ix, iy, iz = lax.axis_index("gx"), lax.axis_index("gy"), lax.axis_index("gz")
    rows = pl.ds(PAD, cy)

    ends_in = [
        pltpu.make_async_copy(vel_hbm.at[:, cx - 1], x_send.at[0, 0], local_sem.at[0]),
        pltpu.make_async_copy(vel_hbm.at[:, 0], x_send.at[0, 1], local_sem.at[1]),
    ]
    vel_in = [
        pltpu.make_async_copy(vel_hbm.at[comp], v0.at[comp, pl.ds(1, cx), rows, :], local_sem.at[2 + comp])
        for comp in range(3)
    ]
    forc_in = pltpu.make_async_copy(forc_hbm, forc, local_sem.at[5])
    mats_in = pltpu.make_async_copy(mats_hbm, mats, local_sem.at[6])
    phase_in = pltpu.make_async_copy(phase_hbm, phase_ref, local_sem.at[7])
    pref_in = pltpu.make_async_copy(pref_hbm, pref_ref, local_sem.at[8])
    yield_in = pltpu.make_async_copy(yield_hbm, yield_ref, local_sem.at[9])
    for copy in ends_in + vel_in:
        copy.start()

    barrier = pltpu.get_barrier_semaphore()
    one_stage = nx * ny * nz <= ONE_STAGE
    me_xy = ix * ny + iy
    me_first = me_xy * nz + iz if one_stage else me_xy

    def first_peers():
        if one_stage:
            others = [lax.rem(me_first + k, nx * ny * nz) for k in range(1, nx * ny * nz)]
            return [(o // (ny * nz), lax.rem(o // nz, ny), lax.rem(o, nz)) for o in others]
        others = [lax.rem(me_first + k, nx * ny) for k in range(1, nx * ny)]
        return [(o // ny, lax.rem(o, ny), iz) for o in others]

    line_peers = [] if one_stage else [(ix, iy, lax.rem(iz + k, nz)) for k in range(1, nz)]
    has_up = (ix < nx - 1, iy < ny - 1, iz < nz - 1)
    has_down = (ix > 0, iy > 0, iz > 0)
    up_ids = (
        (lax.rem(ix + 1, nx), iy, iz),
        (ix, lax.rem(iy + 1, ny), iz),
        (ix, iy, lax.rem(iz + 1, nz)),
    )
    down_ids = (
        (lax.rem(ix + nx - 1, nx), iy, iz),
        (ix, lax.rem(iy + ny - 1, ny), iz),
        (ix, iy, lax.rem(iz + nz - 1, nz)),
    )
    z_line = [(ix, iy, lax.rem(iz + k, nz)) for k in range(1, nz)]
    steps = [nx - 1, ny - 1, nz - 1] if one_stage else [nx - 1, ny - 1]
    near_only = one_stage and steps[0] + steps[1] <= ROUNDS and steps[2] <= ROUNDS
    if near_only:
        met = 0
        for there, peer in list(zip(has_up, up_ids)) + list(zip(has_down, down_ids)):
            met = met + there.astype(jnp.int32)

            @pl.when(there)
            def _():
                pl.semaphore_signal(barrier, inc=1, device_id=peer, device_id_type=MESH)
    else:
        if sum(steps) - max(steps) <= ROUNDS:
            greeted = [(lax.rem(ix + k, nx), iy, iz) for k in range(1, nx)]
            greeted += [(ix, lax.rem(iy + k, ny), iz) for k in range(1, ny)]
            greeted += z_line
        else:
            greeted = first_peers() + line_peers
        met = len(greeted)
        for peer in greeted:
            pl.semaphore_signal(barrier, inc=1, device_id=peer, device_id_type=MESH)
    for copy in (phase_in, pref_in, yield_in):
        copy.start()

    def clear(ref):
        ref[...] = jnp.zeros(ref.shape, jnp.float32)

    for side, present in ((0, has_down), (1, has_up)):
        @pl.when(jnp.logical_not(present[0]))
        def _():
            for r in range(3):
                clear(x_recv.at[r, side])
            clear(visc_x.at[side])
            clear(gx_recv.at[side])

        @pl.when(jnp.logical_not(present[1]))
        def _():
            for r in range(4):
                clear(y_recv.at[r, side])
            clear(gy_recv.at[side])

        @pl.when(jnp.logical_not(present[2]))
        def _():
            for r in range(4):
                clear(z_recv.at[r, side])
            clear(gz_recv.at[side])

    for buf in [v.at[comp] for v in (v0, v1, v2) for comp in range(3)] + [visc]:
        clear(buf.at[0, rows])
        clear(buf.at[cx + 1, rows])
        clear(buf.at[pl.ds(1, cx), pl.ds(PAD - 1, 1)])
        clear(buf.at[pl.ds(1, cx), pl.ds(PAD + cy, 1)])

    lane = lax.broadcasted_iota(jnp.int32, (cy, cz), 1)
    odd_lane = lax.rem(lane, 2) == 1
    lane_pair = lax.rem(lane + (cz - 1), cz) // 2
    own_pair = lane // 2
    first_lane = lane == 0
    last_lane = lane == cz - 1
    end_lane = first_lane | last_lane

    started = []

    def exchange(slot, dim, up_src, up_dst, down_src, down_dst):
        up = pltpu.make_async_remote_copy(
            up_src, up_dst, send_sem.at[slot, 0], recv_sem.at[slot, 0],
            device_id=up_ids[dim], device_id_type=MESH,
        )
        down = pltpu.make_async_remote_copy(
            down_src, down_dst, send_sem.at[slot, 1], recv_sem.at[slot, 1],
            device_id=down_ids[dim], device_id_type=MESH,
        )
        pl.when(has_up[dim])(up.start)
        pl.when(has_down[dim])(down.start)
        started.append((has_up[dim], up))
        started.append((has_down[dim], down))

        def wait():
            pl.when(has_down[dim])(up.wait_recv)
            pl.when(has_up[dim])(down.wait_recv)

        return wait

    def send_x(r, last, low, first, high):
        return exchange(3 * r, 0, last, low, first, high)

    def send_y(r):
        held = pl.ds(0, 1 if r == 1 else 3)
        return exchange(
            3 * r + 1, 1,
            y_send.at[r, 0, held], y_recv.at[r, 0, held],
            y_send.at[r, 1, held], y_recv.at[r, 1, held],
        )

    def send_z(r):
        height = pl.ds(0, visc_rows if r == 1 else cy)
        return exchange(
            3 * r + 2, 2,
            z_send.at[r, height], z_recv.at[r, 0, height],
            z_send.at[r, height], z_recv.at[r, 1, height],
        )

    def send_yz(r):
        sent_z = send_z(r)
        return [send_y(r), sent_z]

    def pack(r, comp, i, value, packed):
        y_send[r, 0, comp, pl.ds(i, 1), :] = value[cy - 1 : cy, :]
        y_send[r, 1, comp, pl.ds(i, 1), :] = value[0:1, :]
        place = 2 * (comp * cx + i) + 1
        return jnp.where(lane_pair == comp * cx + i, pltpu.roll(value, place + 1, 1), packed)

    def unpack_y(r, buf, comps):
        def body(i, carry):
            for comp in range(comps):
                target = buf.at[comp, i + 1] if comps == 3 else buf.at[i + 1]
                target[PAD - 1 : PAD, :] = y_recv[r, 0, comp, pl.ds(i, 1), :]
                target[PAD + cy : PAD + cy + 1, :] = y_recv[r, 1, comp, pl.ds(i, 1), :]
            return carry

        lax.fori_loop(0, cx, body, 0)

    visc_rows = 8 if 2 * cx * (cy // 8) <= cz else cy

    def halos_z(r, height):
        low, high = z_recv[r, 0, :height], z_recv[r, 1, :height]
        odd = odd_lane[:height]
        if r == 3:
            return None, jnp.where(odd, pltpu.roll(low, 1, 1), pltpu.roll(high, cz - 1, 1))
        return jnp.where(odd, low, high), jnp.where(odd, low, pltpu.roll(high, cz - 2, 1))

    for copy in ends_in:
        copy.wait()
    pl.semaphore_wait(barrier, met)
    waits = [send_x(0, x_send.at[0, 0], x_recv.at[0, 0], x_send.at[0, 1], x_recv.at[0, 1])]
    nothing = jnp.zeros((cy, cz), jnp.float32)
    packed = nothing
    for copy in vel_in:
        copy.wait()
    for comp in range(3):
        for i in range(cx):
            packed = pack(0, comp, i, v0[comp, i + 1, rows, :], packed)
    z_send[0] = packed
    waits += send_yz(0)
    forc_in.start()
    mats_in.start()

    phase_in.wait()
    pref_in.wait()
    yield_in.wait()
    blocks = phase_ref[...].astype(jnp.float32)
    n_rows, n_blocks = blocks.shape
    spread_z = lax.broadcasted_iota(jnp.int32, (n_blocks, cz), 1) // BLOCK
    spread_z = (spread_z == lax.broadcasted_iota(jnp.int32, (n_blocks, cz), 0)).astype(jnp.float32)
    spread_y = lax.broadcasted_iota(jnp.int32, (n_rows * BLOCK, n_rows), 0) // BLOCK
    spread_y = (
        spread_y == lax.broadcasted_iota(jnp.int32, (n_rows * BLOCK, n_rows), 1)
    ).astype(jnp.float32)
    cells = jnp.dot(blocks, spread_z, preferred_element_type=jnp.float32, precision=HIGHEST)
    cells = jnp.dot(spread_y, cells, preferred_element_type=jnp.float32, precision=HIGHEST)
    for bx in range(cx // BLOCK):
        phase = cells[bx * cy : (bx + 1) * cy, :]
        pref_value = jnp.zeros((cy, cz), jnp.float32)
        yield_value = jnp.zeros((cy, cz), jnp.float32)
        for p in range(phases):
            here = jnp.abs(phase - float(p)) < 0.5
            pref_value = jnp.where(here, pref_ref[p], pref_value)
            yield_value = jnp.where(here, yield_ref[p], yield_value)
        pref_cells[bx] = pref_value
        yield_cells[bx] = 0.5 * yield_value
    for buf in (cx1, cx2, cx3):
        for edge in (0, PAD + cy):
            buf[:, edge : edge + PAD, :] = jnp.zeros((buf.shape[0], PAD, cz), jnp.float32)
    for buf in (t1, t2a, t2b, t3a, t3b, t3c):
        buf[...] = jnp.zeros(buf.shape, jnp.float32)

    along_x, along_y, along_z = (0, 3, 4), (3, 1, 5), (4, 5, 2)

    def early_strain(i, carry):
        found = {}
        for comp in range(3):
            plane = v0.at[comp, i + 1]
            centre = plane[rows, :]
            low = jnp.where(first_lane, 0.0, pltpu.roll(centre, 1, 1))
            high = jnp.where(last_lane, 0.0, pltpu.roll(centre, cz - 1, 1))
            for n, jump in (
                (along_x[comp], v0[comp, i + 2, rows, :] - v0[comp, i, rows, :]),
                (along_y[comp], plane[PAD + 1 : PAD + 1 + cy, :] - plane[PAD - 1 : PAD - 1 + cy, :]),
                (along_z[comp], high - low),
            ):
                found[n] = found[n] + jump if n in found else jump
        for n in range(6):
            faces[n, i] = found[n]
        return carry

    lax.fori_loop(0, cx, early_strain, 0, unroll=UNROLL)
    wait_x, *others = waits
    for wait in others:
        wait()
    merged0 = halos_z(0, cy)[1]
    signed0 = jnp.where(odd_lane, -merged0, merged0)

    def gate_strain():
        wait_x()
        for comp in range(3):
            n = along_x[comp]
            faces[n, 0] = faces[n, 0] - x_recv[0, 0, comp]
            faces[n, cx - 1] = faces[n, cx - 1] + x_recv[0, 1, comp]

    def late_strain(i):
        for comp in range(3):
            n = along_y[comp]
            faces[n, i, 0:1, :] = faces[n, i, 0:1, :] - y_recv[0, 0, comp, pl.ds(i, 1), :]
            faces[n, i, cy - 1 : cy, :] = faces[n, i, cy - 1 : cy, :] + y_recv[0, 1, comp, pl.ds(i, 1), :]

    inner, outer = list(range(1, cx - 1)), [0, cx - 1]

    def shell_pass(order, gate, fix, edge, value_of, r, send_ends, stages):
        ahead, hold, behind = stages
        height, parts = (visc_rows, cy // visc_rows) if r == 1 else (cy, 1)
        pairs = lane_pair[:height]
        packed = nothing[:height]
        edges, values, rolled = {}, {}, {}
        sent = None
        ends_at = [n for n, i in enumerate(order) if i in outer]
        for t in range(cx + ahead + hold + behind):
            if t < cx:
                edges[t] = edge(order[t])
                fix(order[t])
            n = t - ahead
            if 0 <= n < cx:
                i = order[n]
                if n == ends_at[0]:
                    gate()
                values[n] = []
                for comp, value in enumerate(value_of(i, edges.pop(n))):
                    if r is not None:
                        y_send[r, 0, comp, pl.ds(i, 1), :] = value[cy - 1 : cy, :]
                        y_send[r, 1, comp, pl.ds(i, 1), :] = value[0:1, :]
                        for part in range(parts if r != 3 else 0):
                            piece = value[part * height : (part + 1) * height, :]
                            values[n].append(((comp + part) * cx + i, piece))
                if n == ends_at[1] and send_ends is not None:
                    sent = send_ends()
            n = t - ahead - hold
            if 0 <= n < cx:
                rolled[n] = [(place, turn(value, 2 * place + 2)) for place, value in values.pop(n)]
            n = t - ahead - hold - behind
            if 0 <= n < cx:
                for place, value in rolled.pop(n):
                    packed = jnp.where(pairs == place, value, packed)
        if r is None or r == 3:
            return sent
        z_send[r, pl.ds(0, height)] = packed
        return [sent] + send_yz(r)

    def turn(value, amount):
        return pltpu.roll(value, amount % cz, 1)

    def edge_of(merged, place):
        return turn(merged, cz - 1 - 2 * place)

    def edge_visc(halos, i):
        mixed, merged = halos
        places = [part * cx + i for part in range(cy // visc_rows)]
        if i in outer:
            first = first_lane[:visc_rows]
            found = [jnp.where(first, edge_of(mixed, p), edge_of(mixed, p + 1)) for p in places]
        else:
            found = [edge_of(merged, p) for p in places]
        return jnp.concatenate(found, axis=0) if len(found) > 1 else found[0]

    def edges_visc(i):
        return [edge_of(signed0, comp * cx + i) for comp in range(3)]

    def values_visc(i, edges):
        strain = [faces[n, i] for n in range(6)]
        for comp in range(3):
            n = along_z[comp]
            strain[n] = strain[n] + jnp.where(end_lane, edges[comp], 0.0)
        squared = [term * term for term in strain]
        straight = squared[0] + squared[1] + squared[2]
        skew = squared[3] + squared[4] + squared[5]
        invariant = 1.0 + (0.125 * straight + 0.0625 * skew)
        creeping = pref_cells[i // BLOCK] * jnp.exp(jnp.log(invariant) * (-1.0 / 3.0))
        plastic = yield_cells[i // BLOCK] * lax.rsqrt(invariant)
        value = jnp.minimum(creeping, plastic)
        visc[i + 1, rows, :] = value
        yield value

    def send_visc():
        return send_x(1, visc.at[cx, rows, :], visc_x.at[0], visc.at[1, rows, :], visc_x.at[1])

    waits = shell_pass(inner + outer, gate_strain, late_strain, edges_visc, values_visc, 1, send_visc, STAGES_VISC)
    for comp in range(3):
        v0[comp, 0, rows, :] = x_recv[0, 0, comp]
        v0[comp, cx + 1, rows, :] = x_recv[0, 1, comp]
    unpack_y(0, v0, 3)

    def flag(condition):
        return jnp.where(condition, 1.0, 0.0).astype(jnp.float32)

    def restrict_planes(source, first, held, count, target, level):
        for k in range(-1, count + 1):
            total = None
            for shift, factor in ((-1, 0.125), (0, 0.375), (1, 0.375), (2, 0.125)):
                at = 2 * k + shift - first
                if 0 <= at < held:
                    term = factor * source[at, rows, :]
                    total = term if total is None else total + term
            if k == -1:
                total = total * flag(has_down[0])
                gx_send[1, level] = total
            if k == count:
                total = total * flag(has_up[0])
                gx_send[0, level] = total
            target[k + 1, rows, :] = total

    restrict_planes(visc.at[pl.ds(1, cx)], 0, cx, cx // 2, cx1, 0)
    restrict_planes(cx1, -1, cx // 2 + 2, cx // 4, cx2, 1)
    restrict_planes(cx2, -1, cx // 4 + 2, cx // 8, cx3, 2)
    wait_gx = exchange(12, 0, gx_send.at[0], gx_recv.at[0], gx_send.at[1], gx_recv.at[1])

    forc_in.wait()

    def early_one(i, carry):
        plane = visc.at[i + 1]
        centre = plane[rows, :]
        visc_ref[i] = centre
        sides = (
            centre + visc[i, rows, :],
            centre + visc[i + 2, rows, :],
            centre + plane[PAD - 1 : PAD - 1 + cy, :],
            centre + plane[PAD + 1 : PAD + 1 + cy, :],
            centre + jnp.where(first_lane, 0.0, pltpu.roll(centre, 1, 1)),
            centre + jnp.where(last_lane, 0.0, pltpu.roll(centre, cz - 1, 1)),
        )
        for n in range(4):
            faces[n, i] = sides[n]
        faces[4, i] = jnp.where(first_lane, 0.0, sides[4])
        faces[5, i] = jnp.where(last_lane, 0.0, sides[5])
        diag[i] = (sides[0] + sides[1]) + (sides[2] + sides[3]) + (sides[4] + sides[5])
        for comp in range(3):
            plane = v0.at[comp, i + 1]
            centre = plane[rows, :]
            edge = edge_of(merged0, comp * cx + i)
            edge0[comp, i] = edge
            near = (
                v0[comp, i, rows, :],
                v0[comp, i + 2, rows, :],
                plane[PAD - 1 : PAD - 1 + cy, :],
                plane[PAD + 1 : PAD + 1 + cy, :],
                jnp.where(first_lane, edge, pltpu.roll(centre, 1, 1)),
                jnp.where(last_lane, edge, pltpu.roll(centre, cz - 1, 1)),
            )
            flow = 2.0 * forc[comp, i]
            for n in range(6):
                flow = flow + sides[n] * near[n]
            early[comp, i] = flow
        return carry

    lax.fori_loop(0, cx, early_one, 0, unroll=UNROLL)
    for wait in waits:
        wait()
    halos1 = halos_z(1, visc_rows)

    for side, i, face, halo_plane in ((0, 0, 0, 0), (1, cx - 1, 1, cx + 1)):
        halo = visc_x[side]
        faces[face, i] = faces[face, i] + halo
        diag[i] = diag[i] + halo
        for comp in range(3):
            early[comp, i] = early[comp, i] + halo * v0[comp, halo_plane, rows, :]

    def late_one(i):
        ends = ((0, 2, 0, PAD - 1), (1, 3, cy - 1, PAD + cy))
        for side, face, at, row in ends:
            halo = y_recv[1, side, 0, pl.ds(i, 1), :]
            faces[face, i, at : at + 1, :] = faces[face, i, at : at + 1, :] + halo
            diag[i, at : at + 1, :] = diag[i, at : at + 1, :] + halo
            for comp in range(3):
                near = v0[comp, i + 1, row : row + 1, :]
                early[comp, i, at : at + 1, :] = early[comp, i, at : at + 1, :] + halo * near

    def edges_one(i):
        return [edge_visc(halos1, i)]

    def values_one(i, edges):
        halo = jnp.where(end_lane, edges[0], 0.0)
        total = diag[i] + halo
        scale = RELAXATION / total
        diag[i] = total
        weight[i] = scale
        z_faces[i] = jnp.where(end_lane, visc[i + 1, rows, :] + halo, 0.0)
        for comp in range(3):
            flow = early[comp, i] + halo * edge0[comp, i]
            value = (1.0 - RELAXATION) * v0[comp, i + 1, rows, :] + scale * flow
            v1[comp, i + 1, rows, :] = value
            keep_end(2, comp, i, value)
            yield value

    def send_ends(r):
        s = r - 1
        return lambda: send_x(r, x_send.at[s, 0], x_recv.at[s, 0], x_send.at[s, 1], x_recv.at[s, 1])

    def keep_end(r, comp, i, value):
        if i == cx - 1:
            x_send[r - 1, 0, comp] = value
        if i == 0:
            x_send[r - 1, 1, comp] = value

    waits = shell_pass(outer + inner, lambda: None, late_one, edges_one, values_one, 2, send_ends(2), STAGES)

    wait_gx()
    low_y, high_y = flag(has_down[1]), flag(has_up[1])
    gx_counts = (cx // 2, cx // 4, cx // 8)
    for level, buf in enumerate((cx1, cx2, cx3)):
        buf[1, rows, :] = buf[1, rows, :] + gx_recv[0, level]
        last = gx_counts[level]
        buf[last, rows, :] = buf[last, rows, :] + gx_recv[1, level]

    def restrict_rows(source, target, count):
        size = count + 2
        a, b, c, d = (source[pl.ds(PAD - 3 + s, size, stride=2), :] for s in range(4))
        target[PAD - 1 : PAD - 1 + size, :] = 0.125 * (a + d) + 0.375 * (b + c)
        target[PAD - 1 : PAD, :] = target[PAD - 1 : PAD, :] * low_y
        target[PAD + count : PAD + count + 1, :] = target[PAD + count : PAD + count + 1, :] * high_y

    row = 0
    ghost_rows = []
    for level, (buf, steps) in enumerate(((cx1, (t1,)), (cx2, (t2a, t2b)), (cx3, (t3a, t3b, t3c)))):
        for k in range(gx_counts[level]):
            source = buf.at[k + 1]
            for depth, target in enumerate(steps):
                restrict_rows(source, target.at[k], cy >> (depth + 1))
                source = target.at[k]
            count = cy >> len(steps)
            gy_send[1, row : row + 1, :] = source[PAD - 1 : PAD, :]
            gy_send[0, row : row + 1, :] = source[PAD + count : PAD + count + 1, :]
            ghost_rows.append((steps[-1], k, count, row))
            row += 1
    wait_gy = exchange(13, 1, gy_send.at[0], gy_recv.at[0], gy_send.at[1], gy_recv.at[1])

    def around_inner(buf, comp, i):
        plane = buf.at[comp, i + 1]
        centre = plane[rows, :]
        return centre, (
            buf[comp, i, rows, :],
            buf[comp, i + 2, rows, :],
            plane[PAD - 1 : PAD - 1 + cy, :],
            plane[PAD + 1 : PAD + 1 + cy, :],
            pltpu.roll(centre, 1, 1),
            pltpu.roll(centre, cz - 1, 1),
        )

    def flow_inner(buf, comp, i):
        centre, near = around_inner(buf, comp, i)
        flow = 2.0 * forc[comp, i]
        for n in range(6):
            flow = flow + faces[n, i] * near[n]
        return centre, flow

    def early_two(i, carry):
        z_scaled[i] = weight[i] * z_faces[i]
        for comp in range(3):
            centre, flow = flow_inner(v1, comp, i)
            early[comp, i] = (1.0 - RELAXATION) * centre + weight[i] * flow
        return carry

    def gate(r, scaled, wait_x):
        def late_planes():
            wait_x()
            for side, i, face in ((0, 0, 0), (1, cx - 1, 1)):
                factor = faces[face, i]
                if scaled:
                    factor = factor * weight[i]
                for comp in range(3):
                    early[comp, i] = early[comp, i] + factor * x_recv[r - 1, side, comp]

        return late_planes

    def late_rows(r, scaled):
        def fix(i):
            for side, face, at in ((0, 2, 0), (1, 3, cy - 1)):
                factor = faces[face, i, at : at + 1, :]
                if scaled:
                    factor = factor * weight[i, at : at + 1, :]
                for comp in range(3):
                    halo = y_recv[r, side, comp, pl.ds(i, 1), :]
                    early[comp, i, at : at + 1, :] = early[comp, i, at : at + 1, :] + factor * halo

        return fix

    lax.fori_loop(0, cx, early_two, 0, unroll=UNROLL)
    wait_x, wait_y, wait_z = waits

    def pack_own(packed, value, place):
        return jnp.where(own_pair == place, turn(value, 2 * place + 1), packed)

    z_weight = nothing
    for i in range(cx):
        for comp in range(3):
            z_weight = pack_own(z_weight, z_scaled[i], comp * cx + i)
    wait_y()
    packed = nothing
    for i in inner:
        late_rows(2, True)(i)
        for comp in range(3):
            packed = pack_own(packed, early[comp, i], comp * cx + i)
    gate(2, True, wait_x)()
    for i in outer:
        late_rows(2, True)(i)
        for comp in range(3):
            packed = pack_own(packed, early[comp, i], comp * cx + i)
    wait_z()
    merged2 = halos_z(2, cy)[1]
    z_send[3] = packed + z_weight * merged2
    sent_z = send_z(3)

    def edges_two(i):
        return [edge_of(merged2, comp * cx + i) for comp in range(3)]

    def values_two(i, edges):
        factor = z_scaled[i]
        for comp in range(3):
            value = early[comp, i] + factor * edges[comp]
            v2[comp, i + 1, rows, :] = value
            keep_end(3, comp, i, value)
            yield value

    sent_x = shell_pass(outer + inner, lambda: None, lambda i: None, edges_two, values_two, 3, send_ends(3), STAGES)
    waits = [sent_x, send_y(3), sent_z]

    wait_gy()
    for buf, k, count, row in ghost_rows:
        buf[k, PAD : PAD + 1, :] = buf[k, PAD : PAD + 1, :] + gy_recv[0, row : row + 1, :]
        last = PAD + count - 1
        buf[k, last : last + 1, :] = buf[k, last : last + 1, :] + gy_recv[1, row : row + 1, :]
    mats_in.wait()
    off_low, off_high = 1.0 - flag(has_down[2]), 1.0 - flag(has_up[2])
    results = []
    groups = []
    lane8 = lax.broadcasted_iota(jnp.int32, (8, cz), 1)
    packed = jnp.zeros((8, cz), jnp.float32)
    for level, buf in enumerate((t1, t2b, t3c)):
        count = gx_counts[level]
        height = max(8, cy >> (level + 1))
        matrix = mats[0, level] - off_low * mats[1, level] - off_high * mats[2, level]
        data = buf[:, PAD : PAD + height, :].reshape(count * height, cz)
        result = jnp.dot(data, matrix, preferred_element_type=jnp.float32, precision=HIGHEST)
        for part in range(count * height // 8):
            g = len(groups)
            piece = result[8 * part : 8 * part + 8, :]
            groups.append((level, 8 * part // height, 8 * part % height, piece))
            shifted = pltpu.roll(piece, (2 * g - GHOST) % cz, 1)
            packed = jnp.where((lane8 == 2 * g) | (lane8 == 2 * g + 1), shifted, packed)
    gz_send[...] = packed
    wait_gz = exchange(14, 2, gz_send, gz_recv.at[0], gz_send, gz_recv.at[1])

    def early_misfit(i, carry):
        for comp in range(3):
            centre, flow = flow_inner(v2, comp, i)
            smooth_ref[comp, i] = centre
            early[comp, i] = flow - diag[i] * centre
        return carry

    if near_only:
        for peer in z_line:
            pl.semaphore_signal(hello_sem, inc=1, device_id=peer, device_id_type=MESH)
    lax.fori_loop(0, cx, early_misfit, 0, unroll=UNROLL)
    wait_x, *others = waits
    for wait in others:
        wait()
    merged3 = halos_z(3, cy)[1]
    squares = []

    def edges_three(i):
        return [edge_of(merged3, comp * cx + i) for comp in range(3)]

    def values_three(i, edges):
        total = None
        for comp in range(3):
            value = 0.5 * (early[comp, i] + z_faces[i] * edges[comp])
            misfit_ref[comp, i] = value
            total = value * value if total is None else total + value * value
            yield value
        squares.append(total if not squares else squares[-1] + total)

    shell_pass(inner + outer, gate(3, False, wait_x), late_rows(3, False), edges_three, values_three, None, None, STAGES)
    part = jnp.sum(squares[-1], axis=0, keepdims=True)

    def gather(slots, mine, value, peers, sems):
        slots[mine] = value
        for peer in peers:
            pltpu.make_async_remote_copy(
                slots.at[mine], slots.at[mine], sems.at[0], sems.at[1],
                device_id=peer, device_id_type=MESH,
            ).start()
        others = slots.at[pl.ds(0, len(peers))]
        return pltpu.make_async_remote_copy(
            others, others, sems.at[0], sems.at[1], device_id=peers[0], device_id_type=MESH
        )

    def total_of(slots):
        parts = [slots[n] for n in range(slots.shape[0])]
        while len(parts) > 1:
            parts = [sum(parts[n : n + 2]) for n in range(0, len(parts), 2)]
        return parts[0]

    if near_only:
        pl.semaphore_wait(hello_sem, nz - 1)
    plane_copies = gather(sums_xy, me_first, part, first_peers(), plane_sem)

    wait_gz()
    low_part, high_part = gz_recv[0], gz_recv[1]
    for g, (level, k, at, piece) in enumerate(groups):
        width = cz >> (level + 1)
        height = cy >> (level + 1)
        piece = piece + jnp.where(lane8 == 0, pltpu.roll(low_part, (cz - 2 * g - 1) % cz, 1), 0.0)
        piece = piece + jnp.where(
            lane8 == width - 1, pltpu.roll(high_part, (width - 1 - 2 * g) % cz, 1), 0.0
        )
        target = (one_ref, two_ref, three_ref)[level]
        size = min(8, height - at)
        target[k, at : at + size, :] = piece[:size, :width]

    for condition, copy in started:
        pl.when(condition)(copy.wait_send)
    plane_copies.wait()
    whole = total_of(sums_xy)
    if not one_stage:
        gather(sums_z, iz, whole, line_peers, line_sem).wait()
        whole = total_of(sums_z)
    rms_ref[...] = jnp.broadcast_to(whole, rms_ref.shape)


def writer(cells_all, *refs):
    rms, sems = refs[14], refs[15]
    copies = [pltpu.make_async_copy(refs[n], refs[7 + n], sems.at[n]) for n in (0, 5, 1, 2, 3, 4)]
    copies.append(pltpu.make_async_copy(rms, refs[13], sems.at[6]))
    for copy in copies[:6]:
        copy.start()
    whole = jnp.sum(refs[6][0:1, :], axis=1, keepdims=True)
    rms[...] = jnp.sqrt(whole / cells_all)
    copies[6].start()
    for copy in copies:
        copy.wait()


def per_device(velocity, forcing, phase_block, prefactor, yield_stress):
    _, cx, cy, cz = velocity.shape
    nx, ny, nz = lax.axis_size("gx"), lax.axis_size("gy"), lax.axis_size("gz")
    f32 = jnp.float32
    sizes = (nx, ny, nz, cx, cy, cz, prefactor.shape[0])
    mats = jnp.asarray(coarse_matrices(cz))
    blocks = phase_block.reshape(phase_block.shape[0] * phase_block.shape[1], phase_block.shape[2])
    tall = cy + 2 * PAD
    firsts = nx * ny * nz if nx * ny * nz <= ONE_STAGE else nx * ny
    ghosts = cx // 2 + cx // 4 + cx // 8
    ghosts += -ghosts % 8
    hbm = pl.BlockSpec(memory_space=pltpu.HBM)
    vmem = pl.BlockSpec(memory_space=pltpu.VMEM)
    v = pltpu.VMEM
    field = v((3, cx + 2, tall, cz), f32)
    dma = pltpu.SemaphoreType.DMA
    operands = (velocity, forcing, mats, blocks, prefactor, yield_stress)
    outs = pl.pallas_call(
        functools.partial(kernel, sizes),
        out_shape=(
            jax.ShapeDtypeStruct(velocity.shape, f32),
            jax.ShapeDtypeStruct((cx, cy, cz), f32),
            jax.ShapeDtypeStruct((cx // 2, cy // 2, cz // 2), f32),
            jax.ShapeDtypeStruct((cx // 4, cy // 4, cz // 4), f32),
            jax.ShapeDtypeStruct((cx // 8, cy // 8, cz // 8), f32),
            jax.ShapeDtypeStruct(velocity.shape, f32),
            jax.ShapeDtypeStruct((8, cz), f32),
        ),
        in_specs=[hbm] * 6,
        out_specs=(vmem,) * 7,
        scratch_shapes=[
            field,
            field,
            field,
            v((cx + 2, tall, cz), f32),
            v((3, cx, cy, cz), f32),
            v(mats.shape, f32),
            v(blocks.shape, blocks.dtype),
            pltpu.SMEM(prefactor.shape, f32),
            pltpu.SMEM(yield_stress.shape, f32),
            v((6, cx, cy, cz), f32),
            v((cx, cy, cz), f32),
            v((cx, cy, cz), f32),
            v((3, cx, cy, cz), f32),
            v((3, cx, cy, cz), f32),
            v((cx, cy, cz), f32),
            v((cx, cy, cz), f32),
            v((cx // BLOCK, cy, cz), f32),
            v((cx // BLOCK, cy, cz), f32),
            v((3, 2, 3, cy, cz), f32),
            v((3, 2, 3, cy, cz), f32),
            v((2, cy, cz), f32),
            v((4, 2, 3, cx, cz), f32),
            v((4, 2, 3, cx, cz), f32),
            v((4, cy, cz), f32),
            v((4, 2, cy, cz), f32),
            v((cx // 2 + 2, tall, cz), f32),
            v((cx // 4 + 2, tall, cz), f32),
            v((cx // 8 + 2, tall, cz), f32),
            v((2, 3, cy, cz), f32),
            v((2, 3, cy, cz), f32),
            v((cx // 2, tall, cz), f32),
            v((cx // 4, tall, cz), f32),
            v((cx // 4, tall, cz), f32),
            v((cx // 8, tall, cz), f32),
            v((cx // 8, tall, cz), f32),
            v((cx // 8, tall, cz), f32),
            v((2, ghosts, cz), f32),
            v((2, ghosts, cz), f32),
            v((8, cz), f32),
            v((2, 8, cz), f32),
            v((firsts, 1, cz), f32),
            v((nz, 1, cz), f32),
            dma((10,)),
            dma((15, 2)),
            dma((15, 2)),
            dma((2,)),
            dma((2,)),
            pltpu.SemaphoreType.REGULAR,
        ],
        compiler_params=pltpu.CompilerParams(
            collective_id=0, has_side_effects=True, vmem_limit_bytes=40 * 1024 * 1024
        ),
    )(*(pltpu.with_memory_space_constraint(a, pltpu.HBM) for a in operands))
    outs = pl.pallas_call(
        functools.partial(writer, float(3 * cx * nx * cy * ny * cz * nz)),
        out_shape=tuple(jax.ShapeDtypeStruct(out.shape, f32) for out in outs[:6])
        + (jax.ShapeDtypeStruct((1, 1), f32),),
        in_specs=[vmem] * 7,
        out_specs=(hbm,) * 7,
        scratch_shapes=[v((1, 1), f32), dma((7,))],
        compiler_params=pltpu.CompilerParams(vmem_limit_bytes=8 * 1024 * 1024),
    )(*outs)
    return outs[:6] + (outs[6].reshape(()),)


def solution(mesh):
    grid = P("gx", "gy", "gz")
    vector = P(None, "gx", "gy", "gz")
    return jax.shard_map(
        per_device,
        mesh=mesh,
        in_specs=(vector, vector, grid, P(), P()),
        out_specs=(vector, grid, grid, grid, grid, vector, P()),
        check_vma=False,
    )
```

```python
import functools

import jax
import jax.numpy as jnp
import numpy as np
from jax import lax
from jax.experimental import pallas as pl
from jax.experimental.pallas import tpu as pltpu
from jax.sharding import PartitionSpec as P

BLOCK = 4
RELAXATION = 0.8
PAD = 8
GHOST = 64
UNROLL = 4
STAGES = (3, 0, 1)
STAGES_VISC = (2, 2, 2)
ONE_STAGE = 32
ROUNDS = 4
MESH = pl.DeviceIdType.MESH
HIGHEST = lax.Precision.HIGHEST


def coarse_matrices(length):
    def chain(low_edge, high_edge):
        field = np.eye(length)
        found = []
        first = 0
        for _ in range(3):
            count = length >> (len(found) + 1)
            out = np.zeros((length, count + 2))
            for k in range(-1, count + 1):
                for shift, weight in ((-1, 1.0), (0, 3.0), (1, 3.0), (2, 1.0)):
                    source = 2 * k + shift - first
                    if 0 <= source < field.shape[1]:
                        out[:, k + 1] += weight / 8.0 * field[:, source]
            if low_edge:
                out[:, 0] = 0.0
            if high_edge:
                out[:, -1] = 0.0
            placed = np.zeros((length, length))
            placed[:, :count] = out[:, 1:-1]
            placed[:, GHOST] = out[:, 0]
            placed[:, GHOST + 1] = out[:, -1]
            found.append(placed)
            field = out
            first = -1
        return np.stack(found)

    inner = chain(False, False)
    return np.stack([inner, inner - chain(True, False), inner - chain(False, True)]).astype(np.float32)


def kernel(
    sizes,
    vel_hbm,
    forc_hbm,
    mats_hbm,
    phase_hbm,
    pref_hbm,
    yield_hbm,
    smooth_ref,
    visc_ref,
    one_ref,
    two_ref,
    three_ref,
    misfit_ref,
    rms_ref,
    v0,
    v1,
    v2,
    visc,
    forc,
    mats,
    phase_ref,
    pref_ref,
    yield_ref,
    faces,
    z_faces,
    z_scaled,
    edge0,
    early,
    weight,
    diag,
    pref_cells,
    yield_cells,
    x_send,
    x_recv,
    visc_x,
    y_send,
    y_recv,
    z_send,
    z_recv,
    cx1,
    cx2,
    cx3,
    gx_send,
    gx_recv,
    t1,
    t2a,
    t2b,
    t3a,
    t3b,
    t3c,
    gy_send,
    gy_recv,
    gz_send,
    gz_recv,
    sums_xy,
    sums_z,
    local_sem,
    send_sem,
    recv_sem,
    plane_sem,
    line_sem,
    hello_sem,
):
    nx, ny, nz, cx, cy, cz, phases = sizes
    ix, iy, iz = lax.axis_index("gx"), lax.axis_index("gy"), lax.axis_index("gz")
    rows = pl.ds(PAD, cy)

    ends_in = [
        pltpu.make_async_copy(vel_hbm.at[:, cx - 1], x_send.at[0, 0], local_sem.at[0]),
        pltpu.make_async_copy(vel_hbm.at[:, 0], x_send.at[0, 1], local_sem.at[1]),
    ]
    vel_in = [
        pltpu.make_async_copy(vel_hbm.at[comp], v0.at[comp, pl.ds(1, cx), rows, :], local_sem.at[2 + comp])
        for comp in range(3)
    ]
    forc_in = pltpu.make_async_copy(forc_hbm, forc, local_sem.at[5])
    mats_in = pltpu.make_async_copy(mats_hbm, mats, local_sem.at[6])
    phase_in = pltpu.make_async_copy(phase_hbm, phase_ref, local_sem.at[7])
    pref_in = pltpu.make_async_copy(pref_hbm, pref_ref, local_sem.at[8])
    yield_in = pltpu.make_async_copy(yield_hbm, yield_ref, local_sem.at[9])
    for copy in vel_in + ends_in:
        copy.start()

    barrier = pltpu.get_barrier_semaphore()
    one_stage = nx * ny * nz <= ONE_STAGE
    me_xy = ix * ny + iy
    me_first = me_xy * nz + iz if one_stage else me_xy

    def first_peers():
        if one_stage:
            others = [lax.rem(me_first + k, nx * ny * nz) for k in range(1, nx * ny * nz)]
            return [(o // (ny * nz), lax.rem(o // nz, ny), lax.rem(o, nz)) for o in others]
        others = [lax.rem(me_first + k, nx * ny) for k in range(1, nx * ny)]
        return [(o // ny, lax.rem(o, ny), iz) for o in others]

    line_peers = [] if one_stage else [(ix, iy, lax.rem(iz + k, nz)) for k in range(1, nz)]
    has_up = (ix < nx - 1, iy < ny - 1, iz < nz - 1)
    has_down = (ix > 0, iy > 0, iz > 0)
    up_ids = (
        (lax.rem(ix + 1, nx), iy, iz),
        (ix, lax.rem(iy + 1, ny), iz),
        (ix, iy, lax.rem(iz + 1, nz)),
    )
    down_ids = (
        (lax.rem(ix + nx - 1, nx), iy, iz),
        (ix, lax.rem(iy + ny - 1, ny), iz),
        (ix, iy, lax.rem(iz + nz - 1, nz)),
    )
    z_line = [(ix, iy, lax.rem(iz + k, nz)) for k in range(1, nz)]
    steps = [nx - 1, ny - 1, nz - 1] if one_stage else [nx - 1, ny - 1]
    near_only = one_stage and steps[0] + steps[1] <= ROUNDS and steps[2] <= ROUNDS
    if near_only:
        met = 0
        for there, peer in list(zip(has_up, up_ids)) + list(zip(has_down, down_ids)):
            met = met + there.astype(jnp.int32)

            @pl.when(there)
            def _():
                pl.semaphore_signal(barrier, inc=1, device_id=peer, device_id_type=MESH)
    else:
        if sum(steps) - max(steps) <= ROUNDS:
            greeted = [(lax.rem(ix + k, nx), iy, iz) for k in range(1, nx)]
            greeted += [(ix, lax.rem(iy + k, ny), iz) for k in range(1, ny)]
            greeted += z_line
        else:
            greeted = first_peers() + line_peers
        met = len(greeted)
        for peer in greeted:
            pl.semaphore_signal(barrier, inc=1, device_id=peer, device_id_type=MESH)
    for copy in (phase_in, pref_in, yield_in):
        copy.start()

    def clear(ref):
        ref[...] = jnp.zeros(ref.shape, jnp.float32)

    for side, present in ((0, has_down), (1, has_up)):
        @pl.when(jnp.logical_not(present[0]))
        def _():
            for r in range(3):
                clear(x_recv.at[r, side])
            clear(visc_x.at[side])
            clear(gx_recv.at[side])

        @pl.when(jnp.logical_not(present[1]))
        def _():
            for r in range(4):
                clear(y_recv.at[r, side])
            clear(gy_recv.at[side])

        @pl.when(jnp.logical_not(present[2]))
        def _():
            for r in range(4):
                clear(z_recv.at[r, side])
            clear(gz_recv.at[side])

    for buf in [v.at[comp] for v in (v0, v1, v2) for comp in range(3)] + [visc]:
        clear(buf.at[0, rows])
        clear(buf.at[cx + 1, rows])
        clear(buf.at[pl.ds(1, cx), pl.ds(PAD - 1, 1)])
        clear(buf.at[pl.ds(1, cx), pl.ds(PAD + cy, 1)])

    lane = lax.broadcasted_iota(jnp.int32, (cy, cz), 1)
    odd_lane = lax.rem(lane, 2) == 1
    lane_pair = lax.rem(lane + (cz - 1), cz) // 2
    own_pair = lane // 2
    first_lane = lane == 0
    last_lane = lane == cz - 1
    end_lane = first_lane | last_lane

    started = []

    def exchange(slot, dim, up_src, up_dst, down_src, down_dst):
        up = pltpu.make_async_remote_copy(
            up_src, up_dst, send_sem.at[slot, 0], recv_sem.at[slot, 0],
            device_id=up_ids[dim], device_id_type=MESH,
        )
        down = pltpu.make_async_remote_copy(
            down_src, down_dst, send_sem.at[slot, 1], recv_sem.at[slot, 1],
            device_id=down_ids[dim], device_id_type=MESH,
        )
        pl.when(has_up[dim])(up.start)
        pl.when(has_down[dim])(down.start)
        started.append((has_up[dim], up))
        started.append((has_down[dim], down))

        def wait():
            pl.when(has_down[dim])(up.wait_recv)
            pl.when(has_up[dim])(down.wait_recv)

        return wait

    def send_x(r, last, low, first, high):
        return exchange(3 * r, 0, last, low, first, high)

    def send_y(r):
        held = pl.ds(0, 1 if r == 1 else 3)
        return exchange(
            3 * r + 1, 1,
            y_send.at[r, 0, held], y_recv.at[r, 0, held],
            y_send.at[r, 1, held], y_recv.at[r, 1, held],
        )

    def send_z(r):
        height = pl.ds(0, visc_rows if r == 1 else cy)
        return exchange(
            3 * r + 2, 2,
            z_send.at[r, height], z_recv.at[r, 0, height],
            z_send.at[r, height], z_recv.at[r, 1, height],
        )

    def send_yz(r):
        sent_z = send_z(r)
        return [send_y(r), sent_z]

    def pack(r, comp, i, value, packed):
        y_send[r, 0, comp, pl.ds(i, 1), :] = value[cy - 1 : cy, :]
        y_send[r, 1, comp, pl.ds(i, 1), :] = value[0:1, :]
        place = 2 * (comp * cx + i) + 1
        return jnp.where(lane_pair == comp * cx + i, pltpu.roll(value, place + 1, 1), packed)

    def unpack_y(r, buf, comps):
        def body(i, carry):
            for comp in range(comps):
                target = buf.at[comp, i + 1] if comps == 3 else buf.at[i + 1]
                target[PAD - 1 : PAD, :] = y_recv[r, 0, comp, pl.ds(i, 1), :]
                target[PAD + cy : PAD + cy + 1, :] = y_recv[r, 1, comp, pl.ds(i, 1), :]
            return carry

        lax.fori_loop(0, cx, body, 0)

    visc_rows = 8 if 2 * cx * (cy // 8) <= cz else cy

    def halos_z(r, height):
        low, high = z_recv[r, 0, :height], z_recv[r, 1, :height]
        odd = odd_lane[:height]
        if r == 3:
            return None, jnp.where(odd, pltpu.roll(low, 1, 1), pltpu.roll(high, cz - 1, 1))
        return jnp.where(odd, low, high), jnp.where(odd, low, pltpu.roll(high, cz - 2, 1))

    for copy in ends_in:
        copy.wait()
    pl.semaphore_wait(barrier, met)
    waits = [send_x(0, x_send.at[0, 0], x_recv.at[0, 0], x_send.at[0, 1], x_recv.at[0, 1])]
    nothing = jnp.zeros((cy, cz), jnp.float32)
    packed = nothing
    for copy in vel_in:
        copy.wait()
    for comp in range(3):
        for i in range(cx):
            packed = pack(0, comp, i, v0[comp, i + 1, rows, :], packed)
    z_send[0] = packed
    waits += send_yz(0)
    forc_in.start()
    mats_in.start()

    phase_in.wait()
    pref_in.wait()
    yield_in.wait()
    blocks = phase_ref[...].astype(jnp.float32)
    n_rows, n_blocks = blocks.shape
    spread_z = lax.broadcasted_iota(jnp.int32, (n_blocks, cz), 1) // BLOCK
    spread_z = (spread_z == lax.broadcasted_iota(jnp.int32, (n_blocks, cz), 0)).astype(jnp.float32)
    spread_y = lax.broadcasted_iota(jnp.int32, (n_rows * BLOCK, n_rows), 0) // BLOCK
    spread_y = (
        spread_y == lax.broadcasted_iota(jnp.int32, (n_rows * BLOCK, n_rows), 1)
    ).astype(jnp.float32)
    cells = jnp.dot(blocks, spread_z, preferred_element_type=jnp.float32, precision=HIGHEST)
    cells = jnp.dot(spread_y, cells, preferred_element_type=jnp.float32, precision=HIGHEST)
    for bx in range(cx // BLOCK):
        phase = cells[bx * cy : (bx + 1) * cy, :]
        pref_value = jnp.zeros((cy, cz), jnp.float32)
        yield_value = jnp.zeros((cy, cz), jnp.float32)
        for p in range(phases):
            here = jnp.abs(phase - float(p)) < 0.5
            pref_value = jnp.where(here, pref_ref[p], pref_value)
            yield_value = jnp.where(here, yield_ref[p], yield_value)
        pref_cells[bx] = pref_value
        yield_cells[bx] = 0.5 * yield_value
    for buf in (cx1, cx2, cx3):
        for edge in (0, PAD + cy):
            buf[:, edge : edge + PAD, :] = jnp.zeros((buf.shape[0], PAD, cz), jnp.float32)
    for buf in (t1, t2a, t2b, t3a, t3b, t3c):
        buf[...] = jnp.zeros(buf.shape, jnp.float32)

    along_x, along_y, along_z = (0, 3, 4), (3, 1, 5), (4, 5, 2)

    def early_strain(i, carry):
        found = {}
        for comp in range(3):
            plane = v0.at[comp, i + 1]
            centre = plane[rows, :]
            low = jnp.where(first_lane, 0.0, pltpu.roll(centre, 1, 1))
            high = jnp.where(last_lane, 0.0, pltpu.roll(centre, cz - 1, 1))
            for n, jump in (
                (along_x[comp], v0[comp, i + 2, rows, :] - v0[comp, i, rows, :]),
                (along_y[comp], plane[PAD + 1 : PAD + 1 + cy, :] - plane[PAD - 1 : PAD - 1 + cy, :]),
                (along_z[comp], high - low),
            ):
                found[n] = found[n] + jump if n in found else jump
        for n in range(6):
            faces[n, i] = found[n]
        return carry

    lax.fori_loop(0, cx, early_strain, 0, unroll=UNROLL)
    wait_x, *others = waits
    for wait in others:
        wait()
    merged0 = halos_z(0, cy)[1]
    signed0 = jnp.where(odd_lane, -merged0, merged0)

    def gate_strain():
        wait_x()
        for comp in range(3):
            n = along_x[comp]
            faces[n, 0] = faces[n, 0] - x_recv[0, 0, comp]
            faces[n, cx - 1] = faces[n, cx - 1] + x_recv[0, 1, comp]

    def late_strain(i):
        for comp in range(3):
            n = along_y[comp]
            faces[n, i, 0:1, :] = faces[n, i, 0:1, :] - y_recv[0, 0, comp, pl.ds(i, 1), :]
            faces[n, i, cy - 1 : cy, :] = faces[n, i, cy - 1 : cy, :] + y_recv[0, 1, comp, pl.ds(i, 1), :]

    inner, outer = list(range(1, cx - 1)), [0, cx - 1]

    def shell_pass(order, gate, fix, edge, value_of, r, send_ends, stages):
        ahead, hold, behind = stages
        height, parts = (visc_rows, cy // visc_rows) if r == 1 else (cy, 1)
        pairs = lane_pair[:height]
        packed = nothing[:height]
        edges, values, rolled = {}, {}, {}
        sent = None
        ends_at = [n for n, i in enumerate(order) if i in outer]
        for t in range(cx + ahead + hold + behind):
            if t < cx:
                edges[t] = edge(order[t])
                fix(order[t])
            n = t - ahead
            if 0 <= n < cx:
                i = order[n]
                if n == ends_at[0]:
                    gate()
                values[n] = []
                for comp, value in enumerate(value_of(i, edges.pop(n))):
                    if r is not None:
                        y_send[r, 0, comp, pl.ds(i, 1), :] = value[cy - 1 : cy, :]
                        y_send[r, 1, comp, pl.ds(i, 1), :] = value[0:1, :]
                        for part in range(parts if r != 3 else 0):
                            piece = value[part * height : (part + 1) * height, :]
                            values[n].append(((comp + part) * cx + i, piece))
                if n == ends_at[1] and send_ends is not None:
                    sent = send_ends()
            n = t - ahead - hold
            if 0 <= n < cx:
                rolled[n] = [(place, turn(value, 2 * place + 2)) for place, value in values.pop(n)]
            n = t - ahead - hold - behind
            if 0 <= n < cx:
                for place, value in rolled.pop(n):
                    packed = jnp.where(pairs == place, value, packed)
        if r is None or r == 3:
            return sent
        z_send[r, pl.ds(0, height)] = packed
        return [sent] + send_yz(r)

    def turn(value, amount):
        return pltpu.roll(value, amount % cz, 1)

    def edge_of(merged, place):
        return turn(merged, cz - 1 - 2 * place)

    def edge_visc(halos, i):
        mixed, merged = halos
        places = [part * cx + i for part in range(cy // visc_rows)]
        if i in outer:
            first = first_lane[:visc_rows]
            found = [jnp.where(first, edge_of(mixed, p), edge_of(mixed, p + 1)) for p in places]
        else:
            found = [edge_of(merged, p) for p in places]
        return jnp.concatenate(found, axis=0) if len(found) > 1 else found[0]

    def edges_visc(i):
        return [edge_of(signed0, comp * cx + i) for comp in range(3)]

    def values_visc(i, edges):
        strain = [faces[n, i] for n in range(6)]
        for comp in range(3):
            n = along_z[comp]
            strain[n] = strain[n] + jnp.where(end_lane, edges[comp], 0.0)
        squared = [term * term for term in strain]
        straight = squared[0] + squared[1] + squared[2]
        skew = squared[3] + squared[4] + squared[5]
        invariant = 1.0 + (0.125 * straight + 0.0625 * skew)
        creeping = pref_cells[i // BLOCK] * jnp.exp(jnp.log(invariant) * (-1.0 / 3.0))
        plastic = yield_cells[i // BLOCK] * lax.rsqrt(invariant)
        value = jnp.minimum(creeping, plastic)
        visc[i + 1, rows, :] = value
        yield value

    def send_visc():
        return send_x(1, visc.at[cx, rows, :], visc_x.at[0], visc.at[1, rows, :], visc_x.at[1])

    waits = shell_pass(inner + outer, gate_strain, late_strain, edges_visc, values_visc, 1, send_visc, STAGES_VISC)
    for comp in range(3):
        v0[comp, 0, rows, :] = x_recv[0, 0, comp]
        v0[comp, cx + 1, rows, :] = x_recv[0, 1, comp]
    unpack_y(0, v0, 3)

    def flag(condition):
        return jnp.where(condition, 1.0, 0.0).astype(jnp.float32)

    def restrict_planes(source, first, held, count, target, level):
        for k in range(-1, count + 1):
            total = None
            for shift, factor in ((-1, 0.125), (0, 0.375), (1, 0.375), (2, 0.125)):
                at = 2 * k + shift - first
                if 0 <= at < held:
                    term = factor * source[at, rows, :]
                    total = term if total is None else total + term
            if k == -1:
                total = total * flag(has_down[0])
                gx_send[1, level] = total
            if k == count:
                total = total * flag(has_up[0])
                gx_send[0, level] = total
            target[k + 1, rows, :] = total

    restrict_planes(visc.at[pl.ds(1, cx)], 0, cx, cx // 2, cx1, 0)
    restrict_planes(cx1, -1, cx // 2 + 2, cx // 4, cx2, 1)
    restrict_planes(cx2, -1, cx // 4 + 2, cx // 8, cx3, 2)
    wait_gx = exchange(12, 0, gx_send.at[0], gx_recv.at[0], gx_send.at[1], gx_recv.at[1])

    forc_in.wait()

    def early_one(i, carry):
        plane = visc.at[i + 1]
        centre = plane[rows, :]
        visc_ref[i] = centre
        sides = (
            centre + visc[i, rows, :],
            centre + visc[i + 2, rows, :],
            centre + plane[PAD - 1 : PAD - 1 + cy, :],
            centre + plane[PAD + 1 : PAD + 1 + cy, :],
            centre + jnp.where(first_lane, 0.0, pltpu.roll(centre, 1, 1)),
            centre + jnp.where(last_lane, 0.0, pltpu.roll(centre, cz - 1, 1)),
        )
        for n in range(4):
            faces[n, i] = sides[n]
        faces[4, i] = jnp.where(first_lane, 0.0, sides[4])
        faces[5, i] = jnp.where(last_lane, 0.0, sides[5])
        diag[i] = (sides[0] + sides[1]) + (sides[2] + sides[3]) + (sides[4] + sides[5])
        for comp in range(3):
            plane = v0.at[comp, i + 1]
            centre = plane[rows, :]
            edge = edge_of(merged0, comp * cx + i)
            edge0[comp, i] = edge
            near = (
                v0[comp, i, rows, :],
                v0[comp, i + 2, rows, :],
                plane[PAD - 1 : PAD - 1 + cy, :],
                plane[PAD + 1 : PAD + 1 + cy, :],
                jnp.where(first_lane, edge, pltpu.roll(centre, 1, 1)),
                jnp.where(last_lane, edge, pltpu.roll(centre, cz - 1, 1)),
            )
            flow = 2.0 * forc[comp, i]
            for n in range(6):
                flow = flow + sides[n] * near[n]
            early[comp, i] = flow
        return carry

    lax.fori_loop(0, cx, early_one, 0, unroll=UNROLL)
    for wait in waits:
        wait()
    halos1 = halos_z(1, visc_rows)

    for side, i, face, halo_plane in ((0, 0, 0, 0), (1, cx - 1, 1, cx + 1)):
        halo = visc_x[side]
        diag[i] = diag[i] + halo
        for comp in range(3):
            early[comp, i] = early[comp, i] + halo * v0[comp, halo_plane, rows, :]

    def late_one(i):
        ends = ((0, 2, 0, PAD - 1), (1, 3, cy - 1, PAD + cy))
        for side, face, at, row in ends:
            halo = y_recv[1, side, 0, pl.ds(i, 1), :]
            diag[i, at : at + 1, :] = diag[i, at : at + 1, :] + halo
            for comp in range(3):
                near = v0[comp, i + 1, row : row + 1, :]
                early[comp, i, at : at + 1, :] = early[comp, i, at : at + 1, :] + halo * near

    def edges_one(i):
        return [edge_visc(halos1, i)]

    def values_one(i, edges):
        halo = jnp.where(end_lane, edges[0], 0.0)
        total = diag[i] + halo
        scale = RELAXATION / total
        diag[i] = total
        weight[i] = scale
        z_faces[i] = jnp.where(end_lane, visc[i + 1, rows, :] + halo, 0.0)
        for comp in range(3):
            flow = early[comp, i] + halo * edge0[comp, i]
            value = (1.0 - RELAXATION) * v0[comp, i + 1, rows, :] + scale * flow
            v1[comp, i + 1, rows, :] = value
            keep_end(2, comp, i, value)
            yield value

    def send_ends(r):
        s = r - 1
        return lambda: send_x(r, x_send.at[s, 0], x_recv.at[s, 0], x_send.at[s, 1], x_recv.at[s, 1])

    def keep_end(r, comp, i, value):
        if i == cx - 1:
            x_send[r - 1, 0, comp] = value
        if i == 0:
            x_send[r - 1, 1, comp] = value

    waits = shell_pass(outer + inner, lambda: None, late_one, edges_one, values_one, 2, send_ends(2), STAGES)

    wait_gx()
    low_y, high_y = flag(has_down[1]), flag(has_up[1])
    gx_counts = (cx // 2, cx // 4, cx // 8)
    for level, buf in enumerate((cx1, cx2, cx3)):
        buf[1, rows, :] = buf[1, rows, :] + gx_recv[0, level]
        last = gx_counts[level]
        buf[last, rows, :] = buf[last, rows, :] + gx_recv[1, level]

    def restrict_rows(source, target, count):
        size = count + 2
        a, b, c, d = (source[pl.ds(PAD - 3 + s, size, stride=2), :] for s in range(4))
        target[PAD - 1 : PAD - 1 + size, :] = 0.125 * (a + d) + 0.375 * (b + c)
        target[PAD - 1 : PAD, :] = target[PAD - 1 : PAD, :] * low_y
        target[PAD + count : PAD + count + 1, :] = target[PAD + count : PAD + count + 1, :] * high_y

    row = 0
    ghost_rows = []
    for level, (buf, steps) in enumerate(((cx1, (t1,)), (cx2, (t2a, t2b)), (cx3, (t3a, t3b, t3c)))):
        for k in range(gx_counts[level]):
            source = buf.at[k + 1]
            for depth, target in enumerate(steps):
                restrict_rows(source, target.at[k], cy >> (depth + 1))
                source = target.at[k]
            count = cy >> len(steps)
            gy_send[1, row : row + 1, :] = source[PAD - 1 : PAD, :]
            gy_send[0, row : row + 1, :] = source[PAD + count : PAD + count + 1, :]
            ghost_rows.append((steps[-1], k, count, row))
            row += 1
    wait_gy = exchange(13, 1, gy_send.at[0], gy_recv.at[0], gy_send.at[1], gy_recv.at[1])

    def around_inner(buf, comp, i):
        plane = buf.at[comp, i + 1]
        centre = plane[rows, :]
        return centre, (
            buf[comp, i, rows, :],
            buf[comp, i + 2, rows, :],
            plane[PAD - 1 : PAD - 1 + cy, :],
            plane[PAD + 1 : PAD + 1 + cy, :],
            pltpu.roll(centre, 1, 1),
            pltpu.roll(centre, cz - 1, 1),
        )

    def flow_inner(buf, comp, i):
        centre, near = around_inner(buf, comp, i)
        flow = 2.0 * forc[comp, i]
        for n in range(6):
            flow = flow + faces[n, i] * near[n]
        return centre, flow

    for side, i, face in ((0, 0, 0), (1, cx - 1, 1)):
        faces[face, i] = faces[face, i] + visc_x[side]

    def early_two(i, carry):
        for side, face, at in ((0, 2, 0), (1, 3, cy - 1)):
            halo = y_recv[1, side, 0, pl.ds(i, 1), :]
            faces[face, i, at : at + 1, :] = faces[face, i, at : at + 1, :] + halo
        z_scaled[i] = weight[i] * z_faces[i]
        for comp in range(3):
            centre, flow = flow_inner(v1, comp, i)
            early[comp, i] = (1.0 - RELAXATION) * centre + weight[i] * flow
        return carry

    def gate(r, scaled, wait_x):
        def late_planes():
            wait_x()
            for side, i, face in ((0, 0, 0), (1, cx - 1, 1)):
                factor = faces[face, i]
                if scaled:
                    factor = factor * weight[i]
                for comp in range(3):
                    early[comp, i] = early[comp, i] + factor * x_recv[r - 1, side, comp]

        return late_planes

    def late_rows(r, scaled):
        def fix(i):
            for side, face, at in ((0, 2, 0), (1, 3, cy - 1)):
                factor = faces[face, i, at : at + 1, :]
                if scaled:
                    factor = factor * weight[i, at : at + 1, :]
                for comp in range(3):
                    halo = y_recv[r, side, comp, pl.ds(i, 1), :]
                    early[comp, i, at : at + 1, :] = early[comp, i, at : at + 1, :] + factor * halo

        return fix

    lax.fori_loop(0, cx, early_two, 0, unroll=UNROLL)
    wait_x, wait_y, wait_z = waits

    def pack_own(packed, value, place):
        return jnp.where(own_pair == place, turn(value, 2 * place + 1), packed)

    z_weight = nothing
    for i in range(cx):
        for comp in range(3):
            z_weight = pack_own(z_weight, z_scaled[i], comp * cx + i)
    wait_y()
    packed = nothing
    for i in inner:
        late_rows(2, True)(i)
        for comp in range(3):
            packed = pack_own(packed, early[comp, i], comp * cx + i)
    gate(2, True, wait_x)()
    for i in outer:
        late_rows(2, True)(i)
        for comp in range(3):
            packed = pack_own(packed, early[comp, i], comp * cx + i)
    wait_z()
    merged2 = halos_z(2, cy)[1]
    z_send[3] = packed + z_weight * merged2
    sent_z = send_z(3)

    def edges_two(i):
        return [edge_of(merged2, comp * cx + i) for comp in range(3)]

    def values_two(i, edges):
        factor = z_scaled[i]
        for comp in range(3):
            value = early[comp, i] + factor * edges[comp]
            v2[comp, i + 1, rows, :] = value
            keep_end(3, comp, i, value)
            yield value

    sent_x = shell_pass(outer + inner, lambda: None, lambda i: None, edges_two, values_two, 3, send_ends(3), STAGES)
    waits = [sent_x, send_y(3), sent_z]

    wait_gy()
    for buf, k, count, row in ghost_rows:
        buf[k, PAD : PAD + 1, :] = buf[k, PAD : PAD + 1, :] + gy_recv[0, row : row + 1, :]
        last = PAD + count - 1
        buf[k, last : last + 1, :] = buf[k, last : last + 1, :] + gy_recv[1, row : row + 1, :]
    mats_in.wait()
    off_low, off_high = 1.0 - flag(has_down[2]), 1.0 - flag(has_up[2])
    results = []
    groups = []
    lane8 = lax.broadcasted_iota(jnp.int32, (8, cz), 1)
    packed = jnp.zeros((8, cz), jnp.float32)
    for level, buf in enumerate((t1, t2b, t3c)):
        count = gx_counts[level]
        height = max(8, cy >> (level + 1))
        matrix = mats[0, level] - off_low * mats[1, level] - off_high * mats[2, level]
        data = buf[:, PAD : PAD + height, :].reshape(count * height, cz)
        result = jnp.dot(data, matrix, preferred_element_type=jnp.float32, precision=HIGHEST)
        for part in range(count * height // 8):
            g = len(groups)
            piece = result[8 * part : 8 * part + 8, :]
            groups.append((level, 8 * part // height, 8 * part % height, piece))
            shifted = pltpu.roll(piece, (2 * g - GHOST) % cz, 1)
            packed = jnp.where((lane8 == 2 * g) | (lane8 == 2 * g + 1), shifted, packed)
    gz_send[...] = packed
    wait_gz = exchange(14, 2, gz_send, gz_recv.at[0], gz_send, gz_recv.at[1])

    def early_misfit(i, carry):
        for comp in range(3):
            centre, flow = flow_inner(v2, comp, i)
            smooth_ref[comp, i] = centre
            early[comp, i] = flow - diag[i] * centre
        return carry

    if near_only:
        for peer in z_line:
            pl.semaphore_signal(hello_sem, inc=1, device_id=peer, device_id_type=MESH)
    lax.fori_loop(0, cx, early_misfit, 0, unroll=UNROLL)
    wait_x, *others = waits
    for wait in others:
        wait()
    merged3 = halos_z(3, cy)[1]
    squares = []

    def edges_three(i):
        return [edge_of(merged3, comp * cx + i) for comp in range(3)]

    def values_three(i, edges):
        total = None
        for comp in range(3):
            value = 0.5 * (early[comp, i] + z_faces[i] * edges[comp])
            misfit_ref[comp, i] = value
            total = value * value if total is None else total + value * value
            yield value
        squares.append(total if not squares else squares[-1] + total)

    shell_pass(inner + outer, gate(3, False, wait_x), late_rows(3, False), edges_three, values_three, None, None, STAGES)
    part = jnp.sum(squares[-1], axis=0, keepdims=True)

    def gather(slots, mine, value, peers, sems):
        slots[mine] = value
        for peer in peers:
            pltpu.make_async_remote_copy(
                slots.at[mine], slots.at[mine], sems.at[0], sems.at[1],
                device_id=peer, device_id_type=MESH,
            ).start()
        others = slots.at[pl.ds(0, len(peers))]
        return pltpu.make_async_remote_copy(
            others, others, sems.at[0], sems.at[1], device_id=peers[0], device_id_type=MESH
        )

    def total_of(slots):
        parts = [slots[n] for n in range(slots.shape[0])]
        while len(parts) > 1:
            parts = [sum(parts[n : n + 2]) for n in range(0, len(parts), 2)]
        return parts[0]

    if near_only:
        pl.semaphore_wait(hello_sem, nz - 1)
    plane_copies = gather(sums_xy, me_first, part, first_peers(), plane_sem)

    wait_gz()
    low_part, high_part = gz_recv[0], gz_recv[1]
    for g, (level, k, at, piece) in enumerate(groups):
        width = cz >> (level + 1)
        height = cy >> (level + 1)
        piece = piece + jnp.where(lane8 == 0, pltpu.roll(low_part, (cz - 2 * g - 1) % cz, 1), 0.0)
        piece = piece + jnp.where(
            lane8 == width - 1, pltpu.roll(high_part, (width - 1 - 2 * g) % cz, 1), 0.0
        )
        target = (one_ref, two_ref, three_ref)[level]
        size = min(8, height - at)
        target[k, at : at + size, :] = piece[:size, :width]

    for condition, copy in started:
        pl.when(condition)(copy.wait_send)
    plane_copies.wait()
    whole = total_of(sums_xy)
    if not one_stage:
        gather(sums_z, iz, whole, line_peers, line_sem).wait()
        whole = total_of(sums_z)
    rms_ref[...] = jnp.broadcast_to(whole, rms_ref.shape)


def writer(cells_all, *refs):
    rms, sems = refs[14], refs[15]
    copies = [pltpu.make_async_copy(refs[n], refs[7 + n], sems.at[n]) for n in (0, 5, 1, 2, 3, 4)]
    copies.append(pltpu.make_async_copy(rms, refs[13], sems.at[6]))
    for copy in copies[:6]:
        copy.start()
    whole = jnp.sum(refs[6][0:1, :], axis=1, keepdims=True)
    rms[...] = jnp.sqrt(whole / cells_all)
    copies[6].start()
    for copy in copies:
        copy.wait()


def per_device(velocity, forcing, phase_block, prefactor, yield_stress):
    _, cx, cy, cz = velocity.shape
    nx, ny, nz = lax.axis_size("gx"), lax.axis_size("gy"), lax.axis_size("gz")
    f32 = jnp.float32
    sizes = (nx, ny, nz, cx, cy, cz, prefactor.shape[0])
    mats = jnp.asarray(coarse_matrices(cz))
    blocks = phase_block.reshape(phase_block.shape[0] * phase_block.shape[1], phase_block.shape[2])
    tall = cy + 2 * PAD
    firsts = nx * ny * nz if nx * ny * nz <= ONE_STAGE else nx * ny
    ghosts = cx // 2 + cx // 4 + cx // 8
    ghosts += -ghosts % 8
    hbm = pl.BlockSpec(memory_space=pltpu.HBM)
    vmem = pl.BlockSpec(memory_space=pltpu.VMEM)
    v = pltpu.VMEM
    field = v((3, cx + 2, tall, cz), f32)
    dma = pltpu.SemaphoreType.DMA
    operands = (velocity, forcing, mats, blocks, prefactor, yield_stress)
    outs = pl.pallas_call(
        functools.partial(kernel, sizes),
        out_shape=(
            jax.ShapeDtypeStruct(velocity.shape, f32),
            jax.ShapeDtypeStruct((cx, cy, cz), f32),
            jax.ShapeDtypeStruct((cx // 2, cy // 2, cz // 2), f32),
            jax.ShapeDtypeStruct((cx // 4, cy // 4, cz // 4), f32),
            jax.ShapeDtypeStruct((cx // 8, cy // 8, cz // 8), f32),
            jax.ShapeDtypeStruct(velocity.shape, f32),
            jax.ShapeDtypeStruct((8, cz), f32),
        ),
        in_specs=[hbm] * 6,
        out_specs=(vmem,) * 7,
        scratch_shapes=[
            field,
            field,
            field,
            v((cx + 2, tall, cz), f32),
            v((3, cx, cy, cz), f32),
            v(mats.shape, f32),
            v(blocks.shape, blocks.dtype),
            pltpu.SMEM(prefactor.shape, f32),
            pltpu.SMEM(yield_stress.shape, f32),
            v((6, cx, cy, cz), f32),
            v((cx, cy, cz), f32),
            v((cx, cy, cz), f32),
            v((3, cx, cy, cz), f32),
            v((3, cx, cy, cz), f32),
            v((cx, cy, cz), f32),
            v((cx, cy, cz), f32),
            v((cx // BLOCK, cy, cz), f32),
            v((cx // BLOCK, cy, cz), f32),
            v((3, 2, 3, cy, cz), f32),
            v((3, 2, 3, cy, cz), f32),
            v((2, cy, cz), f32),
            v((4, 2, 3, cx, cz), f32),
            v((4, 2, 3, cx, cz), f32),
            v((4, cy, cz), f32),
            v((4, 2, cy, cz), f32),
            v((cx // 2 + 2, tall, cz), f32),
            v((cx // 4 + 2, tall, cz), f32),
            v((cx // 8 + 2, tall, cz), f32),
            v((2, 3, cy, cz), f32),
            v((2, 3, cy, cz), f32),
            v((cx // 2, tall, cz), f32),
            v((cx // 4, tall, cz), f32),
            v((cx // 4, tall, cz), f32),
            v((cx // 8, tall, cz), f32),
            v((cx // 8, tall, cz), f32),
            v((cx // 8, tall, cz), f32),
            v((2, ghosts, cz), f32),
            v((2, ghosts, cz), f32),
            v((8, cz), f32),
            v((2, 8, cz), f32),
            v((firsts, 1, cz), f32),
            v((nz, 1, cz), f32),
            dma((10,)),
            dma((15, 2)),
            dma((15, 2)),
            dma((2,)),
            dma((2,)),
            pltpu.SemaphoreType.REGULAR,
        ],
        compiler_params=pltpu.CompilerParams(
            collective_id=0, has_side_effects=True, vmem_limit_bytes=40 * 1024 * 1024
        ),
    )(*(pltpu.with_memory_space_constraint(a, pltpu.HBM) for a in operands))
    outs = pl.pallas_call(
        functools.partial(writer, float(3 * cx * nx * cy * ny * cz * nz)),
        out_shape=tuple(jax.ShapeDtypeStruct(out.shape, f32) for out in outs[:6])
        + (jax.ShapeDtypeStruct((1, 1), f32),),
        in_specs=[vmem] * 7,
        out_specs=(hbm,) * 7,
        scratch_shapes=[v((1, 1), f32), dma((7,))],
        compiler_params=pltpu.CompilerParams(vmem_limit_bytes=8 * 1024 * 1024),
    )(*outs)
    return outs[:6] + (outs[6].reshape(()),)


def solution(mesh):
    grid = P("gx", "gy", "gz")
    vector = P(None, "gx", "gy", "gz")
    return jax.shard_map(
        per_device,
        mesh=mesh,
        in_specs=(vector, vector, grid, P(), P()),
        out_specs=(vector, grid, grid, grid, grid, vector, P()),
        check_vma=False,
    )
```
